256 devices in a mesh: gx: 8 (over x, core), gy: 32 (over y, z).
Axes of the slice: x: 4, y: 4, z: 8, core: 2. Of those that a mesh axis runs over, the one named last changes fastest.
Arguments:
- features: bfloat16 [65536, 128], P(('gx', 'gy')), may hold values from -6 to 6
- tile_vals: bfloat16 [16384, 128, 128], P(('gx', 'gy')), may hold values from -0.125 to 0.125
- tile_row: int32 [16384], P(('gx', 'gy')), may hold values from 0 to 511, as said below
- tile_col: int32 [16384], P(('gx', 'gy')), may hold values from 0 to 511, as said below
- tile_work: int32 [16384], P(('gx', 'gy')), may hold values from 0 to 16384, as said below
Outputs:
- product: float32 [65536, 128], P(('gx', 'gy'))
- moved_vals: bfloat16 [8192, 128, 128], P(('gx', 'gy'))
- moved_row: int32 [8192], P(('gx', 'gy'))
- moved_col: int32 [8192], P(('gx', 'gy'))
- moved_work: int32 [8192], P(('gx', 'gy'))
The draws below stay inside these ranges and needn't reach their ends.
Inputs may be any that keep to these rules, and one draw needn't show every extreme that they name: `tile_work`: on every device the live slots come first; each gx row of 32 devices holds exactly 1024 live tiles, and in every row one device has all 64 slots live. `tile_row`: A tile held by device (a, b) has a row block owned by a device of gx index a. `tile_col`: A tile held by device (a, b) has a column block owned by a device of gy index b.
All inputs are finite; a program needn't handle non-finite values.
Results may differ from the reference program's by a relative error of at most 0.001.
Values may be sent and summed in bfloat16 or wider, within the bound.
No kernel may reach another device: no remote copies, remote signals or barrier semaphores. Data moves between devices by JAX's collectives and lax.ppermute only.
A program may use at most 64 MiB of HBM per device.

```python
import jax
import jax.numpy as jnp
from jax import lax

B = 128
K = 128
VBD = 2
TD = 64
OWN = 32
NB = 512
NV = 65536
NT = 16384
N_GX = 8
N_GY = 32


def skewed_index(key, shape, extent):
    first = jax.random.randint(jax.random.fold_in(key, 11), shape, 0, extent)
    second = jax.random.randint(jax.random.fold_in(key, 12), shape, 0, extent)
    rotate = jax.random.randint(jax.random.fold_in(key, 13), (), 0, extent)
    return (first * second // extent + rotate) % extent


def draw_tile_work(key, part):
    half = N_GY // 2
    delta = jax.random.randint(jax.random.fold_in(key, 1), (N_GX, half), 1 - OWN, OWN)
    forced = jax.random.randint(jax.random.fold_in(key, 2), (N_GX,), 0, half)
    delta = jnp.where(jnp.arange(half)[None, :] == forced[:, None], OWN, delta)
    paired = jnp.concatenate([OWN + delta, OWN - delta], axis=1)
    row_keys = jax.random.split(jax.random.fold_in(key, 3), N_GX)
    counts = jax.vmap(lambda row_key, row: jax.random.permutation(row_key, row))(row_keys, paired)
    slot = jnp.arange(TD, dtype=jnp.int32)[None, None, :]
    amounts = jax.random.randint(jax.random.fold_in(key, 4), (N_GX, N_GY, TD), 1, B * B + 1)
    return jnp.where(slot < counts[:, :, None], amounts, 0).reshape(-1).astype(jnp.int32)


def draw_tile_row(key, part):
    extent = N_GY * VBD
    device = jnp.arange(NT, dtype=jnp.int32) // TD
    outer = device // N_GY
    local = skewed_index(jax.random.fold_in(key, 21), (NT,), extent)
    return (outer * extent + local).astype(jnp.int32)


def draw_tile_col(key, part):
    extent = N_GX * VBD
    device = jnp.arange(NT, dtype=jnp.int32) // TD
    inner = device % N_GY
    local = skewed_index(jax.random.fold_in(key, 31), (NT,), extent)
    return ((local // VBD * N_GY + inner) * VBD + local % VBD).astype(jnp.int32)


def block_scale(key, dims, shards, smallest, high):
    level, own = 1.0, jax.random.fold_in(key, 6)
    for axis_at, blocks in shards:
        draws = jnp.exp(jax.random.uniform(jax.random.fold_in(own, axis_at), (blocks,), jnp.float32, smallest / len(shards), high / len(shards)))
        level = level * jnp.repeat(draws, dims[axis_at] // blocks).reshape([-1 if axis == axis_at else 1 for axis in range(len(dims))])
    return level


def gaussian(key, dims, scale, limit, shards=(), kind=jnp.bfloat16):
    loudness = block_scale(key, dims, shards, -0.22, 0.18) if shards else 1.0
    entries = jax.random.normal(key, dims, jnp.float32) * scale * loudness
    return jnp.minimum(jnp.maximum(entries, -limit), limit).astype(kind)


def setup_inputs(seed: int = 0) -> dict:
    key_of = jax.random.split(jax.random.key(seed), 6)
    features = gaussian(key_of[0], (NV, K), 1.0, 6.0, ((0, 256),))
    tile_vals = gaussian(key_of[1], (NT, B, B), (B * OWN // VBD) ** -0.5, 0.125, ((0, 256),))
    tile_row = draw_tile_row(jax.random.fold_in(key_of[5], 71), 0)
    tile_col = draw_tile_col(jax.random.fold_in(key_of[5], 71), 0)
    tile_work = draw_tile_work(jax.random.fold_in(key_of[5], 71), 0)
    return dict(features=features, tile_vals=tile_vals, tile_row=tile_row, tile_col=tile_col, tile_work=tile_work)


def reference(features, tile_vals, tile_row, tile_col, tile_work):
    devices = N_GX * N_GY
    live = (tile_work > 0).astype(jnp.int32).reshape(N_GX, N_GY, TD)
    counts = jnp.sum(live, axis=2)
    offsets = jnp.cumsum(counts, axis=1) - counts
    position = offsets[:, :, None] + jnp.arange(TD, dtype=jnp.int32)[None, None, :]
    row_index = jnp.arange(N_GX, dtype=jnp.int32)[:, None, None]
    target = (row_index * N_GY + position % N_GY) * OWN + position // N_GY
    target = jnp.where(live > 0, target, devices * OWN).reshape(-1).astype(jnp.int32)
    moved_vals = jnp.zeros((devices * OWN, B, B), jnp.bfloat16).at[target].set(tile_vals, mode="drop")
    moved_row = jnp.zeros((devices * OWN,), jnp.int32).at[target].set(tile_row, mode="drop")
    moved_col = jnp.zeros((devices * OWN,), jnp.int32).at[target].set(tile_col, mode="drop")
    moved_work = jnp.zeros((devices * OWN,), jnp.int32).at[target].set(tile_work, mode="drop")
    pattern = jnp.arange(B * B, dtype=jnp.int32).reshape(B, B)
    blocks = features.reshape(NB, B, K)

    def one_device(total, device):
        begin = (device * TD).astype(jnp.int32)
        values = lax.dynamic_slice_in_dim(tile_vals, begin, TD, 0)
        work = lax.dynamic_slice_in_dim(tile_work, begin, TD, 0)
        rows = lax.dynamic_slice_in_dim(tile_row, begin, TD, 0)
        columns = lax.dynamic_slice_in_dim(tile_col, begin, TD, 0)
        masked = jnp.where(pattern[None, :, :] < work[:, None, None], values, jnp.zeros((), jnp.bfloat16))
        vectors = jnp.take(blocks, columns, axis=0)
        products = jnp.einsum("tij,tjk->tik", masked.astype(jnp.float32), vectors.astype(jnp.float32))
        return total + jax.ops.segment_sum(products, rows, num_segments=NB), None

    summed, unused = lax.scan(one_device, jnp.zeros((NB, B, K), jnp.float32), jnp.arange(devices, dtype=jnp.int32))
    return summed.reshape(NB * B, K), moved_vals, moved_row, moved_col, moved_work
```

```python
import jax
import jax.numpy as jnp
from jax import lax
from jax.experimental import pallas as pl
from jax.experimental.pallas import tpu as pltpu
from jax.sharding import Mesh
from jax.sharding import PartitionSpec as P

GY = ("y", "z")
GX_GY = ("gx", "y", "z")

ANY = pl.BlockSpec(memory_space=pl.ANY)
SMEM = pl.BlockSpec(memory_space=pltpu.SMEM)
VMEM = pl.BlockSpec(memory_space=pltpu.VMEM)


def shifted(array, axis, by):
    size = lax.axis_size(axis)
    return lax.ppermute(array, axis, [(i, (i + by) % size) for i in range(size)])


def plan_kernel(peers, slots, me_ref, meta_ref, vals_ref, sent_ref, row_ref, col_ref, work_ref, slot_ref, sems):
    me = me_ref[0]
    share = slots // peers

    def before(s, total):
        return total + jnp.where(s < me, meta_ref[s, 3 * slots], 0)

    first = lax.fori_loop(0, peers, before, jnp.int32(0))
    turn = lax.rem(first, peers)

    def copy(d, w):
        tile = lax.rem(d - turn + peers, peers) + w * peers
        return pltpu.make_async_copy(vals_ref.at[tile], sent_ref.at[d * share + w], sems.at[0])

    def start(d, carry):
        for w in range(share):
            copy(d, w).start()
        return carry

    lax.fori_loop(0, peers, start, 0)

    def source(s, begin):
        count = meta_ref[s, 3 * slots]
        j = lax.rem(me - lax.rem(begin, peers) + peers, peers)
        for w in range(share):
            at = j + w * peers

            @pl.when(at < count)
            def _():
                k = (begin + at) // peers
                row_ref[k] = meta_ref[s, at]
                col_ref[k] = meta_ref[s, slots + at]
                work_ref[k] = meta_ref[s, 2 * slots + at]
                slot_ref[k] = s * share + w

        return begin + count

    lax.fori_loop(0, peers, source, jnp.int32(0))

    pltpu.make_async_copy(vals_ref, sent_ref, sems.at[0]).wait()


def keep_kernel(owned, slot_ref, got_ref, out_ref, sems):
    def copy(k):
        return pltpu.make_async_copy(got_ref.at[slot_ref[k]], out_ref.at[k], sems.at[0])

    def start(k, carry):
        copy(k).start()
        return carry

    lax.fori_loop(0, owned, start, 0)
    pltpu.make_async_copy(got_ref.at[pl.ds(0, owned)], out_ref, sems.at[0]).wait()


def coded(x, q_ref, exps_ref, at, row):
    top = jnp.maximum(jnp.max(jnp.abs(x), axis=0, keepdims=True), 1e-30)
    exponent = jnp.ceil(jnp.log2(top))
    scaled = jnp.round(x * jnp.exp2(15.0 - exponent))
    scaled = jnp.minimum(jnp.maximum(scaled, -32767.0), 32767.0)
    q_ref[pl.ds(at, x.shape[0]), :] = scaled.astype(jnp.int32).astype(jnp.int16)
    exps_ref[pl.ds(row, 1), :] = exponent


def product_kernel(gx, gy, groups, steps, me_ref, row_ref, col_ref, work_ref, vals_ref, *refs):
    feats, rest = refs[:gx], refs[gx:]
    own_ref, q_refs, (acc, held, exps, sems) = rest[0], rest[1:groups], rest[groups:]
    step = pl.program_id(0)
    per_step, order, width = vals_ref.shape
    vblocks = held.shape[0] // gx
    blocks = acc.shape[0]
    span = blocks // groups
    a, y = me_ref[1], me_ref[2]

    @pl.when(step == 0)
    def _():
        copies = [
            pltpu.make_async_copy(f, held.at[pl.ds(k * vblocks, vblocks)], sems.at[k])
            for k, f in enumerate(feats)
        ]
        for c in copies:
            c.start()
        acc[...] = jnp.zeros_like(acc)
        for c in copies:
            c.wait()

    pattern = lax.broadcasted_iota(jnp.int32, (order, order), 0) * order + lax.broadcasted_iota(
        jnp.int32, (order, order), 1
    )
    for t in range(per_step):
        tile = step * per_step + t
        row = lax.rem(row_ref[tile], blocks)
        col = col_ref[tile]
        home = lax.div(col, gy * vblocks)
        place = lax.rem(a - home + gx, gx) * vblocks + lax.rem(col, vblocks)
        masked = jnp.where(pattern < work_ref[tile], vals_ref[t], jnp.zeros((), jnp.bfloat16))
        acc[row] += jnp.dot(masked, held[place], preferred_element_type=jnp.float32)

    @pl.when(step == steps - 1)
    def _():
        def own(i, carry):
            own_ref[pl.ds(i * order, order), :] = acc[y * span + i]
            return carry

        lax.fori_loop(0, span, own, 0)
        for k, q_ref in enumerate(q_refs, 1):
            base = lax.rem(y + k, groups) * span

            def code(i, carry):
                coded(acc[base + i], q_ref, exps, i * order, i)
                return carry

            lax.fori_loop(0, span, code, 0)
            q_ref[pl.ds(span * order, 16), :] = exps[...].astype(jnp.int32).astype(jnp.int16)


def scales_of(ref, at):
    return jnp.exp2(ref[pl.ds(at, 16), :].astype(jnp.int32).astype(jnp.float32) - 15.0)


def middle_kernel(order, groups, me_ref, own_ref, *refs):
    n = len(refs) - groups - 2
    got, own_out, q_refs, scales, exps = refs[:n], refs[n], refs[n + 1 : n + groups], refs[-2], refs[-1]
    rows = own_ref.shape[0]
    span = rows // order // groups
    z = me_ref[3]
    exps[...] = jnp.zeros_like(exps)
    for n, g in enumerate(got):
        scales[pl.ds(16 * n, 16), :] = scales_of(g, rows)

    def total(block):
        at = block * order
        x = own_ref[pl.ds(at, order), :]
        for n, g in enumerate(got):
            part = g[pl.ds(at, order), :].astype(jnp.int32).astype(jnp.float32)
            x = x + part * scales[pl.ds(16 * n + block, 1), :]
        return x

    for i in range(span):
        own_out[pl.ds(i * order, order), :] = total(z * span + i)
    for k, q_ref in enumerate(q_refs, 1):
        base = lax.rem(z + k, groups) * span
        for i in range(span):
            coded(total(base + i), q_ref, exps, i * order, i)
        q_ref[pl.ds(span * order, 16), :] = exps[...].astype(jnp.int32).astype(jnp.int16)


def last_kernel(order, own_ref, *refs):
    got, out_ref = refs[:-1], refs[-1]
    rows = own_ref.shape[0]
    for i in range(rows // order):
        at = i * order
        x = own_ref[pl.ds(at, order), :]
        for g in got:
            part = g[pl.ds(at, order), :].astype(jnp.int32).astype(jnp.float32)
            x = x + part * scales_of(g, rows)[i : i + 1, :]
        out_ref[pl.ds(at, order), :] = x


def on_device(features, tile_vals, tile_row, tile_col, tile_work):
    peers = lax.axis_size(GY)
    gx, ny, nz = (lax.axis_size(axis) for axis in GX_GY)
    slots, order, _ = tile_vals.shape
    owned = slots // 2
    width = features.shape[1]
    vblocks = features.shape[0] // order
    blocks = peers * vblocks
    me = jnp.stack([lax.axis_index(GY), *(lax.axis_index(axis) for axis in GX_GY)]).astype(jnp.int32)

    count = jnp.sum((tile_work > 0).astype(jnp.int32))
    mine = jnp.concatenate([tile_row, tile_col, tile_work, jnp.broadcast_to(count, (slots,))])
    meta = lax.all_to_all(
        jnp.broadcast_to(mine, (peers, 4 * slots)), GY, split_axis=0, concat_axis=0, tiled=True
    )

    feats = [features.reshape(vblocks, order, width)]
    feats += [shifted(feats[0], "gx", k) for k in range(1, gx)]

    small = jax.ShapeDtypeStruct((owned,), jnp.int32)
    sent, moved_row, moved_col, moved_work, kept = pl.pallas_call(
        lambda *refs: plan_kernel(peers, slots, *refs),
        in_specs=[SMEM, SMEM, ANY],
        out_specs=[ANY, SMEM, SMEM, SMEM, SMEM],
        out_shape=[jax.ShapeDtypeStruct(tile_vals.shape, tile_vals.dtype), small, small, small, small],
        scratch_shapes=[pltpu.SemaphoreType.DMA((1,))],
        name="plan",
    )(me, meta, tile_vals)
    got = lax.all_to_all(sent, GY, split_axis=0, concat_axis=0, tiled=True)

    steps = 8
    span = blocks // ny
    i16 = jnp.int16
    own, *coded_y = pl.pallas_call(
        lambda *refs: product_kernel(gx, peers, ny, steps, *refs),
        grid=(steps,),
        in_specs=[SMEM] * 4
        + [pl.BlockSpec((slots // steps, order, order), lambda i: (i, 0, 0))]
        + [ANY] * gx,
        out_specs=[pl.BlockSpec((span * order, width), lambda i: (0, 0))]
        + [pl.BlockSpec((span * order + 16, width), lambda i: (0, 0))] * (ny - 1),
        out_shape=[jax.ShapeDtypeStruct((span * order, width), jnp.float32)]
        + [jax.ShapeDtypeStruct((span * order + 16, width), i16)] * (ny - 1),
        scratch_shapes=[
            pltpu.VMEM((blocks, order, width), jnp.float32),
            pltpu.VMEM((gx * vblocks, order, width), jnp.bfloat16),
            pltpu.VMEM((span, width), jnp.float32),
            pltpu.SemaphoreType.DMA((gx,)),
        ],
        name="products",
    )(me, tile_row, tile_col, tile_work, tile_vals, *feats)
    got_y = [shifted(q, "y", k) for k, q in enumerate(coded_y, 1)]

    own, *coded_z = pl.pallas_call(
        lambda *refs: middle_kernel(order, nz, *refs),
        in_specs=[SMEM] + [VMEM] * ny,
        out_specs=[VMEM] * nz,
        out_shape=[jax.ShapeDtypeStruct((vblocks * order, width), jnp.float32)]
        + [jax.ShapeDtypeStruct((vblocks * order + 16, width), i16)] * (nz - 1),
        scratch_shapes=[
            pltpu.VMEM((16 * (ny - 1), width), jnp.float32),
            pltpu.VMEM((16, width), jnp.float32),
        ],
        name="middle",
    )(me, own, *got_y)
    got_z = [shifted(q, "z", k) for k, q in enumerate(coded_z, 1)]

    product = pl.pallas_call(
        lambda *refs: last_kernel(order, *refs),
        in_specs=[VMEM] * nz,
        out_specs=VMEM,
        out_shape=jax.ShapeDtypeStruct((vblocks * order, width), jnp.float32),
        name="last",
    )(own, *got_z)

    moved_vals = pl.pallas_call(
        lambda *refs: keep_kernel(owned, *refs),
        in_specs=[SMEM, ANY],
        out_specs=ANY,
        out_shape=jax.ShapeDtypeStruct((owned, *tile_vals.shape[1:]), tile_vals.dtype),
        scratch_shapes=[pltpu.SemaphoreType.DMA((1,))],
        name="keep",
    )(kept, got)
    return (product, moved_vals, moved_row, moved_col, moved_work)


def solution(mesh):
    finer = Mesh(mesh.devices.reshape(mesh.shape["gx"], 4, 8), GX_GY)
    in_specs = (P(GX_GY, None), P(GX_GY, None, None), P(GX_GY), P(GX_GY), P(GX_GY))
    return jax.shard_map(
        on_device, mesh=finer, in_specs=in_specs, out_specs=in_specs, check_vma=False
    )
```

```python
import jax
import jax.numpy as jnp
from jax import lax
from jax.experimental import pallas as pl
from jax.experimental.pallas import tpu as pltpu
from jax.sharding import Mesh
from jax.sharding import PartitionSpec as P

GY = ("y", "z")
GX_GY = ("gx", "y", "z")

ANY = pl.BlockSpec(memory_space=pl.ANY)
SMEM = pl.BlockSpec(memory_space=pltpu.SMEM)
VMEM = pl.BlockSpec(memory_space=pltpu.VMEM)


def in_vmem(array):
    return pltpu.with_memory_space_constraint(array, pltpu.VMEM)


def in_hbm(array):
    return pltpu.with_memory_space_constraint(array, pltpu.HBM)


def vmem(shape, dtype):
    return pltpu.VMEM(shape, dtype)


def limit(mib):
    return pltpu.CompilerParams(vmem_limit_bytes=mib * 2**20)


def shifted(array, axis, by):
    size = lax.axis_size(axis)
    return lax.ppermute(array, axis, [(i, (i + by) % size) for i in range(size)])


def tell_kernel(slots, row_ref, col_ref, work_ref, out_ref):
    work = work_ref[...].reshape(1, slots)
    count = jnp.sum((work > 0).astype(jnp.int32), axis=1, keepdims=True)
    pairs = (
        (row_ref[...].reshape(1, slots), col_ref[...].reshape(1, slots)),
        (work, jnp.broadcast_to(count, (1, slots))),
    )
    for i, pair in enumerate(pairs):
        line = jnp.concatenate(pair, axis=1)
        out_ref[:, i, :] = jnp.broadcast_to(line, (out_ref.shape[0], 2 * slots))


def plan_kernel(peers, slots, me_ref, meta_ref, vals_ref, sent_ref, row_ref, col_ref, work_ref, slot_ref, held, sems, out_sems):
    me = me_ref[0]
    share = slots // peers

    def before(s, total):
        return total + jnp.where(s < me, meta_ref[s, 1, slots], 0)

    first = lax.fori_loop(0, peers, before, jnp.int32(0))
    turn = lax.rem(first, peers)

    groups = sems.shape[0]
    part = peers // groups
    size = part * share

    def start(d, carry):
        for w in range(share):
            tile = lax.rem(d - turn + peers, peers) + w * peers
            pltpu.make_async_copy(vals_ref.at[tile], held.at[d * share + w], sems.at[d // part]).start()
        return carry

    lax.fori_loop(0, peers, start, 0)

    def piece(ref, g):
        return ref.at[pl.ds(g * size, size)]

    leaving = [
        pltpu.make_async_copy(piece(held, g), piece(sent_ref, g), out_sems.at[g]) for g in range(groups)
    ]
    for g, c in enumerate(leaving):
        pltpu.make_async_copy(piece(vals_ref, g), piece(held, g), sems.at[g]).wait()
        c.start()

    def source(s, begin):
        count = meta_ref[s, 1, slots]
        j = lax.rem(me - lax.rem(begin, peers) + peers, peers)
        for w in range(share):
            at = j + w * peers

            @pl.when(at < count)
            def _():
                k = (begin + at) // peers
                row_ref[k] = meta_ref[s, 0, at]
                col_ref[k] = meta_ref[s, 0, slots + at]
                work_ref[k] = meta_ref[s, 1, at]
                slot_ref[k] = s * share + w

        return begin + count

    lax.fori_loop(0, peers, source, jnp.int32(0))

    for c in leaving:
        c.wait()


def keep_kernel(owned, slot_ref, got_ref, out_ref, sems):
    def start(k, carry):
        pltpu.make_async_copy(got_ref.at[slot_ref[k]], out_ref.at[k], sems.at[0]).start()
        return carry

    lax.fori_loop(0, owned, start, 0)
    pltpu.make_async_copy(got_ref.at[pl.ds(0, owned)], out_ref, sems.at[0]).wait()


def coded(x, q_ref, exps_ref, at, row):
    top = jnp.maximum(jnp.max(jnp.abs(x), axis=0, keepdims=True), 1e-30)
    exponent = jnp.ceil(jnp.log2(top))
    scaled = jnp.round(x * jnp.exp2(15.0 - exponent))
    scaled = jnp.minimum(jnp.maximum(scaled, -32767.0), 32767.0)
    q_ref[pl.ds(at, x.shape[0]), :] = scaled.astype(jnp.int32).astype(jnp.int16)
    exps_ref[pl.ds(row, 1), :] = exponent


def product_kernel(gx, gy, groups, steps, me_ref, row_ref, col_ref, work_ref, vals_ref, feats_ref, *refs):
    x_refs, rest = refs[: gx // 2 - 1], refs[gx // 2 - 1 :]
    own_ref, q_refs, (tiles, acc, held, made, exps, sems) = rest[0], rest[1:groups], rest[groups:]
    slots, order, _ = tiles.shape
    per_step = slots // steps
    vblocks = held.shape[0] // gx
    blocks = acc.shape[0]
    span = blocks // groups
    a, y = me_ref[1], me_ref[2]
    cores = 2

    loads = [
        pltpu.make_async_copy(
            vals_ref.at[pl.ds(i * per_step, per_step)], tiles.at[pl.ds(i * per_step, per_step)], sems.at[i]
        )
        for i in range(steps)
    ]
    for c in loads:
        c.start()
    acc[...] = jnp.zeros_like(acc)
    for k, f in enumerate((feats_ref, *x_refs)):
        held[pl.ds(k * cores * vblocks, cores * vblocks)] = f[...]

    pattern = lax.broadcasted_iota(jnp.int32, (order, order), 0) * order + lax.broadcasted_iota(
        jnp.int32, (order, order), 1
    )
    for i in range(steps):
        loads[i].wait()

        def form(t, carry):
            tile = i * per_step + t
            col = col_ref[tile]
            home = lax.div(col, gy * vblocks)
            away = lax.rem(lax.div(a, cores) - lax.div(home, cores) + gx, gx // cores)
            side = lax.rem(a + home, cores)
            place = (away * cores + side) * vblocks + lax.rem(col, vblocks)
            masked = jnp.where(pattern < work_ref[tile], tiles[tile], jnp.zeros((), jnp.bfloat16))
            made[t] = jnp.dot(masked, held[place], preferred_element_type=jnp.float32)
            return carry

        lax.fori_loop(0, per_step, form, 0, unroll=True)

        def add(t, carry):
            row = lax.rem(row_ref[i * per_step + t], blocks)
            acc[row] += made[t]
            return carry

        lax.fori_loop(0, per_step, add, 0, unroll=True)

    def own(i, carry):
        own_ref[pl.ds(i * order, order), :] = acc[y * span + i]
        return carry

    for k, q_ref in enumerate(q_refs, 1):
        base = lax.rem(y + k, groups) * span

        def code(i, carry):
            coded(acc[base + i], q_ref, exps, i * order, i)
            return carry

        lax.fori_loop(0, span, code, 0, unroll=2)
        q_ref[pl.ds(span * order, 16), :] = exps[...].astype(jnp.int32).astype(jnp.int16)
    lax.fori_loop(0, span, own, 0)


def scales_of(ref, at):
    return jnp.exp2(ref[pl.ds(at, 16), :].astype(jnp.int32).astype(jnp.float32) - 15.0)


def middle_kernel(order, groups, me_ref, own_ref, *refs):
    n = len(refs) - groups - 2
    got, own_out, q_refs, scales, exps = refs[:n], refs[n], refs[n + 1 : n + groups], refs[-2], refs[-1]
    rows = own_ref.shape[0]
    span = rows // order // groups
    z = me_ref[3]
    exps[...] = jnp.zeros_like(exps)
    for n, g in enumerate(got):
        scales[pl.ds(16 * n, 16), :] = scales_of(g, rows)

    def total(block):
        at = block * order
        x = own_ref[pl.ds(at, order), :]
        for n, g in enumerate(got):
            part = g[pl.ds(at, order), :].astype(jnp.int32).astype(jnp.float32)
            x = x + part * scales[pl.ds(16 * n + block, 1), :]
        return x

    for i in range(span):
        own_out[pl.ds(i * order, order), :] = total(z * span + i)
    for k, q_ref in enumerate(q_refs, 1):
        base = lax.rem(z + k, groups) * span
        for i in range(span):
            coded(total(base + i), q_ref, exps, i * order, i)
        q_ref[pl.ds(span * order, 16), :] = exps[...].astype(jnp.int32).astype(jnp.int16)


def last_kernel(order, own_ref, *refs):
    got, out_ref = refs[:-1], refs[-1]
    rows = own_ref.shape[0]
    for i in range(rows // order):
        at = i * order
        x = own_ref[pl.ds(at, order), :]
        for g in got:
            part = g[pl.ds(at, order), :].astype(jnp.int32).astype(jnp.float32)
            x = x + part * scales_of(g, rows)[i : i + 1, :]
        out_ref[pl.ds(at, order), :] = x


def on_device(features, tile_vals, tile_row, tile_col, tile_work):
    peers = lax.axis_size(GY)
    gx, ny, nz = (lax.axis_size(axis) for axis in GX_GY)
    slots, order, _ = tile_vals.shape
    owned = slots // 2
    width = features.shape[1]
    vblocks = features.shape[0] // order
    blocks = peers * vblocks
    me = jnp.stack([lax.axis_index(GY), *(lax.axis_index(axis) for axis in GX_GY)]).astype(jnp.int32)

    told = pl.pallas_call(
        lambda *refs: tell_kernel(slots, *refs),
        in_specs=[VMEM] * 3,
        out_specs=VMEM,
        out_shape=vmem((peers, 2, 2 * slots), jnp.int32),
        compiler_params=limit(4),
        name="tell",
    )(tile_row, tile_col, tile_work)

    cores = 2
    mine = features.reshape(vblocks, order, width)
    swap = lax.ppermute(mine, "gx", [(i, i ^ 1) for i in range(gx)])
    meta = lax.all_to_all(told, GY, split_axis=0, concat_axis=0, tiled=True)
    both = jnp.concatenate([mine, swap])
    around = []
    for k in range(1, gx // cores):
        around.append(lax.ppermute(both, "gx", [(i, (i + cores * k) % gx) for i in range(gx)]))

    small = jax.ShapeDtypeStruct((owned,), jnp.int32)
    sent, moved_row, moved_col, moved_work, kept = pl.pallas_call(
        lambda *refs: plan_kernel(peers, slots, *refs),
        in_specs=[SMEM, SMEM, ANY],
        out_specs=[ANY, SMEM, SMEM, SMEM, SMEM],
        out_shape=[pltpu.HBM(tile_vals.shape, tile_vals.dtype), small, small, small, small],
        scratch_shapes=[
            pltpu.VMEM(tile_vals.shape, tile_vals.dtype),
            pltpu.SemaphoreType.DMA((8,)),
            pltpu.SemaphoreType.DMA((8,)),
        ],
        compiler_params=limit(4),
        name="plan",
    )(me, meta, in_hbm(tile_vals))
    got = lax.all_to_all(sent, GY, split_axis=0, concat_axis=0, tiled=True)

    steps = 8
    span = blocks // ny
    i16 = jnp.int16
    own, *coded_y = pl.pallas_call(
        lambda *refs: product_kernel(gx, peers, ny, steps, *refs),
        in_specs=[SMEM] * 4 + [ANY] + [VMEM] * (gx // cores),
        out_specs=[VMEM] * ny,
        out_shape=[vmem((span * order, width), jnp.float32)]
        + [vmem((span * order + 16, width), i16)] * (ny - 1),
        scratch_shapes=[
            pltpu.VMEM((slots, order, order), jnp.bfloat16),
            pltpu.VMEM((blocks, order, width), jnp.float32),
            pltpu.VMEM((gx * vblocks, order, width), jnp.bfloat16),
            pltpu.VMEM((slots // steps, order, width), jnp.float32),
            pltpu.VMEM((span, width), jnp.float32),
            pltpu.SemaphoreType.DMA((steps,)),
        ],
        compiler_params=limit(16),
        name="products",
    )(me, tile_row, tile_col, tile_work, in_hbm(tile_vals), *(in_vmem(f) for f in (both, *around)))
    got_y = [shifted(q, "y", k) for k, q in enumerate(coded_y, 1)]

    own, *coded_z = pl.pallas_call(
        lambda *refs: middle_kernel(order, nz, *refs),
        in_specs=[SMEM] + [VMEM] * ny,
        out_specs=[VMEM] * nz,
        out_shape=[vmem((vblocks * order, width), jnp.float32)]
        + [vmem((vblocks * order + 16, width), i16)] * (nz - 1),
        scratch_shapes=[
            pltpu.VMEM((16 * (ny - 1), width), jnp.float32),
            pltpu.VMEM((16, width), jnp.float32),
        ],
        compiler_params=limit(8),
        name="middle",
    )(me, own, *(in_vmem(g) for g in got_y))
    got_z = [shifted(q, "z", k) for k, q in enumerate(coded_z, 1)]

    product = pl.pallas_call(
        lambda *refs: last_kernel(order, *refs),
        in_specs=[VMEM] * nz,
        out_specs=VMEM,
        out_shape=jax.ShapeDtypeStruct((vblocks * order, width), jnp.float32),
        compiler_params=limit(8),
        name="last",
    )(own, *(in_vmem(g) for g in got_z))

    moved_vals = pl.pallas_call(
        lambda *refs: keep_kernel(owned, *refs),
        in_specs=[SMEM, VMEM],
        out_specs=ANY,
        out_shape=jax.ShapeDtypeStruct((owned, *tile_vals.shape[1:]), tile_vals.dtype),
        scratch_shapes=[pltpu.SemaphoreType.DMA((1,))],
        compiler_params=limit(4),
        name="keep",
    )(kept, in_vmem(got))
    return (product, moved_vals, moved_row, moved_col, moved_work)


def solution(mesh):
    finer = Mesh(mesh.devices.reshape(mesh.shape["gx"], 4, 8), GX_GY)
    in_specs = (P(GX_GY, None), P(GX_GY, None, None), P(GX_GY), P(GX_GY), P(GX_GY))

    return jax.shard_map(on_device, mesh=finer, in_specs=in_specs, out_specs=in_specs, check_vma=False)
```

```python
import jax
import jax.numpy as jnp
from jax import lax
from jax.experimental import pallas as pl
from jax.experimental.pallas import tpu as pltpu
from jax.sharding import Mesh
from jax.sharding import PartitionSpec as P

GY = ("y", "z")
GX_GY = ("gx", "y", "z")

ANY = pl.BlockSpec(memory_space=pl.ANY)
SMEM = pl.BlockSpec(memory_space=pltpu.SMEM)
VMEM = pl.BlockSpec(memory_space=pltpu.VMEM)


def in_vmem(array):
    return pltpu.with_memory_space_constraint(array, pltpu.VMEM)


def in_hbm(array):
    return pltpu.with_memory_space_constraint(array, pltpu.HBM)


def vmem(shape, dtype):
    return pltpu.VMEM(shape, dtype)


def limit(mib):
    return pltpu.CompilerParams(vmem_limit_bytes=mib * 2**20)


def shifted(array, axis, by):
    size = lax.axis_size(axis)
    return lax.ppermute(array, axis, [(i, (i + by) % size) for i in range(size)])


def tell_kernel(slots, row_ref, col_ref, work_ref, out_ref, held, sems):
    copies = [
        pltpu.make_async_copy(ref, held.at[i], sems.at[i]) for i, ref in enumerate((row_ref, col_ref, work_ref))
    ]
    for c in copies:
        c.start()
    for c in copies:
        c.wait()
    row, col, work = (held[i].reshape(1, slots) for i in range(3))
    count = jnp.sum((work > 0).astype(jnp.int32), axis=1, keepdims=True)
    for i, pair in enumerate(((row, col), (work, jnp.broadcast_to(count, (1, slots))))):
        line = jnp.concatenate(pair, axis=1)
        out_ref[:, i, :] = jnp.broadcast_to(line, (out_ref.shape[0], 2 * slots))


def stage_kernel(vals_ref, out_ref, sems):
    groups = sems.shape[0]
    size = vals_ref.shape[0] // groups
    copies = [
        pltpu.make_async_copy(
            vals_ref.at[pl.ds(g * size, size)], out_ref.at[pl.ds(g * size, size)], sems.at[g]
        )
        for g in range(groups)
    ]
    for c in copies:
        c.start()
    for c in copies:
        c.wait()


def plan_kernel(peers, slots, meta_ref, vals_ref, sent_ref, row_ref, col_ref, work_ref, slot_ref, sems):
    me = lax.axis_index("y") * lax.axis_size("z") + lax.axis_index("z")
    share = slots // peers

    def before(s, total):
        return total + jnp.where(s < me, meta_ref[s, 1, slots], 0)

    first = lax.fori_loop(0, peers, before, jnp.int32(0))
    turn = lax.rem(first, peers)

    def start(d, carry):
        for w in range(share):
            tile = lax.rem(d - turn + peers, peers) + w * peers
            pltpu.make_async_copy(vals_ref.at[tile], sent_ref.at[d * share + w], sems.at[0]).start()
        return carry

    lax.fori_loop(0, peers, start, 0, unroll=4)

    def source(s, begin):
        count = meta_ref[s, 1, slots]
        j = lax.rem(me - lax.rem(begin, peers) + peers, peers)
        for w in range(share):
            at = j + w * peers

            @pl.when(at < count)
            def _():
                k = (begin + at) // peers
                row_ref[k] = meta_ref[s, 0, at]
                col_ref[k] = meta_ref[s, 0, slots + at]
                work_ref[k] = meta_ref[s, 1, at]
                slot_ref[k] = s * share + w

        return begin + count

    lax.fori_loop(0, peers, source, jnp.int32(0))

    pltpu.make_async_copy(vals_ref, sent_ref, sems.at[0]).wait()


def keep_kernel(owned, slot_ref, got_ref, out_ref, sems):
    def start(k, carry):
        pltpu.make_async_copy(got_ref.at[slot_ref[k]], out_ref.at[k], sems.at[0]).start()
        return carry

    lax.fori_loop(0, owned, start, 0)
    pltpu.make_async_copy(got_ref.at[pl.ds(0, owned)], out_ref, sems.at[0]).wait()


def coded(x, q_ref, exps_ref, at, row):
    top = jnp.maximum(jnp.max(jnp.abs(x), axis=0, keepdims=True), 1e-30)
    exponent = jnp.ceil(jnp.log2(top))
    scaled = jnp.round(x * jnp.exp2(15.0 - exponent))
    scaled = jnp.minimum(jnp.maximum(scaled, -32767.0), 32767.0)
    q_ref[pl.ds(at, x.shape[0]), :] = scaled.astype(jnp.int32).astype(jnp.int16)
    exps_ref[pl.ds(row, 1), :] = exponent


def product_kernel(gx, gy, groups, steps, row_ref, col_ref, work_ref, tiles, feats_ref, *refs):
    x_refs, rest = refs[: gx // 2 - 1], refs[gx // 2 - 1 :]
    own_ref, q_refs, (acc, held, made, exps) = rest[0], rest[1:groups], rest[groups:]
    slots, order, _ = tiles.shape
    per_step = slots // steps
    vblocks = held.shape[0] // gx
    blocks = acc.shape[0]
    span = blocks // groups
    a, y = lax.axis_index("gx"), lax.axis_index("y")
    cores = 2

    acc[...] = jnp.zeros_like(acc)
    for k, f in enumerate((feats_ref, *x_refs)):
        held[pl.ds(k * cores * vblocks, cores * vblocks)] = f[...]

    pattern = lax.broadcasted_iota(jnp.int32, (order, order), 0) * order + lax.broadcasted_iota(
        jnp.int32, (order, order), 1
    )
    for i in range(steps):

        def form(t, carry):
            tile = i * per_step + t
            col = col_ref[tile]
            home = lax.div(col, gy * vblocks)
            away = lax.rem(lax.div(a, cores) - lax.div(home, cores) + gx, gx // cores)
            side = lax.rem(a + home, cores)
            place = (away * cores + side) * vblocks + lax.rem(col, vblocks)
            masked = jnp.where(pattern < work_ref[tile], tiles[tile], jnp.zeros((), jnp.bfloat16))
            made[t] = jnp.dot(masked, held[place], preferred_element_type=jnp.float32)
            return carry

        lax.fori_loop(0, per_step, form, 0, unroll=True)

        def add(t, carry):
            row = lax.rem(row_ref[i * per_step + t], blocks)
            acc[row] += made[t]
            return carry

        lax.fori_loop(0, per_step, add, 0, unroll=True)

    def own(i, carry):
        own_ref[pl.ds(i * order, order), :] = acc[y * span + i]
        return carry

    for k, q_ref in enumerate(q_refs, 1):
        base = lax.rem(y + k, groups) * span

        def code(i, carry):
            coded(acc[base + i], q_ref, exps, i * order, i)
            return carry

        lax.fori_loop(0, span, code, 0, unroll=2)
        q_ref[pl.ds(span * order, 16), :] = exps[...].astype(jnp.int32).astype(jnp.int16)
    lax.fori_loop(0, span, own, 0)


def scales_of(ref, at):
    return jnp.exp2(ref[pl.ds(at, 16), :].astype(jnp.int32).astype(jnp.float32) - 15.0)


def middle_kernel(order, groups, own_ref, *refs):
    n = len(refs) - groups - 2
    got, own_out, q_refs, scales, exps = refs[:n], refs[n], refs[n + 1 : n + groups], refs[-2], refs[-1]
    rows = own_ref.shape[0]
    span = rows // order // groups
    z = lax.axis_index("z")
    exps[...] = jnp.zeros_like(exps)
    for n, g in enumerate(got):
        scales[pl.ds(16 * n, 16), :] = scales_of(g, rows)

    def total(block):
        at = block * order
        x = own_ref[pl.ds(at, order), :]
        for n, g in enumerate(got):
            part = g[pl.ds(at, order), :].astype(jnp.int32).astype(jnp.float32)
            x = x + part * scales[pl.ds(16 * n + block, 1), :]
        return x

    for i in range(span):
        own_out[pl.ds(i * order, order), :] = total(z * span + i)
    for k, q_ref in enumerate(q_refs, 1):
        base = lax.rem(z + k, groups) * span
        for i in range(span):
            coded(total(base + i), q_ref, exps, i * order, i)
        q_ref[pl.ds(span * order, 16), :] = exps[...].astype(jnp.int32).astype(jnp.int16)


def last_kernel(order, own_ref, *refs):
    got, out_ref = refs[:-1], refs[-1]
    rows = own_ref.shape[0]
    for i in range(rows // order):
        at = i * order
        x = own_ref[pl.ds(at, order), :]
        for g in got:
            part = g[pl.ds(at, order), :].astype(jnp.int32).astype(jnp.float32)
            x = x + part * scales_of(g, rows)[i : i + 1, :]
        out_ref[pl.ds(at, order), :] = x


def on_device(features, tile_vals, tile_row, tile_col, tile_work):
    peers = lax.axis_size(GY)
    gx, ny, nz = (lax.axis_size(axis) for axis in GX_GY)
    slots, order, _ = tile_vals.shape
    owned = slots // 2
    width = features.shape[1]
    vblocks = features.shape[0] // order
    blocks = peers * vblocks
    told = pl.pallas_call(
        lambda *refs: tell_kernel(slots, *refs),
        in_specs=[ANY] * 3,
        out_specs=VMEM,
        out_shape=jax.ShapeDtypeStruct((peers, 2, 2 * slots), jnp.int32),
        scratch_shapes=[pltpu.VMEM((3, slots), jnp.int32), pltpu.SemaphoreType.DMA((3,))],
        compiler_params=limit(4),
        name="tell",
    )(*(in_hbm(t) for t in (tile_row, tile_col, tile_work)))

    cores = 2
    mine = features.reshape(vblocks, order, width)
    swap = lax.ppermute(mine, "gx", [(i, i ^ 1) for i in range(gx)])
    meta = lax.all_to_all(told, GY, split_axis=0, concat_axis=0, tiled=True)
    both = jnp.concatenate([mine, swap])
    tiles = pl.pallas_call(
        stage_kernel,
        in_specs=[ANY],
        out_specs=VMEM,
        out_shape=vmem(tile_vals.shape, tile_vals.dtype),
        scratch_shapes=[pltpu.SemaphoreType.DMA((8,))],
        compiler_params=limit(4),
        name="stage",
    )(in_hbm(tile_vals))
    around = []
    for k in range(1, gx // cores):
        around.append(lax.ppermute(both, "gx", [(i, (i + cores * k) % gx) for i in range(gx)]))

    small = jax.ShapeDtypeStruct((owned,), jnp.int32)
    sent, moved_row, moved_col, moved_work, kept = pl.pallas_call(
        lambda *refs: plan_kernel(peers, slots, *refs),
        in_specs=[SMEM, VMEM],
        out_specs=[ANY, SMEM, SMEM, SMEM, SMEM],
        out_shape=[pltpu.HBM(tile_vals.shape, tile_vals.dtype), small, small, small, small],
        scratch_shapes=[pltpu.SemaphoreType.DMA((1,))],
        compiler_params=limit(4),
        name="plan",
    )(meta, in_vmem(tiles))
    got = lax.all_to_all(sent, GY, split_axis=0, concat_axis=0, tiled=True)

    steps = 8
    span = blocks // ny
    i16 = jnp.int16
    own, *coded_y = pl.pallas_call(
        lambda *refs: product_kernel(gx, peers, ny, steps, *refs),
        in_specs=[SMEM] * 3 + [VMEM] * (1 + gx // cores),
        out_specs=[VMEM] * ny,
        out_shape=[vmem((span * order, width), jnp.float32)]
        + [vmem((span * order + 16, width), i16)] * (ny - 1),
        scratch_shapes=[
            pltpu.VMEM((blocks, order, width), jnp.float32),
            pltpu.VMEM((gx * vblocks, order, width), jnp.bfloat16),
            pltpu.VMEM((slots // steps, order, width), jnp.float32),
            pltpu.VMEM((span, width), jnp.float32),
        ],
        compiler_params=limit(16),
        name="products",
    )(tile_row, tile_col, tile_work, *(in_vmem(f) for f in (tiles, both, *around)))
    got_y = []
    for k, q in enumerate(coded_y, 1):
        got_y.append(shifted(q, "y", k))

    own, *coded_z = pl.pallas_call(
        lambda *refs: middle_kernel(order, nz, *refs),
        in_specs=[VMEM] * ny,
        out_specs=[VMEM] * nz,
        out_shape=[vmem((vblocks * order, width), jnp.float32)]
        + [vmem((vblocks * order + 16, width), i16)] * (nz - 1),
        scratch_shapes=[
            pltpu.VMEM((16 * (ny - 1), width), jnp.float32),
            pltpu.VMEM((16, width), jnp.float32),
        ],
        compiler_params=limit(8),
        name="middle",
    )(own, *(in_vmem(g) for g in got_y))
    got_z = [shifted(q, "z", k) for k, q in enumerate(coded_z, 1)]

    product = pl.pallas_call(
        lambda *refs: last_kernel(order, *refs),
        in_specs=[VMEM] * nz,
        out_specs=VMEM,
        out_shape=jax.ShapeDtypeStruct((vblocks * order, width), jnp.float32),
        compiler_params=limit(8),
        name="last",
    )(own, *(in_vmem(g) for g in got_z))

    moved_vals = pl.pallas_call(
        lambda *refs: keep_kernel(owned, *refs),
        in_specs=[SMEM, VMEM],
        out_specs=ANY,
        out_shape=jax.ShapeDtypeStruct((owned, *tile_vals.shape[1:]), tile_vals.dtype),
        scratch_shapes=[pltpu.SemaphoreType.DMA((1,))],
        compiler_params=limit(4),
        name="keep",
    )(kept, in_vmem(got))
    return (product, moved_vals, moved_row, moved_col, moved_work)


def solution(mesh):
    finer = Mesh(mesh.devices.reshape(mesh.shape["gx"], 4, 8), GX_GY)
    in_specs = (P(GX_GY, None), P(GX_GY, None, None), P(GX_GY), P(GX_GY), P(GX_GY))

    return jax.shard_map(on_device, mesh=finer, in_specs=in_specs, out_specs=in_specs, check_vma=False)
```

```python
import jax
import jax.numpy as jnp
from jax import lax
from jax.experimental import pallas as pl
from jax.experimental.pallas import tpu as pltpu
from jax.sharding import Mesh
from jax.sharding import PartitionSpec as P

GY = ("y", "z")
GX_GY = ("gx", "y", "z")

ANY = pl.BlockSpec(memory_space=pl.ANY)
SMEM = pl.BlockSpec(memory_space=pltpu.SMEM)
VMEM = pl.BlockSpec(memory_space=pltpu.VMEM)


def in_vmem(array):
    return pltpu.with_memory_space_constraint(array, pltpu.VMEM)


def in_hbm(array):
    return pltpu.with_memory_space_constraint(array, pltpu.HBM)


def vmem(shape, dtype):
    return pltpu.VMEM(shape, dtype)


def limit(mib):
    return pltpu.CompilerParams(vmem_limit_bytes=mib * 2**20)


def shifted(array, axis, by):
    size = lax.axis_size(axis)
    return lax.ppermute(array, axis, [(i, (i + by) % size) for i in range(size)])


def tell_kernel(slots, row_ref, col_ref, work_ref, out_ref, held, sems):
    copies = [
        pltpu.make_async_copy(ref, held.at[i], sems.at[i]) for i, ref in enumerate((row_ref, col_ref, work_ref))
    ]
    for c in copies:
        c.start()
    for c in copies:
        c.wait()
    row, col, work = (held[i].reshape(1, slots) for i in range(3))
    count = jnp.sum((work > 0).astype(jnp.int32), axis=1, keepdims=True)
    for i, pair in enumerate(((row, col), (work, jnp.broadcast_to(count, (1, slots))))):
        line = jnp.concatenate(pair, axis=1)
        out_ref[:, i, :] = jnp.broadcast_to(line, (out_ref.shape[0], 2 * slots))


def stage_kernel(vals_ref, out_ref, sems):
    groups = sems.shape[0]
    size = vals_ref.shape[0] // groups
    copies = [
        pltpu.make_async_copy(
            vals_ref.at[pl.ds(g * size, size)], out_ref.at[pl.ds(g * size, size)], sems.at[g]
        )
        for g in range(groups)
    ]
    for c in copies:
        c.start()
    for c in copies:
        c.wait()


def plan_kernel(peers, slots, meta_ref, vals_ref, sent_ref, row_ref, col_ref, work_ref, slot_ref, sems):
    me = lax.axis_index("y") * lax.axis_size("z") + lax.axis_index("z")
    share = slots // peers

    def before(s, total):
        return total + jnp.where(s < me, meta_ref[s, 1, slots], 0)

    first = lax.fori_loop(0, peers, before, jnp.int32(0))
    turn = lax.rem(first, peers)

    def start(d, carry):
        for w in range(share):
            tile = lax.rem(d - turn + peers, peers) + w * peers
            pltpu.make_async_copy(vals_ref.at[tile], sent_ref.at[d * share + w], sems.at[0]).start()
        return carry

    lax.fori_loop(0, peers, start, 0, unroll=4)

    def source(s, begin):
        count = meta_ref[s, 1, slots]
        j = lax.rem(me - lax.rem(begin, peers) + peers, peers)
        for w in range(share):
            at = j + w * peers

            @pl.when(at < count)
            def _():
                k = (begin + at) // peers
                row_ref[k] = meta_ref[s, 0, at]
                col_ref[k] = meta_ref[s, 0, slots + at]
                work_ref[k] = meta_ref[s, 1, at]
                slot_ref[k] = s * share + w

        return begin + count

    lax.fori_loop(0, peers, source, jnp.int32(0))

    pltpu.make_async_copy(vals_ref, sent_ref, sems.at[0]).wait()


def keep_kernel(owned, slot_ref, got_ref, out_ref, sems):
    def start(k, carry):
        pltpu.make_async_copy(got_ref.at[slot_ref[k]], out_ref.at[k], sems.at[0]).start()
        return carry

    lax.fori_loop(0, owned, start, 0)
    pltpu.make_async_copy(got_ref.at[pl.ds(0, owned)], out_ref, sems.at[0]).wait()


def coded(x, q_ref, exps_ref, at, row):
    top = jnp.maximum(jnp.max(jnp.abs(x), axis=0, keepdims=True), 1e-30)
    exponent = jnp.ceil(jnp.log2(top))
    scaled = jnp.round(x * jnp.exp2(15.0 - exponent))
    scaled = jnp.minimum(jnp.maximum(scaled, -32767.0), 32767.0)
    q_ref[pl.ds(at, x.shape[0]), :] = scaled.astype(jnp.int32).astype(jnp.int16)
    exps_ref[pl.ds(row, 1), :] = exponent


def product_kernel(gx, gy, groups, steps, row_ref, col_ref, work_ref, tiles, feats_ref, swap_ref, *refs):
    own_ref, q_refs, (acc, held, made, exps) = refs[0], refs[1:-4], refs[-4:]
    slots, order, _ = tiles.shape
    per_step = slots // steps
    vblocks = held.shape[0] // gx
    blocks = acc.shape[0]
    span = blocks // groups
    a, y = lax.axis_index("gx"), lax.axis_index("y")
    cores = 2
    halves = vblocks
    each = span // halves

    acc[...] = jnp.zeros_like(acc)
    for k, f in enumerate((feats_ref, swap_ref)):
        held[pl.ds(k * f.shape[0], f.shape[0])] = f[...]

    pattern = lax.broadcasted_iota(jnp.int32, (order, order), 0) * order + lax.broadcasted_iota(
        jnp.int32, (order, order), 1
    )
    for i in range(steps):

        def form(t, carry):
            tile = i * per_step + t
            col = col_ref[tile]
            home = lax.div(col, gy * vblocks)
            away = lax.rem(lax.div(a, cores) - lax.div(home, cores) + gx, gx // cores)
            side = lax.rem(a + home, cores)
            place = (side * (gx // cores) + away) * vblocks + lax.rem(col, vblocks)
            masked = jnp.where(pattern < work_ref[tile], tiles[tile], jnp.zeros((), jnp.bfloat16))
            made[t] = jnp.dot(masked, held[place], preferred_element_type=jnp.float32)
            return carry

        lax.fori_loop(0, per_step, form, 0, unroll=True)

        def add(t, carry):
            row = lax.rem(row_ref[i * per_step + t], blocks)
            acc[row] += made[t]
            return carry

        lax.fori_loop(0, per_step, add, 0, unroll=True)

    def own(i, carry):
        own_ref[pl.ds(i * order, order), :] = acc[y * span + i]
        return carry

    for n, q_ref in enumerate(q_refs):
        base = lax.rem(y + 1 + n % (groups - 1), groups) * span + n // (groups - 1)

        def code(i, carry):
            coded(acc[base + i * halves], q_ref, exps, i * order, i)
            return carry

        lax.fori_loop(0, each, code, 0, unroll=2)
        q_ref[pl.ds(each * order, each), :] = exps[...].astype(jnp.int32).astype(jnp.int16)
    lax.fori_loop(0, span, own, 0)


def scales_of(ref, at):
    exps = ref[pl.ds(at, ref.shape[0] - at), :].astype(jnp.int32).astype(jnp.float32)
    return jnp.exp2(exps - 15.0)


def middle_kernel(order, halves, half, own_ref, *refs):
    got, own_out, q_refs, scales, exps = refs[:3], refs[3], refs[4:-2], refs[-2], refs[-1]
    groups = len(q_refs) + 1
    rows = groups * order
    z = lax.axis_index("z")
    exps[...] = jnp.zeros_like(exps)
    for n, g in enumerate(got):
        scales[pl.ds(groups * n, groups), :] = scales_of(g, rows)

    def total(block):
        x = own_ref[pl.ds((block * halves + half) * order, order), :]
        for n, g in enumerate(got):
            part = g[pl.ds(block * order, order), :].astype(jnp.int32).astype(jnp.float32)
            x = x + part * scales[pl.ds(groups * n + block, 1), :]
        return x

    own_out[...] = total(z)
    for k, q_ref in enumerate(q_refs, 1):
        coded(total(lax.rem(z + k, groups)), q_ref, exps, 0, 0)
        q_ref[pl.ds(order, exps.shape[0]), :] = exps[...].astype(jnp.int32).astype(jnp.int16)


def last_kernel(order, halves, *refs):
    out_ref = refs[-1]
    each = (len(refs) - 1) // halves
    for h in range(halves):
        own, got = refs[h * each], refs[h * each + 1 : (h + 1) * each]
        x = own[...]
        for g in got:
            part = g[pl.ds(0, order), :].astype(jnp.int32).astype(jnp.float32)
            x = x + part * scales_of(g, order)[0:1, :]
        out_ref[pl.ds(h * order, order), :] = x


def on_device(features, tile_vals, tile_row, tile_col, tile_work):
    peers = lax.axis_size(GY)
    gx, ny, nz = (lax.axis_size(axis) for axis in GX_GY)
    slots, order, _ = tile_vals.shape
    owned = slots // 2
    width = features.shape[1]
    vblocks = features.shape[0] // order
    blocks = peers * vblocks
    told = pl.pallas_call(
        lambda *refs: tell_kernel(slots, *refs),
        in_specs=[ANY] * 3,
        out_specs=VMEM,
        out_shape=jax.ShapeDtypeStruct((peers, 2, 2 * slots), jnp.int32),
        scratch_shapes=[pltpu.VMEM((3, slots), jnp.int32), pltpu.SemaphoreType.DMA((3,))],
        compiler_params=limit(4),
        name="tell",
    )(*(in_hbm(t) for t in (tile_row, tile_col, tile_work)))

    cores = 2
    mine = [features.reshape(vblocks, order, width)]
    for k in range(1, gx // cores):
        mine.append(lax.ppermute(mine[0], "gx", [(i, (i + cores * k) % gx) for i in range(gx)]))
    meta = lax.all_to_all(told, GY, split_axis=0, concat_axis=0, tiled=True)
    feats = jnp.concatenate(mine)
    swapped = lax.ppermute(feats, "gx", [(i, i ^ 1) for i in range(gx)])
    tiles = pl.pallas_call(
        stage_kernel,
        in_specs=[ANY],
        out_specs=VMEM,
        out_shape=vmem(tile_vals.shape, tile_vals.dtype),
        scratch_shapes=[pltpu.SemaphoreType.DMA((8,))],
        compiler_params=limit(4),
        name="stage",
    )(in_hbm(tile_vals))
    small = jax.ShapeDtypeStruct((owned,), jnp.int32)
    sent, moved_row, moved_col, moved_work, kept = pl.pallas_call(
        lambda *refs: plan_kernel(peers, slots, *refs),
        in_specs=[SMEM, VMEM],
        out_specs=[ANY, SMEM, SMEM, SMEM, SMEM],
        out_shape=[pltpu.HBM(tile_vals.shape, tile_vals.dtype), small, small, small, small],
        scratch_shapes=[pltpu.SemaphoreType.DMA((1,))],
        compiler_params=limit(4),
        name="plan",
    )(meta, in_vmem(tiles))
    got = lax.all_to_all(sent, GY, split_axis=0, concat_axis=0, tiled=True)

    steps = 8
    span = blocks // ny
    halves = vblocks
    i16 = jnp.int16
    own, *coded_y = pl.pallas_call(
        lambda *refs: product_kernel(gx, peers, ny, steps, *refs),
        in_specs=[SMEM] * 3 + [VMEM] * 3,
        out_specs=[VMEM] * (1 + halves * (ny - 1)),
        out_shape=[vmem((span * order, width), jnp.float32)]
        + [vmem((nz * order + nz, width), i16)] * (halves * (ny - 1)),
        scratch_shapes=[
            pltpu.VMEM((blocks, order, width), jnp.float32),
            pltpu.VMEM((gx * vblocks, order, width), jnp.bfloat16),
            pltpu.VMEM((slots // steps, order, width), jnp.float32),
            pltpu.VMEM((nz, width), jnp.float32),
        ],
        compiler_params=limit(16),
        name="products",
    )(tile_row, tile_col, tile_work, *(in_vmem(f) for f in (tiles, feats, swapped)))

    pieces = []
    for h in range(halves):
        got_y = []
        for k in range(1, ny):
            got_y.append(shifted(coded_y[h * (ny - 1) + k - 1], "y", k))
        own_z, *coded_z = pl.pallas_call(
            lambda *refs: middle_kernel(order, halves, h, *refs),
            in_specs=[VMEM] * ny,
            out_specs=[VMEM] * nz,
            out_shape=[vmem((order, width), jnp.float32)] + [vmem((order + 8, width), i16)] * (nz - 1),
            scratch_shapes=[
                pltpu.VMEM((nz * (ny - 1), width), jnp.float32),
                pltpu.VMEM((8, width), jnp.float32),
            ],
            compiler_params=limit(8),
        )(in_vmem(own), *(in_vmem(g) for g in got_y))
        pieces.append(own_z)
        for k, q in enumerate(coded_z, 1):
            pieces.append(shifted(q, "z", k))

    product = pl.pallas_call(
        lambda *refs: last_kernel(order, halves, *refs),
        in_specs=[VMEM] * len(pieces),
        out_specs=VMEM,
        out_shape=jax.ShapeDtypeStruct((vblocks * order, width), jnp.float32),
        compiler_params=limit(8),
        name="last",
    )(*(in_vmem(g) for g in pieces))

    moved_vals = pl.pallas_call(
        lambda *refs: keep_kernel(owned, *refs),
        in_specs=[SMEM, VMEM],
        out_specs=ANY,
        out_shape=jax.ShapeDtypeStruct((owned, *tile_vals.shape[1:]), tile_vals.dtype),
        scratch_shapes=[pltpu.SemaphoreType.DMA((1,))],
        compiler_params=limit(4),
        name="keep",
    )(kept, in_vmem(got))
    return (product, moved_vals, moved_row, moved_col, moved_work)


def solution(mesh):
    finer = Mesh(mesh.devices.reshape(mesh.shape["gx"], 4, 8), GX_GY)
    in_specs = (P(GX_GY, None), P(GX_GY, None, None), P(GX_GY), P(GX_GY), P(GX_GY))

    return jax.shard_map(on_device, mesh=finer, in_specs=in_specs, out_specs=in_specs, check_vma=False)
```

```python
import jax
import jax.numpy as jnp
from jax import lax
from jax.experimental import pallas as pl
from jax.experimental.pallas import tpu as pltpu
from jax.sharding import Mesh
from jax.sharding import PartitionSpec as P

GY = ("y", "z")
GX_GY = ("gx", "y", "z")

ANY = pl.BlockSpec(memory_space=pl.ANY)
SMEM = pl.BlockSpec(memory_space=pltpu.SMEM)
VMEM = pl.BlockSpec(memory_space=pltpu.VMEM)


def in_vmem(array):
    return pltpu.with_memory_space_constraint(array, pltpu.VMEM)


def in_hbm(array):
    return pltpu.with_memory_space_constraint(array, pltpu.HBM)


def vmem(shape, dtype):
    return pltpu.VMEM(shape, dtype)


def limit(mib):
    return pltpu.CompilerParams(vmem_limit_bytes=mib * 2**20)


def shifted(array, axis, by):
    size = lax.axis_size(axis)
    return lax.ppermute(array, axis, [(i, (i + by) % size) for i in range(size)])


def tell_kernel(slots, row_ref, col_ref, work_ref, out_ref, held, sems):
    copies = [
        pltpu.make_async_copy(ref, held.at[i], sems.at[i]) for i, ref in enumerate((row_ref, col_ref, work_ref))
    ]
    for c in copies:
        c.start()
    for c in copies:
        c.wait()
    row, col, work = (held[i].reshape(1, slots) for i in range(3))
    count = jnp.sum((work > 0).astype(jnp.int32), axis=1, keepdims=True)
    for i, pair in enumerate(((row, col), (work, jnp.broadcast_to(count, (1, slots))))):
        line = jnp.concatenate(pair, axis=1)
        out_ref[:, i, :] = jnp.broadcast_to(line, (out_ref.shape[0], 2 * slots))


def stage_kernel(vals_ref, out_ref, sems):
    groups = sems.shape[0]
    size = vals_ref.shape[0] // groups
    copies = [
        pltpu.make_async_copy(
            vals_ref.at[pl.ds(g * size, size)], out_ref.at[pl.ds(g * size, size)], sems.at[g]
        )
        for g in range(groups)
    ]
    for c in copies:
        c.start()
    for c in copies:
        c.wait()


def plan_kernel(peers, slots, meta_ref, vals_ref, sent_ref, row_ref, col_ref, work_ref, slot_ref, sems):
    me = lax.axis_index("y") * lax.axis_size("z") + lax.axis_index("z")
    share = slots // peers

    def before(s, total):
        return total + jnp.where(s < me, meta_ref[s, 1, slots], 0)

    first = lax.fori_loop(0, peers, before, jnp.int32(0))
    turn = lax.rem(first, peers)

    def start(d, carry):
        for w in range(share):
            tile = lax.rem(d - turn + peers, peers) + w * peers
            pltpu.make_async_copy(vals_ref.at[tile], sent_ref.at[d * share + w], sems.at[0]).start()
        return carry

    lax.fori_loop(0, peers, start, 0, unroll=4)

    def source(s, begin):
        count = meta_ref[s, 1, slots]
        j = lax.rem(me - lax.rem(begin, peers) + peers, peers)
        for w in range(share):
            at = j + w * peers

            @pl.when(at < count)
            def _():
                k = (begin + at) // peers
                row_ref[k] = meta_ref[s, 0, at]
                col_ref[k] = meta_ref[s, 0, slots + at]
                work_ref[k] = meta_ref[s, 1, at]
                slot_ref[k] = s * share + w

        return begin + count

    lax.fori_loop(0, peers, source, jnp.int32(0))

    pltpu.make_async_copy(vals_ref, sent_ref, sems.at[0]).wait()


def keep_kernel(owned, slot_ref, got_ref, out_ref, sems):
    def start(k, carry):
        pltpu.make_async_copy(got_ref.at[slot_ref[k]], out_ref.at[k], sems.at[0]).start()
        return carry

    lax.fori_loop(0, owned, start, 0)
    pltpu.make_async_copy(got_ref.at[pl.ds(0, owned)], out_ref, sems.at[0]).wait()


def coded(x, q_ref, exps_ref, at, row):
    top = jnp.maximum(jnp.max(jnp.abs(x), axis=0, keepdims=True), 1e-30)
    exponent = jnp.ceil(jnp.log2(top))
    scaled = jnp.round(x * jnp.exp2(15.0 - exponent))
    scaled = jnp.minimum(jnp.maximum(scaled, -32767.0), 32767.0)
    q_ref[pl.ds(at, x.shape[0]), :] = scaled.astype(jnp.int32).astype(jnp.int16)
    exps_ref[pl.ds(row, 1), :] = exponent


def product_kernel(gx, gy, groups, steps, row_ref, col_ref, work_ref, tiles, feats_ref, swap_ref, *refs):
    own_ref, q_refs, (acc, held, made, exps) = refs[0], refs[1:-4], refs[-4:]
    slots, order, _ = tiles.shape
    per_step = slots // steps
    vblocks = held.shape[0] // gx
    blocks = acc.shape[0]
    span = blocks // groups
    a, y = lax.axis_index("gx"), lax.axis_index("y")
    cores = 2

    acc[...] = jnp.zeros_like(acc)
    for k, f in enumerate((feats_ref, swap_ref)):
        held[pl.ds(k * f.shape[0], f.shape[0])] = f[...]

    pattern = lax.broadcasted_iota(jnp.int32, (order, order), 0) * order + lax.broadcasted_iota(
        jnp.int32, (order, order), 1
    )
    for i in range(steps):

        def form(t, carry):
            tile = i * per_step + t
            col = col_ref[tile]
            home = lax.div(col, gy * vblocks)
            away = lax.rem(lax.div(a, cores) - lax.div(home, cores) + gx, gx // cores)
            side = lax.rem(a + home, cores)
            place = (side * (gx // cores) + away) * vblocks + lax.rem(col, vblocks)
            masked = jnp.where(pattern < work_ref[tile], tiles[tile], jnp.zeros((), jnp.bfloat16))
            made[t] = jnp.dot(masked, held[place], preferred_element_type=jnp.float32)
            return carry

        lax.fori_loop(0, per_step, form, 0, unroll=True)

        def add(t, carry):
            row = lax.rem(row_ref[i * per_step + t], blocks)
            acc[row] += made[t]
            return carry

        lax.fori_loop(0, per_step, add, 0, unroll=True)

    def own(i, carry):
        own_ref[pl.ds(i * order, order), :] = acc[y * span + i]
        return carry

    for k, q_ref in enumerate(q_refs, 1):
        base = lax.rem(y + k, groups) * span

        def code(i, carry):
            coded(acc[base + i], q_ref, exps, i * order, i)
            return carry

        lax.fori_loop(0, span, code, 0, unroll=2)
        q_ref[pl.ds(span * order, span), :] = exps[...].astype(jnp.int32).astype(jnp.int16)
    lax.fori_loop(0, span, own, 0)


def scales_of(ref, at):
    exps = ref[pl.ds(at, ref.shape[0] - at), :].astype(jnp.int32).astype(jnp.float32)
    return jnp.exp2(exps - 15.0)


def part_of(ref, i, order, count):
    x = ref[pl.ds(i * order, order), :].astype(jnp.int32).astype(jnp.float32)
    return x * scales_of(ref, count * order)[i : i + 1, :]


def store_exps(q_ref, exps, count, order):
    q_ref[pl.ds(count * order, exps.shape[0]), :] = exps[...].astype(jnp.int32).astype(jnp.int16)


def middle_kernel(order, vblocks, own_ref, *refs):
    got, part_ref, q_refs, scales, exps = refs[:-5], refs[-5], refs[-4:-2], refs[-2], refs[-1]
    blocks = part_ref.shape[0] // order
    owners = blocks // vblocks
    z = lax.axis_index("z")
    exps[...] = jnp.zeros_like(exps)
    for n, g in enumerate(got):
        scales[pl.ds(blocks * n, blocks), :] = scales_of(g, blocks * order)

    def add(block, carry):
        at = block * order
        x = own_ref[pl.ds(at, order), :]
        for n, g in enumerate(got):
            part = g[pl.ds(at, order), :].astype(jnp.int32).astype(jnp.float32)
            x = x + part * scales[pl.ds(blocks * n + block, 1), :]
        part_ref[pl.ds(at, order), :] = x
        return carry

    lax.fori_loop(0, blocks, add, 0, unroll=2)
    far = lax.rem(z + owners // 2, owners) * vblocks
    for v, q_ref in enumerate(q_refs):
        coded(part_ref[pl.ds((far + v) * order, order), :], q_ref, exps, 0, 0)
        store_exps(q_ref, exps, 1, order)


def ring_kernel(order, vblocks, away, first, part_ref, right_ref, left_ref, to_right, to_left, exps):
    owners = part_ref.shape[0] // order // vblocks
    z = lax.axis_index("z")
    exps[...] = jnp.zeros_like(exps)
    ways = ((right_ref, to_right, away, 0), (left_ref, to_left, owners - away, 1))
    for got, q_ref, by, side in ways:
        base = lax.rem(z + by, owners) * vblocks
        for v in range(vblocks):
            x = part_ref[pl.ds((base + v) * order, order), :]
            if not first:
                x = x + part_of(got, v, order, vblocks)
            elif v == side:
                x = x + part_of(got, 0, order, 1)
            coded(x, q_ref, exps, v * order, v)
        store_exps(q_ref, exps, vblocks, order)


def last_kernel(order, vblocks, part_ref, right_ref, left_ref, out_ref):
    base = lax.axis_index("z") * vblocks
    for v in range(vblocks):
        x = part_ref[pl.ds((base + v) * order, order), :]
        for got in (right_ref, left_ref):
            x = x + part_of(got, v, order, vblocks)
        out_ref[pl.ds(v * order, order), :] = x


def on_device(features, tile_vals, tile_row, tile_col, tile_work):
    peers = lax.axis_size(GY)
    gx, ny, nz = (lax.axis_size(axis) for axis in GX_GY)
    slots, order, _ = tile_vals.shape
    owned = slots // 2
    width = features.shape[1]
    vblocks = features.shape[0] // order
    blocks = peers * vblocks
    told = pl.pallas_call(
        lambda *refs: tell_kernel(slots, *refs),
        in_specs=[ANY] * 3,
        out_specs=VMEM,
        out_shape=jax.ShapeDtypeStruct((peers, 2, 2 * slots), jnp.int32),
        scratch_shapes=[pltpu.VMEM((3, slots), jnp.int32), pltpu.SemaphoreType.DMA((3,))],
        compiler_params=limit(4),
        name="tell",
    )(*(in_hbm(t) for t in (tile_row, tile_col, tile_work)))

    cores = 2
    mine = [features.reshape(vblocks, order, width)]
    for k in range(1, gx // cores):
        mine.append(lax.ppermute(mine[0], "gx", [(i, (i + cores * k) % gx) for i in range(gx)]))
    meta = lax.all_to_all(told, GY, split_axis=0, concat_axis=0, tiled=True)
    feats = jnp.concatenate(mine)
    swapped = lax.ppermute(feats, "gx", [(i, i ^ 1) for i in range(gx)])
    tiles = pl.pallas_call(
        stage_kernel,
        in_specs=[ANY],
        out_specs=VMEM,
        out_shape=vmem(tile_vals.shape, tile_vals.dtype),
        scratch_shapes=[pltpu.SemaphoreType.DMA((8,))],
        compiler_params=limit(4),
        name="stage",
    )(in_hbm(tile_vals))
    small = jax.ShapeDtypeStruct((owned,), jnp.int32)
    sent, moved_row, moved_col, moved_work, kept = pl.pallas_call(
        lambda *refs: plan_kernel(peers, slots, *refs),
        in_specs=[SMEM, VMEM],
        out_specs=[ANY, SMEM, SMEM, SMEM, SMEM],
        out_shape=[pltpu.HBM(tile_vals.shape, tile_vals.dtype), small, small, small, small],
        scratch_shapes=[pltpu.SemaphoreType.DMA((1,))],
        compiler_params=limit(4),
        name="plan",
    )(meta, in_vmem(tiles))
    got = lax.all_to_all(sent, GY, split_axis=0, concat_axis=0, tiled=True)

    steps = 8
    span = blocks // ny
    i16 = jnp.int16
    own, *coded_y = pl.pallas_call(
        lambda *refs: product_kernel(gx, peers, ny, steps, *refs),
        in_specs=[SMEM] * 3 + [VMEM] * 3,
        out_specs=[VMEM] * ny,
        out_shape=[vmem((span * order, width), jnp.float32)]
        + [vmem((span * order + span, width), i16)] * (ny - 1),
        scratch_shapes=[
            pltpu.VMEM((blocks, order, width), jnp.float32),
            pltpu.VMEM((gx * vblocks, order, width), jnp.bfloat16),
            pltpu.VMEM((slots // steps, order, width), jnp.float32),
            pltpu.VMEM((span, width), jnp.float32),
        ],
        compiler_params=limit(16),
        name="products",
    )(tile_row, tile_col, tile_work, *(in_vmem(f) for f in (tiles, feats, swapped)))
    got_y = []
    for k, q in enumerate(coded_y, 1):
        got_y.append(shifted(q, "y", k))

    def line(count):
        return vmem((count * order + 8, width), i16)

    part, *coded_z = pl.pallas_call(
        lambda *refs: middle_kernel(order, vblocks, *refs),
        in_specs=[VMEM] * ny,
        out_specs=[VMEM] * 3,
        out_shape=[vmem((span * order, width), jnp.float32), line(1), line(1)],
        scratch_shapes=[pltpu.VMEM((span * (ny - 1), width), jnp.float32), pltpu.VMEM((8, width), jnp.float32)],
        compiler_params=limit(8),
        name="middle",
    )(*(in_vmem(g) for g in (own, *got_y)))
    for away in range(nz // 2 - 1, 0, -1):
        ring = [shifted(coded_z[0], "z", 1), shifted(coded_z[1], "z", -1)]
        first = away == nz // 2 - 1
        coded_z = pl.pallas_call(
            lambda *refs: ring_kernel(order, vblocks, away, first, *refs),
            in_specs=[VMEM] * 3,
            out_specs=[VMEM] * 2,
            out_shape=[line(vblocks)] * 2,
            scratch_shapes=[pltpu.VMEM((8, width), jnp.float32)],
            compiler_params=limit(4),
        )(*(in_vmem(g) for g in (part, *ring)))
    ring = [shifted(coded_z[0], "z", 1), shifted(coded_z[1], "z", -1)]
    product = pl.pallas_call(
        lambda *refs: last_kernel(order, vblocks, *refs),
        in_specs=[VMEM] * 3,
        out_specs=VMEM,
        out_shape=jax.ShapeDtypeStruct((vblocks * order, width), jnp.float32),
        compiler_params=limit(4),
        name="last",
    )(*(in_vmem(g) for g in (part, *ring)))

    moved_vals = pl.pallas_call(
        lambda *refs: keep_kernel(owned, *refs),
        in_specs=[SMEM, VMEM],
        out_specs=ANY,
        out_shape=jax.ShapeDtypeStruct((owned, *tile_vals.shape[1:]), tile_vals.dtype),
        scratch_shapes=[pltpu.SemaphoreType.DMA((1,))],
        compiler_params=limit(4),
        name="keep",
    )(kept, in_vmem(got))
    return (product, moved_vals, moved_row, moved_col, moved_work)


def solution(mesh):
    finer = Mesh(mesh.devices.reshape(mesh.shape["gx"], 4, 8), GX_GY)
    in_specs = (P(GX_GY, None), P(GX_GY, None, None), P(GX_GY), P(GX_GY), P(GX_GY))

    return jax.shard_map(on_device, mesh=finer, in_specs=in_specs, out_specs=in_specs, check_vma=False)
```

```python
import jax
import jax.numpy as jnp
from jax import lax
from jax.experimental import pallas as pl
from jax.experimental.pallas import tpu as pltpu
from jax.sharding import Mesh
from jax.sharding import PartitionSpec as P

GY = ("y", "z")
GX_GY = ("gx", "y", "z")

ANY = pl.BlockSpec(memory_space=pl.ANY)
SMEM = pl.BlockSpec(memory_space=pltpu.SMEM)
VMEM = pl.BlockSpec(memory_space=pltpu.VMEM)


def in_vmem(array):
    return pltpu.with_memory_space_constraint(array, pltpu.VMEM)


def in_hbm(array):
    return pltpu.with_memory_space_constraint(array, pltpu.HBM)


def vmem(shape, dtype):
    return pltpu.VMEM(shape, dtype)


def limit(mib):
    return pltpu.CompilerParams(vmem_limit_bytes=mib * 2**20)


def shifted(array, axis, by):
    size = lax.axis_size(axis)
    return lax.ppermute(array, axis, [(i, (i + by) % size) for i in range(size)])


def tell_kernel(slots, row_ref, col_ref, work_ref, out_ref, held, sems):
    copies = [
        pltpu.make_async_copy(ref, held.at[i], sems.at[i]) for i, ref in enumerate((row_ref, col_ref, work_ref))
    ]
    for c in copies:
        c.start()
    for c in copies:
        c.wait()
    row, col, work = (held[i].reshape(1, slots) for i in range(3))
    count = jnp.sum((work > 0).astype(jnp.int32), axis=1, keepdims=True)
    for i, pair in enumerate(((row, col), (work, jnp.broadcast_to(count, (1, slots))))):
        line = jnp.concatenate(pair, axis=1)
        out_ref[:, i, :] = jnp.broadcast_to(line, (out_ref.shape[0], 2 * slots))


def stage_kernel(vals_ref, out_ref, sems):
    groups = sems.shape[0]
    size = vals_ref.shape[0] // groups
    copies = [
        pltpu.make_async_copy(
            vals_ref.at[pl.ds(g * size, size)], out_ref.at[pl.ds(g * size, size)], sems.at[g]
        )
        for g in range(groups)
    ]
    for c in copies:
        c.start()
    for c in copies:
        c.wait()


def place_of():
    return lax.axis_index("y") * lax.axis_size("z") + lax.axis_index("z")


def plan_kernel(peers, slots, meta_ref, vals_ref, sent_ref, sems):
    me = place_of()
    share = slots // peers

    def before(s, total):
        return total + jnp.where(s < me, meta_ref[s, 1, slots], 0)

    first = lax.fori_loop(0, peers, before, jnp.int32(0), unroll=8)
    turn = lax.rem(first, peers)

    def start(d, carry):
        at = lax.rem(d - turn + peers, peers)
        for w in range(share):
            pltpu.make_async_copy(
                vals_ref.at[at + w * peers], sent_ref.at[d * share + w], sems.at[0]
            ).start()
        return carry

    lax.fori_loop(0, peers, start, 0, unroll=8)
    pltpu.make_async_copy(vals_ref, sent_ref, sems.at[0]).wait()


def list_kernel(peers, slots, meta_ref, row_ref, col_ref, work_ref, slot_ref):
    me = place_of()
    share = slots // peers

    def source(s, begin):
        count = meta_ref[s, 1, slots]
        j = lax.rem(me - lax.rem(begin, peers) + peers, peers)
        for w in range(share):
            at = j + w * peers

            @pl.when(at < count)
            def _():
                k = lax.div(begin + at, peers)
                row_ref[k] = meta_ref[s, 0, at]
                col_ref[k] = meta_ref[s, 0, slots + at]
                work_ref[k] = meta_ref[s, 1, at]
                slot_ref[k] = s * share + w

        return begin + count

    lax.fori_loop(0, peers, source, jnp.int32(0))


def keep_kernel(owned, slot_ref, got_ref, out_ref, sems):
    def start(k, carry):
        pltpu.make_async_copy(got_ref.at[slot_ref[k]], out_ref.at[k], sems.at[0]).start()
        return carry

    lax.fori_loop(0, owned, start, 0)
    pltpu.make_async_copy(got_ref.at[pl.ds(0, owned)], out_ref, sems.at[0]).wait()


def coded(x, q_ref, exps_ref, at, row):
    top = jnp.maximum(jnp.max(jnp.abs(x), axis=0, keepdims=True), 1e-30)
    exponent = jnp.ceil(jnp.log2(top))
    scaled = jnp.round(x * jnp.exp2(15.0 - exponent))
    scaled = jnp.minimum(jnp.maximum(scaled, -32767.0), 32767.0)
    q_ref[pl.ds(at, x.shape[0]), :] = scaled.astype(jnp.int32).astype(jnp.int16)
    exps_ref[pl.ds(row, 1), :] = exponent


def product_kernel(gx, gy, groups, steps, row_ref, col_ref, work_ref, tiles, feats_ref, swap_ref, *refs):
    own_ref, rest_ref, right_ref, left_ref, acc, held, made, exps, sems = refs
    slots, order, _ = tiles.shape
    per_step = slots // steps
    vblocks = held.shape[0] // gx
    blocks = acc.shape[0]
    span = blocks // groups
    a, y = lax.axis_index("gx"), lax.axis_index("y")
    cores = 2

    acc[...] = jnp.zeros_like(acc)
    for k, f in enumerate((feats_ref, swap_ref)):
        held[pl.ds(k * f.shape[0], f.shape[0])] = f[...]

    pattern = lax.broadcasted_iota(jnp.int32, (order, order), 0) * order + lax.broadcasted_iota(
        jnp.int32, (order, order), 1
    )
    for i in range(steps):

        def form(t, carry):
            tile = i * per_step + t
            col = col_ref[tile]
            home = lax.div(col, gy * vblocks)
            away = lax.rem(lax.div(a, cores) - lax.div(home, cores) + gx, gx // cores)
            side = lax.rem(a + home, cores)
            place = (side * (gx // cores) + away) * vblocks + lax.rem(col, vblocks)
            masked = jnp.where(pattern < work_ref[tile], tiles[tile], jnp.zeros((), jnp.bfloat16))
            made[t] = jnp.dot(masked, held[place], preferred_element_type=jnp.float32)
            return carry

        lax.fori_loop(0, per_step, form, 0, unroll=True)

        def add(t, carry):
            row = lax.rem(row_ref[i * per_step + t], blocks)
            acc[row] += made[t]
            return carry

        lax.fori_loop(0, per_step, add, 0, unroll=True)

    half = span // 2
    there, behind = (lax.rem(y + k, groups) * span for k in (1, groups - 1))
    far = lax.rem(y + groups // 2, groups) * span
    leaving = [
        pltpu.make_async_copy(acc.at[pl.ds(at, n)], ref, sems.at[i])
        for i, (at, n, ref) in enumerate(
            (
                (y * span, span, own_ref),
                (there, half, rest_ref.at[pl.ds(0, half)]),
                (behind + half, half, rest_ref.at[pl.ds(half, half)]),
            )
        )
    ]
    for c in leaving:
        c.start()
    for q_ref, starts in ((right_ref, (far, there + half)), (left_ref, (far + half, behind))):
        for n, base in enumerate(starts):

            def code(i, carry):
                coded(acc[base + i], q_ref, exps, (n * half + i) * order, n * half + i)
                return carry

            lax.fori_loop(0, half, code, 0, unroll=2)
        store_exps(q_ref, exps, span, order)
    for c in leaving:
        c.wait()


def scales_of(ref, at):
    exps = ref[pl.ds(at, ref.shape[0] - at), :].astype(jnp.int32).astype(jnp.float32)
    return jnp.exp2(exps - 15.0)


def part_of(ref, i, order, count):
    x = ref[pl.ds(i * order, order), :].astype(jnp.int32).astype(jnp.float32)
    return x * scales_of(ref, count * order)[i : i + 1, :]


def store_exps(q_ref, exps, count, order):
    q_ref[pl.ds(count * order, exps.shape[0]), :] = exps[...].astype(jnp.int32).astype(jnp.int16)


def relay_kernel(order, rest_ref, low_ref, high_ref, right_ref, left_ref, scales, exps):
    span = rest_ref.shape[0]
    half = span // 2
    for side, (got, q_ref) in enumerate(((low_ref, right_ref), (high_ref, left_ref))):
        scales[...] = scales_of(got, span * order)

        def add(i, carry):
            part = got[pl.ds(i * order, order), :].astype(jnp.int32).astype(jnp.float32)
            x = rest_ref[side * half + i] + part * scales[pl.ds(i, 1), :]
            coded(x, q_ref, exps, i * order, i)
            return carry

        lax.fori_loop(0, half, add, 0, unroll=2)
        store_exps(q_ref, exps, half, order)


def middle_kernel(order, vblocks, own_ref, low_ref, high_ref, low2_ref, high2_ref, out_ref, *refs):
    q_refs, (total, scales, exps) = refs[:-3], refs[-3:]
    span = own_ref.shape[0]
    half = span // 2
    owners = span // vblocks
    z = lax.axis_index("z")
    exps[...] = jnp.zeros_like(exps)
    scales[pl.ds(0, half), :] = scales_of(high_ref, span * order)[half:, :]
    scales[pl.ds(half, half), :] = scales_of(low_ref, span * order)[half:, :]
    scales[pl.ds(span, half), :] = scales_of(low2_ref, half * order)
    scales[pl.ds(span + half, half), :] = scales_of(high2_ref, half * order)

    def part(ref, at, scale):
        x = ref[pl.ds(at * order, order), :].astype(jnp.int32).astype(jnp.float32)
        return x * scales[pl.ds(scale, 1), :]

    for side, (near, last) in enumerate(((high_ref, low2_ref), (low_ref, high2_ref))):

        def add(i, carry):
            at = side * half + i
            total[at] = own_ref[at] + part(near, half + i, at) + part(last, i, span + at)
            return carry

        lax.fori_loop(0, half, add, 0, unroll=2)
    for v in range(vblocks):
        out_ref[pl.ds(v * order, order), :] = total[z * vblocks + v]
    for k, q_ref in enumerate(q_refs, 1):
        base = lax.rem(z + k, owners) * vblocks
        for v in range(vblocks):
            coded(total[base + v], q_ref, exps, v * order, v)
        store_exps(q_ref, exps, vblocks, order)


def last_kernel(order, vblocks, own_ref, *refs):
    got, out_ref = refs[:-1], refs[-1]
    for v in range(vblocks):
        x = own_ref[pl.ds(v * order, order), :]
        for g in got:
            x = x + part_of(g, v, order, vblocks)
        out_ref[pl.ds(v * order, order), :] = x


def on_device(features, tile_vals, tile_row, tile_col, tile_work):
    peers = lax.axis_size(GY)
    gx, ny, nz = (lax.axis_size(axis) for axis in GX_GY)
    slots, order, _ = tile_vals.shape
    owned = slots // 2
    width = features.shape[1]
    vblocks = features.shape[0] // order
    blocks = peers * vblocks
    told = pl.pallas_call(
        lambda *refs: tell_kernel(slots, *refs),
        in_specs=[ANY] * 3,
        out_specs=VMEM,
        out_shape=jax.ShapeDtypeStruct((peers, 2, 2 * slots), jnp.int32),
        scratch_shapes=[pltpu.VMEM((3, slots), jnp.int32), pltpu.SemaphoreType.DMA((3,))],
        compiler_params=limit(4),
        name="tell",
    )(*(in_hbm(t) for t in (tile_row, tile_col, tile_work)))

    cores = 2
    mine = [features.reshape(vblocks, order, width)]
    for k in range(1, gx // cores):
        mine.append(lax.ppermute(mine[0], "gx", [(i, (i + cores * k) % gx) for i in range(gx)]))
    meta = lax.all_to_all(told, GY, split_axis=0, concat_axis=0, tiled=True)
    feats = jnp.concatenate(mine)
    swapped = lax.ppermute(feats, "gx", [(i, i ^ 1) for i in range(gx)])
    tiles = pl.pallas_call(
        stage_kernel,
        in_specs=[ANY],
        out_specs=VMEM,
        out_shape=vmem(tile_vals.shape, tile_vals.dtype),
        scratch_shapes=[pltpu.SemaphoreType.DMA((8,))],
        compiler_params=limit(4),
        name="stage",
    )(in_hbm(tile_vals))
    small = jax.ShapeDtypeStruct((owned,), jnp.int32)
    sent = pl.pallas_call(
        lambda *refs: plan_kernel(peers, slots, *refs),
        in_specs=[SMEM, VMEM],
        out_specs=ANY,
        out_shape=pltpu.HBM(tile_vals.shape, tile_vals.dtype),
        scratch_shapes=[pltpu.SemaphoreType.DMA((1,))],
        compiler_params=limit(4),
        name="plan",
    )(meta, in_vmem(tiles))
    moved_row, moved_col, moved_work, kept = pl.pallas_call(
        lambda *refs: list_kernel(peers, slots, *refs),
        in_specs=[SMEM],
        out_specs=[SMEM] * 4,
        out_shape=[small] * 4,
        compiler_params=limit(4),
        name="list",
    )(meta)
    got = lax.all_to_all(sent, GY, split_axis=0, concat_axis=0, tiled=True)

    steps = 8
    span = blocks // ny
    i16 = jnp.int16

    def line(count, more=8):
        return vmem((count * order + more, width), i16)

    f32_blocks = pltpu.HBM((span, order, width), jnp.float32)
    own, rest, right, left = pl.pallas_call(
        lambda *refs: product_kernel(gx, peers, ny, steps, *refs),
        in_specs=[SMEM] * 3 + [VMEM] * 3,
        out_specs=[ANY, ANY, VMEM, VMEM],
        out_shape=[f32_blocks, f32_blocks, line(span, span), line(span, span)],
        scratch_shapes=[
            pltpu.VMEM((blocks, order, width), jnp.float32),
            pltpu.VMEM((gx * vblocks, order, width), jnp.bfloat16),
            pltpu.VMEM((slots // steps, order, width), jnp.float32),
            pltpu.VMEM((span, width), jnp.float32),
            pltpu.SemaphoreType.DMA((3,)),
        ],
        compiler_params=limit(16),
        name="products",
    )(tile_row, tile_col, tile_work, *(in_vmem(f) for f in (tiles, feats, swapped)))
    low = shifted(right, "y", 1)
    high = shifted(left, "y", -1)
    right, left = pl.pallas_call(
        lambda *refs: relay_kernel(order, *refs),
        in_specs=[VMEM] * 3,
        out_specs=[VMEM] * 2,
        out_shape=[line(span // 2)] * 2,
        scratch_shapes=[pltpu.VMEM((span, width), jnp.float32), pltpu.VMEM((span // 2, width), jnp.float32)],
        compiler_params=limit(8),
        name="relay",
    )(rest, low, high)
    low2, high2 = shifted(right, "y", 1), shifted(left, "y", -1)
    own_z, *coded_z = pl.pallas_call(
        lambda *refs: middle_kernel(order, vblocks, *refs),
        in_specs=[VMEM] * 5,
        out_specs=[VMEM] * nz,
        out_shape=[vmem((vblocks * order, width), jnp.float32)] + [line(vblocks)] * (nz - 1),
        scratch_shapes=[
            pltpu.VMEM((span, order, width), jnp.float32),
            pltpu.VMEM((2 * span, width), jnp.float32),
            pltpu.VMEM((8, width), jnp.float32),
        ],
        compiler_params=limit(12),
        name="middle",
    )(own, low, high, low2, high2)
    got_z = [shifted(q, "z", k) for k, q in enumerate(coded_z, 1)]
    product = pl.pallas_call(
        lambda *refs: last_kernel(order, vblocks, *refs),
        in_specs=[VMEM] * nz,
        out_specs=VMEM,
        out_shape=jax.ShapeDtypeStruct((vblocks * order, width), jnp.float32),
        compiler_params=limit(4),
        name="last",
    )(*(in_vmem(g) for g in (own_z, *got_z)))

    moved_vals = pl.pallas_call(
        lambda *refs: keep_kernel(owned, *refs),
        in_specs=[SMEM, VMEM],
        out_specs=ANY,
        out_shape=jax.ShapeDtypeStruct((owned, *tile_vals.shape[1:]), tile_vals.dtype),
        scratch_shapes=[pltpu.SemaphoreType.DMA((1,))],
        compiler_params=limit(4),
        name="keep",
    )(kept, in_vmem(got))
    return (product, moved_vals, moved_row, moved_col, moved_work)


def solution(mesh):
    finer = Mesh(mesh.devices.reshape(mesh.shape["gx"], 4, 8), GX_GY)
    in_specs = (P(GX_GY, None), P(GX_GY, None, None), P(GX_GY), P(GX_GY), P(GX_GY))

    return jax.shard_map(on_device, mesh=finer, in_specs=in_specs, out_specs=in_specs, check_vma=False)
```

```python
import jax
import jax.numpy as jnp
from jax import lax
from jax.experimental import pallas as pl
from jax.experimental.pallas import tpu as pltpu
from jax.sharding import Mesh
from jax.sharding import PartitionSpec as P

GY = ("y", "z")
GX_GY = ("gx", "y", "z")

ANY = pl.BlockSpec(memory_space=pl.ANY)
SMEM = pl.BlockSpec(memory_space=pltpu.SMEM)
VMEM = pl.BlockSpec(memory_space=pltpu.VMEM)


def in_vmem(array):
    return pltpu.with_memory_space_constraint(array, pltpu.VMEM)


def in_hbm(array):
    return pltpu.with_memory_space_constraint(array, pltpu.HBM)


def vmem(shape, dtype):
    return pltpu.VMEM(shape, dtype)


def limit(mib):
    return pltpu.CompilerParams(vmem_limit_bytes=mib * 2**20)


def shifted(array, axis, by):
    size = lax.axis_size(axis)
    return lax.ppermute(array, axis, [(i, (i + by) % size) for i in range(size)])


def tell_kernel(slots, row_ref, col_ref, work_ref, out_ref, held, sems):
    copies = [
        pltpu.make_async_copy(ref, held.at[i], sems.at[i]) for i, ref in enumerate((row_ref, col_ref, work_ref))
    ]
    for c in copies:
        c.start()
    for c in copies:
        c.wait()
    row, col, work = (held[i].reshape(1, slots) for i in range(3))
    count = jnp.sum((work > 0).astype(jnp.int32), axis=1, keepdims=True)
    for i, pair in enumerate(((row, col), (work, jnp.broadcast_to(count, (1, slots))))):
        line = jnp.concatenate(pair, axis=1)
        out_ref[:, i, :] = jnp.broadcast_to(line, (out_ref.shape[0], 2 * slots))


def stage_kernel(vals_ref, out_ref, sems):
    groups = sems.shape[0]
    size = vals_ref.shape[0] // groups
    copies = [
        pltpu.make_async_copy(
            vals_ref.at[pl.ds(g * size, size)], out_ref.at[pl.ds(g * size, size)], sems.at[g]
        )
        for g in range(groups)
    ]
    for c in copies:
        c.start()
    for c in copies:
        c.wait()


def place_of():
    return lax.axis_index("y") * lax.axis_size("z") + lax.axis_index("z")


def plan_kernel(peers, slots, meta_ref, vals_ref, sent_ref, sems):
    me = place_of()
    share = slots // peers

    def before(s, total):
        return total + jnp.where(s < me, meta_ref[s, 1, slots], 0)

    first = lax.fori_loop(0, peers, before, jnp.int32(0), unroll=8)
    turn = lax.rem(first, peers)

    def start(d, carry):
        at = lax.rem(d - turn + peers, peers)
        for w in range(share):
            pltpu.make_async_copy(
                vals_ref.at[at + w * peers], sent_ref.at[d * share + w], sems.at[0]
            ).start()
        return carry

    lax.fori_loop(0, peers, start, 0, unroll=8)
    pltpu.make_async_copy(vals_ref, sent_ref, sems.at[0]).wait()


def list_kernel(peers, slots, meta_ref, row_ref, col_ref, work_ref, slot_ref):
    me = place_of()
    share = slots // peers

    def source(s, begin):
        count = meta_ref[s, 1, slots]
        j = lax.rem(me - lax.rem(begin, peers) + peers, peers)
        for w in range(share):
            at = j + w * peers

            @pl.when(at < count)
            def _():
                k = lax.div(begin + at, peers)
                row_ref[k] = meta_ref[s, 0, at]
                col_ref[k] = meta_ref[s, 0, slots + at]
                work_ref[k] = meta_ref[s, 1, at]
                slot_ref[k] = s * share + w

        return begin + count

    lax.fori_loop(0, peers, source, jnp.int32(0))


def keep_kernel(owned, slot_ref, got_ref, out_ref, held, sems, out_sems):
    groups = sems.shape[0]
    size = owned // groups

    def piece(ref, g):
        return ref.at[pl.ds(g * size, size)]

    for k in range(owned):
        pltpu.make_async_copy(got_ref.at[slot_ref[k]], held.at[k], sems.at[k // size]).start()
    leaving = [
        pltpu.make_async_copy(piece(held, g), piece(out_ref, g), out_sems.at[g]) for g in range(groups)
    ]
    for g, c in enumerate(leaving):
        pltpu.make_async_copy(piece(got_ref, g), piece(held, g), sems.at[g]).wait()
        c.start()
    for c in leaving:
        c.wait()


def coded(x, q_ref, exps_ref, at, row):
    top = jnp.maximum(jnp.max(jnp.abs(x), axis=0, keepdims=True), 1e-30)
    exponent = jnp.ceil(jnp.log2(top))
    scaled = jnp.round(x * jnp.exp2(15.0 - exponent))
    scaled = jnp.minimum(jnp.maximum(scaled, -32767.0), 32767.0)
    q_ref[pl.ds(at, x.shape[0]), :] = scaled.astype(jnp.int32).astype(jnp.int16)
    exps_ref[pl.ds(row, 1), :] = exponent


def product_kernel(gx, gy, groups, steps, row_ref, col_ref, work_ref, tiles, feats_ref, swap_ref, *refs):
    own_ref, rest_ref, right_ref, left_ref, acc, held, made, exps, sems = refs
    slots, order, _ = tiles.shape
    per_step = slots // steps
    vblocks = held.shape[0] // gx
    blocks = acc.shape[0]
    span = blocks // groups
    a, y = lax.axis_index("gx"), lax.axis_index("y")
    cores = 2

    acc[...] = jnp.zeros_like(acc)
    for k, f in enumerate((feats_ref, swap_ref)):
        held[pl.ds(k * f.shape[0], f.shape[0])] = f[...]

    pattern = lax.broadcasted_iota(jnp.int32, (order, order), 0) * order + lax.broadcasted_iota(
        jnp.int32, (order, order), 1
    )
    for i in range(steps):

        def form(t, carry):
            tile = i * per_step + t
            col = col_ref[tile]
            home = lax.div(col, gy * vblocks)
            away = lax.rem(lax.div(a, cores) - lax.div(home, cores) + gx, gx // cores)
            side = lax.rem(a + home, cores)
            place = (side * (gx // cores) + away) * vblocks + lax.rem(col, vblocks)
            masked = jnp.where(pattern < work_ref[tile], tiles[tile], jnp.zeros((), jnp.bfloat16))
            made[t] = jnp.dot(masked, held[place], preferred_element_type=jnp.float32)
            return carry

        lax.fori_loop(0, per_step, form, 0, unroll=True)

        def add(t, carry):
            row = lax.rem(row_ref[i * per_step + t], blocks)
            acc[row] += made[t]
            return carry

        lax.fori_loop(0, per_step, add, 0, unroll=True)

    half = span // 2
    there, behind = (lax.rem(y + k, groups) * span for k in (1, groups - 1))
    far = lax.rem(y + groups // 2, groups) * span
    leaving = [
        pltpu.make_async_copy(acc.at[pl.ds(at, n)], ref, sems.at[i])
        for i, (at, n, ref) in enumerate(
            (
                (y * span, span, own_ref),
                (there, half, rest_ref.at[pl.ds(0, half)]),
                (behind + half, half, rest_ref.at[pl.ds(half, half)]),
            )
        )
    ]
    for c in leaving:
        c.start()
    for q_ref, starts in ((right_ref, (far, there + half)), (left_ref, (far + half, behind))):
        for n, base in enumerate(starts):

            def code(i, carry):
                coded(acc[base + i], q_ref, exps, (n * half + i) * order, n * half + i)
                return carry

            lax.fori_loop(0, half, code, 0, unroll=2)
        store_exps(q_ref, exps, span, order)
    for c in leaving:
        c.wait()


def scales_of(ref, at):
    exps = ref[pl.ds(at, ref.shape[0] - at), :].astype(jnp.int32).astype(jnp.float32)
    return jnp.exp2(exps - 15.0)


def part_of(ref, i, order, count):
    x = ref[pl.ds(i * order, order), :].astype(jnp.int32).astype(jnp.float32)
    return x * scales_of(ref, count * order)[i : i + 1, :]


def store_exps(q_ref, exps, count, order):
    q_ref[pl.ds(count * order, exps.shape[0]), :] = exps[...].astype(jnp.int32).astype(jnp.int16)


def relay_kernel(order, rest_ref, low_ref, high_ref, right_ref, left_ref, scales, exps):
    span = rest_ref.shape[0]
    half = span // 2
    for side, (got, q_ref) in enumerate(((low_ref, right_ref), (high_ref, left_ref))):
        scales[...] = scales_of(got, span * order)

        def add(i, carry):
            part = got[pl.ds(i * order, order), :].astype(jnp.int32).astype(jnp.float32)
            x = rest_ref[side * half + i] + part * scales[pl.ds(i, 1), :]
            coded(x, q_ref, exps, i * order, i)
            return carry

        lax.fori_loop(0, half, add, 0, unroll=2)
        store_exps(q_ref, exps, half, order)


def middle_kernel(order, vblocks, own_ref, low_ref, high_ref, low2_ref, high2_ref, out_ref, *refs):
    q_refs, (total, scales, exps) = refs[:-3], refs[-3:]
    span = own_ref.shape[0]
    half = span // 2
    owners = span // vblocks
    z = lax.axis_index("z")
    exps[...] = jnp.zeros_like(exps)
    scales[pl.ds(0, half), :] = scales_of(high_ref, span * order)[half:, :]
    scales[pl.ds(half, half), :] = scales_of(low_ref, span * order)[half:, :]
    scales[pl.ds(span, half), :] = scales_of(low2_ref, half * order)
    scales[pl.ds(span + half, half), :] = scales_of(high2_ref, half * order)

    def part(ref, at, scale):
        x = ref[pl.ds(at * order, order), :].astype(jnp.int32).astype(jnp.float32)
        return x * scales[pl.ds(scale, 1), :]

    for side, (near, last) in enumerate(((high_ref, low2_ref), (low_ref, high2_ref))):

        def add(i, carry):
            at = side * half + i
            total[at] = own_ref[at] + part(near, half + i, at) + part(last, i, span + at)
            return carry

        lax.fori_loop(0, half, add, 0, unroll=2)
    for v in range(vblocks):
        out_ref[pl.ds(v * order, order), :] = total[z * vblocks + v]
    for k, q_ref in enumerate(q_refs, 1):
        base = lax.rem(z + k, owners) * vblocks
        for v in range(vblocks):
            coded(total[base + v], q_ref, exps, v * order, v)
        store_exps(q_ref, exps, vblocks, order)


def last_kernel(order, vblocks, own_ref, *refs):
    got, out_ref = refs[:-1], refs[-1]
    for v in range(vblocks):
        x = own_ref[pl.ds(v * order, order), :]
        for g in got:
            x = x + part_of(g, v, order, vblocks)
        out_ref[pl.ds(v * order, order), :] = x


def on_device(features, tile_vals, tile_row, tile_col, tile_work):
    peers = lax.axis_size(GY)
    gx, ny, nz = (lax.axis_size(axis) for axis in GX_GY)
    slots, order, _ = tile_vals.shape
    owned = slots // 2
    width = features.shape[1]
    vblocks = features.shape[0] // order
    blocks = peers * vblocks
    told = pl.pallas_call(
        lambda *refs: tell_kernel(slots, *refs),
        in_specs=[ANY] * 3,
        out_specs=VMEM,
        out_shape=jax.ShapeDtypeStruct((peers, 2, 2 * slots), jnp.int32),
        scratch_shapes=[pltpu.VMEM((3, slots), jnp.int32), pltpu.SemaphoreType.DMA((3,))],
        compiler_params=limit(4),
        name="tell",
    )(*(in_hbm(t) for t in (tile_row, tile_col, tile_work)))

    cores = 2
    mine = [features.reshape(vblocks, order, width)]
    for k in range(1, gx // cores):
        mine.append(lax.ppermute(mine[0], "gx", [(i, (i + cores * k) % gx) for i in range(gx)]))
    meta = lax.all_to_all(told, GY, split_axis=0, concat_axis=0, tiled=True)
    feats = jnp.concatenate(mine)
    swapped = lax.ppermute(feats, "gx", [(i, i ^ 1) for i in range(gx)])
    tiles = pl.pallas_call(
        stage_kernel,
        in_specs=[ANY],
        out_specs=VMEM,
        out_shape=vmem(tile_vals.shape, tile_vals.dtype),
        scratch_shapes=[pltpu.SemaphoreType.DMA((8,))],
        compiler_params=limit(4),
        name="stage",
    )(in_hbm(tile_vals))
    small = jax.ShapeDtypeStruct((owned,), jnp.int32)
    sent = pl.pallas_call(
        lambda *refs: plan_kernel(peers, slots, *refs),
        in_specs=[SMEM, VMEM],
        out_specs=ANY,
        out_shape=pltpu.HBM(tile_vals.shape, tile_vals.dtype),
        scratch_shapes=[pltpu.SemaphoreType.DMA((1,))],
        compiler_params=limit(4),
        name="plan",
    )(meta, in_vmem(tiles))
    moved_row, moved_col, moved_work, kept = pl.pallas_call(
        lambda *refs: list_kernel(peers, slots, *refs),
        in_specs=[SMEM],
        out_specs=[SMEM] * 4,
        out_shape=[small] * 4,
        compiler_params=limit(4),
        name="list",
    )(meta)
    got = lax.all_to_all(sent, GY, split_axis=0, concat_axis=0, tiled=True)

    steps = 8
    span = blocks // ny
    i16 = jnp.int16

    def line(count, more=8):
        return vmem((count * order + more, width), i16)

    f32_blocks = pltpu.HBM((span, order, width), jnp.float32)
    own, rest, right, left = pl.pallas_call(
        lambda *refs: product_kernel(gx, peers, ny, steps, *refs),
        in_specs=[SMEM] * 3 + [VMEM] * 3,
        out_specs=[ANY, ANY, VMEM, VMEM],
        out_shape=[f32_blocks, f32_blocks, line(span, span), line(span, span)],
        scratch_shapes=[
            pltpu.VMEM((blocks, order, width), jnp.float32),
            pltpu.VMEM((gx * vblocks, order, width), jnp.bfloat16),
            pltpu.VMEM((slots // steps, order, width), jnp.float32),
            pltpu.VMEM((span, width), jnp.float32),
            pltpu.SemaphoreType.DMA((3,)),
        ],
        compiler_params=limit(16),
        name="products",
    )(tile_row, tile_col, tile_work, *(in_vmem(f) for f in (tiles, feats, swapped)))
    low = shifted(right, "y", 1)
    high = shifted(left, "y", -1)
    right, left = pl.pallas_call(
        lambda *refs: relay_kernel(order, *refs),
        in_specs=[VMEM] * 3,
        out_specs=[VMEM] * 2,
        out_shape=[line(span // 2)] * 2,
        scratch_shapes=[pltpu.VMEM((span, width), jnp.float32), pltpu.VMEM((span // 2, width), jnp.float32)],
        compiler_params=limit(8),
        name="relay",
    )(rest, low, high)
    low2, high2 = shifted(right, "y", 1), shifted(left, "y", -1)
    own_z, *coded_z = pl.pallas_call(
        lambda *refs: middle_kernel(order, vblocks, *refs),
        in_specs=[VMEM] * 5,
        out_specs=[VMEM] * nz,
        out_shape=[vmem((vblocks * order, width), jnp.float32)] + [line(vblocks)] * (nz - 1),
        scratch_shapes=[
            pltpu.VMEM((span, order, width), jnp.float32),
            pltpu.VMEM((2 * span, width), jnp.float32),
            pltpu.VMEM((8, width), jnp.float32),
        ],
        compiler_params=limit(12),
        name="middle",
    )(own, low, high, low2, high2)
    got_z = [shifted(q, "z", k) for k, q in enumerate(coded_z, 1)]
    product = pl.pallas_call(
        lambda *refs: last_kernel(order, vblocks, *refs),
        in_specs=[VMEM] * nz,
        out_specs=VMEM,
        out_shape=jax.ShapeDtypeStruct((vblocks * order, width), jnp.float32),
        compiler_params=limit(4),
        name="last",
    )(*(in_vmem(g) for g in (own_z, *got_z)))

    moved_vals = pl.pallas_call(
        lambda *refs: keep_kernel(owned, *refs),
        in_specs=[SMEM, ANY],
        out_specs=ANY,
        out_shape=jax.ShapeDtypeStruct((owned, *tile_vals.shape[1:]), tile_vals.dtype),
        scratch_shapes=[
            pltpu.VMEM((owned, *tile_vals.shape[1:]), tile_vals.dtype),
            pltpu.SemaphoreType.DMA((4,)),
            pltpu.SemaphoreType.DMA((4,)),
        ],
        compiler_params=limit(4),
        name="keep",
    )(kept, in_hbm(got))
    return (product, moved_vals, moved_row, moved_col, moved_work)


def solution(mesh):
    finer = Mesh(mesh.devices.reshape(mesh.shape["gx"], 4, 8), GX_GY)
    in_specs = (P(GX_GY, None), P(GX_GY, None, None), P(GX_GY), P(GX_GY), P(GX_GY))

    return jax.shard_map(on_device, mesh=finer, in_specs=in_specs, out_specs=in_specs, check_vma=False)
```

```python
import jax
import jax.numpy as jnp
from jax import lax
from jax.experimental import pallas as pl
from jax.experimental.pallas import tpu as pltpu
from jax.sharding import Mesh
from jax.sharding import PartitionSpec as P

GY = ("y", "z")
GX_GY = ("gx", "y", "z")

ANY = pl.BlockSpec(memory_space=pl.ANY)
SMEM = pl.BlockSpec(memory_space=pltpu.SMEM)
VMEM = pl.BlockSpec(memory_space=pltpu.VMEM)


def in_vmem(array):
    return pltpu.with_memory_space_constraint(array, pltpu.VMEM)


def in_hbm(array):
    return pltpu.with_memory_space_constraint(array, pltpu.HBM)


def vmem(shape, dtype):
    return pltpu.VMEM(shape, dtype)


def limit(mib):
    return pltpu.CompilerParams(vmem_limit_bytes=mib * 2**20)


def shifted(array, axis, by):
    size = lax.axis_size(axis)
    return lax.ppermute(array, axis, [(i, (i + by) % size) for i in range(size)])


def tell_kernel(slots, row_ref, col_ref, work_ref, out_ref, held, sems):
    copies = [
        pltpu.make_async_copy(ref, held.at[i], sems.at[i]) for i, ref in enumerate((row_ref, col_ref, work_ref))
    ]
    for c in copies:
        c.start()
    for c in copies:
        c.wait()
    row, col, work = (held[i].reshape(1, slots) for i in range(3))
    count = jnp.sum((work > 0).astype(jnp.int32), axis=1, keepdims=True)
    for i, pair in enumerate(((row, col), (work, jnp.broadcast_to(count, (1, slots))))):
        line = jnp.concatenate(pair, axis=1)
        out_ref[:, i, :] = jnp.broadcast_to(line, (out_ref.shape[0], 2 * slots))


def stage_kernel(vals_ref, out_ref, sems):
    groups = sems.shape[0]
    size = vals_ref.shape[0] // groups
    copies = [
        pltpu.make_async_copy(
            vals_ref.at[pl.ds(g * size, size)], out_ref.at[pl.ds(g * size, size)], sems.at[g]
        )
        for g in range(groups)
    ]
    for c in copies:
        c.start()
    for c in copies:
        c.wait()


def place_of():
    return lax.axis_index("y") * lax.axis_size("z") + lax.axis_index("z")


def plan_kernel(peers, slots, meta_ref, vals_ref, sent_ref, sems):
    me = place_of()
    share = slots // peers

    def before(s, total):
        return total + jnp.where(s < me, meta_ref[s, 1, slots], 0)

    first = lax.fori_loop(0, peers, before, jnp.int32(0), unroll=8)
    turn = lax.rem(first, peers)

    def start(d, carry):
        at = lax.rem(d - turn + peers, peers)
        for w in range(share):
            pltpu.make_async_copy(
                vals_ref.at[at + w * peers], sent_ref.at[d * share + w], sems.at[0]
            ).start()
        return carry

    lax.fori_loop(0, peers, start, 0, unroll=8)
    pltpu.make_async_copy(vals_ref, sent_ref, sems.at[0]).wait()


def list_kernel(peers, slots, meta_ref, row_ref, col_ref, work_ref, slot_ref):
    me = place_of()
    share = slots // peers

    def source(s, begin):
        count = meta_ref[s, 1, slots]
        j = lax.rem(me - lax.rem(begin, peers) + peers, peers)
        for w in range(share):
            at = j + w * peers

            @pl.when(at < count)
            def _():
                k = lax.div(begin + at, peers)
                row_ref[k] = meta_ref[s, 0, at]
                col_ref[k] = meta_ref[s, 0, slots + at]
                work_ref[k] = meta_ref[s, 1, at]
                slot_ref[k] = s * share + w

        return begin + count

    lax.fori_loop(0, peers, source, jnp.int32(0))


def keep_kernel(owned, slot_ref, got_ref, out_ref, sems):
    def start(k, carry):
        pltpu.make_async_copy(got_ref.at[slot_ref[k]], out_ref.at[k], sems.at[0]).start()
        return carry

    lax.fori_loop(0, owned, start, 0)
    pltpu.make_async_copy(got_ref.at[pl.ds(0, owned)], out_ref, sems.at[0]).wait()


def coded(x, q_ref, exps_ref, at, row):
    top = jnp.maximum(jnp.max(jnp.abs(x), axis=0, keepdims=True), 1e-30)
    exponent = jnp.ceil(jnp.log2(top))
    scaled = jnp.round(x * jnp.exp2(15.0 - exponent))
    scaled = jnp.minimum(jnp.maximum(scaled, -32767.0), 32767.0)
    q_ref[pl.ds(at, x.shape[0]), :] = scaled.astype(jnp.int32).astype(jnp.int16)
    exps_ref[pl.ds(row, 1), :] = exponent


def product_kernel(gx, gy, groups, steps, row_ref, col_ref, work_ref, tiles, feats_ref, swap_ref, *refs):
    keep_ref, even_ref, odd_ref, acc, held, made, exps, sems = refs
    slots, order, _ = tiles.shape
    per_step = slots // steps
    vblocks = held.shape[0] // gx
    blocks = acc.shape[0]
    span = blocks // groups
    a = lax.axis_index("gx")
    cores = 2

    acc[...] = jnp.zeros_like(acc)
    for k, f in enumerate((feats_ref, swap_ref)):
        held[pl.ds(k * f.shape[0], f.shape[0])] = f[...]

    pattern = lax.broadcasted_iota(jnp.int32, (order, order), 0) * order + lax.broadcasted_iota(
        jnp.int32, (order, order), 1
    )
    for i in range(steps):

        def form(t, carry):
            tile = i * per_step + t
            col = col_ref[tile]
            home = lax.div(col, gy * vblocks)
            away = lax.rem(lax.div(a, cores) - lax.div(home, cores) + gx, gx // cores)
            side = lax.rem(a + home, cores)
            place = (side * (gx // cores) + away) * vblocks + lax.rem(col, vblocks)
            masked = jnp.where(pattern < work_ref[tile], tiles[tile], jnp.zeros((), jnp.bfloat16))
            made[t] = jnp.dot(masked, held[place], preferred_element_type=jnp.float32)
            return carry

        lax.fori_loop(0, per_step, form, 0, unroll=True)

        def add(t, carry):
            row = lax.rem(row_ref[i * per_step + t], blocks)
            acc[row] += made[t]
            return carry

        lax.fori_loop(0, per_step, add, 0, unroll=True)

    owners = span // vblocks
    pairs = owners // 2
    side = lax.rem(lax.axis_index("z"), 2)

    def leave(n, carry):
        at = lax.div(n, pairs) * span + (2 * lax.rem(n, pairs) + side) * vblocks
        pltpu.make_async_copy(
            acc.at[pl.ds(at, vblocks)], keep_ref.at[pl.ds(n * vblocks, vblocks)], sems.at[0]
        ).start()
        return carry

    lax.fori_loop(0, groups * pairs, leave, 0)
    for v, q_ref in enumerate((even_ref, odd_ref)):

        def code(n, carry):
            at = lax.div(n, pairs) * span + (2 * lax.rem(n, pairs) + 1 - side) * vblocks + v
            coded(acc[at], q_ref, exps, n * order, n)
            return carry

        lax.fori_loop(0, groups * pairs, code, 0, unroll=2)
        store_exps(q_ref, exps, groups * pairs, order)
    pltpu.make_async_copy(acc.at[pl.ds(0, keep_ref.shape[0])], keep_ref, sems.at[0]).wait()


def scales_of(ref, at):
    exps = ref[pl.ds(at, ref.shape[0] - at), :].astype(jnp.int32).astype(jnp.float32)
    return jnp.exp2(exps - 15.0)


def part_of(ref, i, order, count):
    x = ref[pl.ds(i * order, order), :].astype(jnp.int32).astype(jnp.float32)
    return x * scales_of(ref, count * order)[i : i + 1, :]


def store_exps(q_ref, exps, count, order):
    q_ref[pl.ds(count * order, exps.shape[0]), :] = exps[...].astype(jnp.int32).astype(jnp.int16)


def join_kernel(order, vblocks, groups, keep_ref, even_ref, odd_ref, own_ref, rest_ref, right_ref, left_ref, scales, exps):
    span = keep_ref.shape[0] // groups
    half = span // 2
    lines = groups * span // vblocks
    y = lax.axis_index("y")
    got = (even_ref, odd_ref)
    for v, g in enumerate(got):
        scales[pl.ds(v * lines, lines), :] = scales_of(g, lines * order)

    def total(chunk, pair, v):
        n = chunk * (span // vblocks) + pair
        x = got[v][pl.ds(n * order, order), :].astype(jnp.int32).astype(jnp.float32)
        return keep_ref[n * vblocks + v] + x * scales[pl.ds(v * lines + n, 1), :]

    there, far, behind = (lax.rem(y + k, groups) for k in range(1, groups))
    low, high = 0, half // vblocks
    for chunk, start, at in ((y, low, 0), (y, high, half)):
        for i in range(half // vblocks):
            for v in range(vblocks):
                own_ref[at + i * vblocks + v] = total(chunk, start + i, v)
    for chunk, start, at in ((there, low, 0), (behind, high, half)):
        for i in range(half // vblocks):
            for v in range(vblocks):
                rest_ref[at + i * vblocks + v] = total(chunk, start + i, v)
    for q_ref, parts in ((right_ref, ((far, low), (there, high))), (left_ref, ((far, high), (behind, low)))):
        for n, (chunk, start) in enumerate(parts):
            for i in range(half // vblocks):
                for v in range(vblocks):
                    row = n * half + i * vblocks + v
                    coded(total(chunk, start + i, v), q_ref, exps, row * order, row)
        store_exps(q_ref, exps, span, order)


def relay_kernel(order, rest_ref, low_ref, high_ref, right_ref, left_ref, scales, exps):
    span = rest_ref.shape[0]
    half = span // 2
    exps[...] = jnp.zeros_like(exps)
    for side, (got, q_ref) in enumerate(((low_ref, right_ref), (high_ref, left_ref))):
        scales[...] = scales_of(got, span * order)
        for i in range(half):
            part = got[pl.ds(i * order, order), :].astype(jnp.int32).astype(jnp.float32)
            x = rest_ref[side * half + i] + part * scales[pl.ds(i, 1), :]
            coded(x, q_ref, exps, i * order, i)
        store_exps(q_ref, exps, half, order)


def middle_kernel(order, vblocks, own_ref, low_ref, high_ref, low2_ref, high2_ref, out_ref, *refs):
    q_refs, (total, exps) = refs[:-2], refs[-2:]
    span = own_ref.shape[0]
    half = span // 2
    owners = span // vblocks
    mine = lax.div(lax.axis_index("z"), 2)
    exps[...] = jnp.zeros_like(exps)
    for side, (near, last) in enumerate(((high_ref, low2_ref), (low_ref, high2_ref))):
        near_scales, last_scales = scales_of(near, span * order), scales_of(last, half * order)
        for i in range(half):
            x = own_ref[side * half + i]
            for ref, at, scale in ((near, half + i, near_scales[half + i : half + i + 1]), (last, i, last_scales[i : i + 1])):
                x = x + ref[pl.ds(at * order, order), :].astype(jnp.int32).astype(jnp.float32) * scale
            total[side * half + i] = x
    for v in range(vblocks):
        out_ref[pl.ds(v * order, order), :] = total[mine * vblocks + v]
    for k, q_ref in enumerate(q_refs, 1):
        base = lax.rem(mine + k, owners) * vblocks
        for v in range(vblocks):
            coded(total[base + v], q_ref, exps, v * order, v)
        store_exps(q_ref, exps, vblocks, order)


def last_kernel(order, vblocks, own_ref, *refs):
    got, out_ref = refs[:-1], refs[-1]
    for v in range(vblocks):
        x = own_ref[pl.ds(v * order, order), :]
        for g in got:
            x = x + part_of(g, v, order, vblocks)
        out_ref[pl.ds(v * order, order), :] = x


def on_device(features, tile_vals, tile_row, tile_col, tile_work):
    peers = lax.axis_size(GY)
    gx, ny, nz = (lax.axis_size(axis) for axis in GX_GY)
    slots, order, _ = tile_vals.shape
    owned = slots // 2
    width = features.shape[1]
    vblocks = features.shape[0] // order
    blocks = peers * vblocks
    told = pl.pallas_call(
        lambda *refs: tell_kernel(slots, *refs),
        in_specs=[ANY] * 3,
        out_specs=VMEM,
        out_shape=jax.ShapeDtypeStruct((peers, 2, 2 * slots), jnp.int32),
        scratch_shapes=[pltpu.VMEM((3, slots), jnp.int32), pltpu.SemaphoreType.DMA((3,))],
        compiler_params=limit(4),
        name="tell",
    )(*(in_hbm(t) for t in (tile_row, tile_col, tile_work)))

    cores = 2
    mine = [features.reshape(vblocks, order, width)]
    for k in range(1, gx // cores):
        mine.append(lax.ppermute(mine[0], "gx", [(i, (i + cores * k) % gx) for i in range(gx)]))
    meta = lax.all_to_all(told, GY, split_axis=0, concat_axis=0, tiled=True)
    feats = jnp.concatenate(mine)
    swapped = lax.ppermute(feats, "gx", [(i, i ^ 1) for i in range(gx)])
    tiles = pl.pallas_call(
        stage_kernel,
        in_specs=[ANY],
        out_specs=VMEM,
        out_shape=vmem(tile_vals.shape, tile_vals.dtype),
        scratch_shapes=[pltpu.SemaphoreType.DMA((8,))],
        compiler_params=limit(4),
        name="stage",
    )(in_hbm(tile_vals))
    small = jax.ShapeDtypeStruct((owned,), jnp.int32)
    sent = pl.pallas_call(
        lambda *refs: plan_kernel(peers, slots, *refs),
        in_specs=[SMEM, VMEM],
        out_specs=ANY,
        out_shape=pltpu.HBM(tile_vals.shape, tile_vals.dtype),
        scratch_shapes=[pltpu.SemaphoreType.DMA((1,))],
        compiler_params=limit(4),
        name="plan",
    )(meta, in_vmem(tiles))
    moved_row, moved_col, moved_work, kept = pl.pallas_call(
        lambda *refs: list_kernel(peers, slots, *refs),
        in_specs=[SMEM],
        out_specs=[SMEM] * 4,
        out_shape=[small] * 4,
        compiler_params=limit(4),
        name="list",
    )(meta)
    got = lax.all_to_all(sent, GY, split_axis=0, concat_axis=0, tiled=True)

    steps = 8
    span = blocks // ny
    i16 = jnp.int16

    def line(count, more=8):
        return vmem((count * order + more, width), i16)

    lines = blocks // 2 // vblocks
    few = span // 2
    keep, even, odd = pl.pallas_call(
        lambda *refs: product_kernel(gx, peers, ny, steps, *refs),
        in_specs=[SMEM] * 3 + [VMEM] * 3,
        out_specs=[ANY, VMEM, VMEM],
        out_shape=[pltpu.HBM((blocks // 2, order, width), jnp.float32), line(lines, lines), line(lines, lines)],
        scratch_shapes=[
            pltpu.VMEM((blocks, order, width), jnp.float32),
            pltpu.VMEM((gx * vblocks, order, width), jnp.bfloat16),
            pltpu.VMEM((slots // steps, order, width), jnp.float32),
            pltpu.VMEM((lines, width), jnp.float32),
            pltpu.SemaphoreType.DMA((1,)),
        ],
        compiler_params=limit(16),
        name="products",
    )(tile_row, tile_col, tile_work, *(in_vmem(f) for f in (tiles, feats, swapped)))
    near = []
    for v, q in enumerate((even, odd)):
        near.append(lax.ppermute(q, "z", [(i, ((i + v) ^ 1) - v & nz - 1) for i in range(nz)]))
    some = vmem((few, order, width), jnp.float32)
    own, rest, right, left = pl.pallas_call(
        lambda *refs: join_kernel(order, vblocks, ny, *refs),
        in_specs=[VMEM] * 3,
        out_specs=[VMEM] * 4,
        out_shape=[some, some, line(few), line(few)],
        scratch_shapes=[pltpu.VMEM((2 * lines, width), jnp.float32), pltpu.VMEM((8, width), jnp.float32)],
        compiler_params=limit(12),
        name="join",
    )(keep, *near)
    low, high = shifted(right, "y", 1), shifted(left, "y", -1)
    right, left = pl.pallas_call(
        lambda *refs: relay_kernel(order, *refs),
        in_specs=[VMEM] * 3,
        out_specs=[VMEM] * 2,
        out_shape=[line(few // 2)] * 2,
        scratch_shapes=[pltpu.VMEM((8, width), jnp.float32), pltpu.VMEM((8, width), jnp.float32)],
        compiler_params=limit(8),
        name="relay",
    )(rest, low, high)
    low2, high2 = shifted(right, "y", 1), shifted(left, "y", -1)
    own_z, *coded_z = pl.pallas_call(
        lambda *refs: middle_kernel(order, vblocks, *refs),
        in_specs=[VMEM] * 5,
        out_specs=[VMEM] * (nz // 2),
        out_shape=[vmem((vblocks * order, width), jnp.float32)] + [line(vblocks)] * (nz // 2 - 1),
        scratch_shapes=[pltpu.VMEM((few, order, width), jnp.float32), pltpu.VMEM((8, width), jnp.float32)],
        compiler_params=limit(8),
        name="middle",
    )(own, low, high, low2, high2)
    got_z = []
    for k, q in enumerate(coded_z, 1):
        got_z.append(shifted(q, "z", 2 * k))
    product = pl.pallas_call(
        lambda *refs: last_kernel(order, vblocks, *refs),
        in_specs=[VMEM] * (nz // 2),
        out_specs=VMEM,
        out_shape=jax.ShapeDtypeStruct((vblocks * order, width), jnp.float32),
        compiler_params=limit(4),
        name="last",
    )(*(in_vmem(g) for g in (own_z, *got_z)))

    moved_vals = pl.pallas_call(
        lambda *refs: keep_kernel(owned, *refs),
        in_specs=[SMEM, VMEM],
        out_specs=ANY,
        out_shape=jax.ShapeDtypeStruct((owned, *tile_vals.shape[1:]), tile_vals.dtype),
        scratch_shapes=[pltpu.SemaphoreType.DMA((1,))],
        compiler_params=limit(4),
        name="keep",
    )(kept, in_vmem(got))
    return (product, moved_vals, moved_row, moved_col, moved_work)


def solution(mesh):
    finer = Mesh(mesh.devices.reshape(mesh.shape["gx"], 4, 8), GX_GY)
    in_specs = (P(GX_GY, None), P(GX_GY, None, None), P(GX_GY), P(GX_GY), P(GX_GY))

    return jax.shard_map(on_device, mesh=finer, in_specs=in_specs, out_specs=in_specs, check_vma=False)
```

```python
import jax
import jax.numpy as jnp
from jax import lax
from jax.experimental import pallas as pl
from jax.experimental.pallas import tpu as pltpu
from jax.sharding import Mesh
from jax.sharding import PartitionSpec as P

GY = ("y", "z")
GX_GY = ("gx", "y", "z")

ANY = pl.BlockSpec(memory_space=pl.ANY)
SMEM = pl.BlockSpec(memory_space=pltpu.SMEM)
VMEM = pl.BlockSpec(memory_space=pltpu.VMEM)


def in_vmem(array):
    return pltpu.with_memory_space_constraint(array, pltpu.VMEM)


def in_hbm(array):
    return pltpu.with_memory_space_constraint(array, pltpu.HBM)


def vmem(shape, dtype):
    return pltpu.VMEM(shape, dtype)


def limit(mib):
    return pltpu.CompilerParams(vmem_limit_bytes=mib * 2**20)


def shifted(array, axis, by):
    size = lax.axis_size(axis)
    return lax.ppermute(array, axis, [(i, (i + by) % size) for i in range(size)])


def tell_kernel(slots, row_ref, col_ref, work_ref, out_ref, held, sems):
    copies = [
        pltpu.make_async_copy(ref, held.at[i], sems.at[i]) for i, ref in enumerate((row_ref, col_ref, work_ref))
    ]
    for c in copies:
        c.start()
    for c in copies:
        c.wait()
    row, col, work = (held[i].reshape(1, slots) for i in range(3))
    count = jnp.sum((work > 0).astype(jnp.int32), axis=1, keepdims=True)
    for i, pair in enumerate(((row, col), (work, jnp.broadcast_to(count, (1, slots))))):
        line = jnp.concatenate(pair, axis=1)
        out_ref[:, i, :] = jnp.broadcast_to(line, (out_ref.shape[0], 2 * slots))


def stage_kernel(vals_ref, out_ref, sems):
    groups = sems.shape[0]
    size = vals_ref.shape[0] // groups
    copies = [
        pltpu.make_async_copy(
            vals_ref.at[pl.ds(g * size, size)], out_ref.at[pl.ds(g * size, size)], sems.at[g]
        )
        for g in range(groups)
    ]
    for c in copies:
        c.start()
    for c in copies:
        c.wait()


def place_of():
    return lax.axis_index("y") * lax.axis_size("z") + lax.axis_index("z")


def plan_kernel(peers, slots, meta_ref, vals_ref, sent_ref, sems):
    me = place_of()
    share = slots // peers

    counts = meta_ref[:, 1, :]
    earlier = (lax.broadcasted_iota(jnp.int32, counts.shape, 0) < me) & (
        lax.broadcasted_iota(jnp.int32, counts.shape, 1) == slots
    )
    first = jnp.sum(jnp.where(earlier, counts, 0).astype(jnp.float32)).astype(jnp.int32)
    turn = lax.rem(first, peers)

    def start(d, carry):
        at = lax.rem(d - turn + peers, peers)
        for w in range(share):
            pltpu.make_async_copy(
                vals_ref.at[at + w * peers], sent_ref.at[d * share + w], sems.at[0]
            ).start()
        return carry

    lax.fori_loop(0, peers, start, 0, unroll=8)
    pltpu.make_async_copy(vals_ref, sent_ref, sems.at[0]).wait()


def list_kernel(peers, slots, meta_ref, row_ref, col_ref, work_ref, slot_ref):
    me = place_of()
    share = slots // peers

    def source(s, begin):
        count = meta_ref[s, 1, slots]
        j = lax.rem(me - lax.rem(begin, peers) + peers, peers)
        for w in range(share):
            at = j + w * peers

            @pl.when(at < count)
            def _():
                k = lax.div(begin + at, peers)
                row_ref[k] = meta_ref[s, 0, at]
                col_ref[k] = meta_ref[s, 0, slots + at]
                work_ref[k] = meta_ref[s, 1, at]
                slot_ref[k] = s * share + w

        return begin + count

    lax.fori_loop(0, peers, source, jnp.int32(0))


def keep_kernel(owned, slot_ref, got_ref, out_ref, sems):
    def start(k, carry):
        pltpu.make_async_copy(got_ref.at[slot_ref[k]], out_ref.at[k], sems.at[0]).start()
        return carry

    lax.fori_loop(0, owned, start, 0)
    pltpu.make_async_copy(got_ref.at[pl.ds(0, owned)], out_ref, sems.at[0]).wait()


MARGIN = 0.999


def coded(x, q_ref, exps_ref, at, row):
    top = jnp.maximum(jnp.max(jnp.abs(x), axis=0, keepdims=True), 1e-30)
    exponent = jnp.ceil(jnp.log2(top))
    scaled = jnp.round(x * (jnp.exp2(15.0 - exponent) * MARGIN))
    q_ref[pl.ds(at, x.shape[0]), :] = scaled.astype(jnp.int32).astype(jnp.int16)
    exps_ref[pl.ds(row, 1), :] = exponent


def product_kernel(gx, gy, groups, steps, row_ref, col_ref, work_ref, tiles, *refs):
    feats, refs = refs[:gx], refs[gx:]
    keep_ref, even_ref, odd_ref, acc, held, made, exps, codes, sems = refs
    slots, order, _ = tiles.shape
    per_step = slots // steps
    vblocks = held.shape[0] // gx
    blocks = acc.shape[0]
    span = blocks // groups
    a = lax.axis_index("gx")
    cores = 2

    acc[...] = jnp.zeros_like(acc)
    for k, f in enumerate(feats):
        held[pl.ds(k * f.shape[0], f.shape[0])] = f[...]

    pattern = lax.broadcasted_iota(jnp.int32, (order, order), 0) * order + lax.broadcasted_iota(
        jnp.int32, (order, order), 1
    )
    for i in range(steps):

        def form(t, carry):
            tile = i * per_step + t
            col = col_ref[tile]
            home = lax.div(col, gy * vblocks)
            away = lax.rem(lax.div(a, cores) - lax.div(home, cores) + gx, gx // cores)
            side = lax.rem(a + home, cores)
            place = (side * (gx // cores) + away) * vblocks + lax.rem(col, vblocks)
            masked = jnp.where(pattern < work_ref[tile], tiles[tile], jnp.zeros((), jnp.bfloat16))
            made[t] = jnp.dot(masked, held[place], preferred_element_type=jnp.float32)
            return carry

        lax.fori_loop(0, per_step, form, 0, unroll=True)

        def add(t, carry):
            row = lax.rem(row_ref[i * per_step + t], blocks)
            acc[row] += made[t]
            return carry

        lax.fori_loop(0, per_step, add, 0, unroll=True)

    owners = span // vblocks
    pairs = owners // 2
    side = lax.rem(lax.axis_index("z"), 2)

    def leave(n, carry):
        at = lax.div(n, pairs) * span + (2 * lax.rem(n, pairs) + side) * vblocks
        pltpu.make_async_copy(
            acc.at[pl.ds(at, vblocks)], keep_ref.at[pl.ds(n * vblocks, vblocks)], sems.at[0]
        ).start()
        return carry

    lax.fori_loop(0, groups * pairs, leave, 0)
    lines = groups * pairs
    parts = 2
    leaving = []
    for v, q_ref in enumerate((even_ref, odd_ref)):
        held_codes = codes.at[v]

        def code(n, carry):
            at = lax.div(n, pairs) * span + (2 * lax.rem(n, pairs) + 1 - side) * vblocks + v
            coded(acc[at], held_codes, exps, n * order, n)
            return carry

        for i in range(parts):
            lax.fori_loop(i * lines // parts, (i + 1) * lines // parts, code, 0, unroll=2)
            if i == parts - 1:
                store_exps(held_codes, exps, lines, order)
            begin = i * lines * order // parts
            size = q_ref.shape[0] - begin if i == parts - 1 else lines * order // parts
            leaving.append(
                pltpu.make_async_copy(
                    held_codes.at[pl.ds(begin, size)], q_ref.at[pl.ds(begin, size)], sems.at[1 + v * parts + i]
                )
            )
            leaving[-1].start()
    for c in leaving:
        c.wait()
    pltpu.make_async_copy(acc.at[pl.ds(0, keep_ref.shape[0])], keep_ref, sems.at[0]).wait()


def scales_of(ref, at):
    exps = ref[pl.ds(at, ref.shape[0] - at), :].astype(jnp.int32).astype(jnp.float32)
    return jnp.exp2(exps - 15.0) * (1.0 / MARGIN)


def part_of(ref, i, order, count):
    x = ref[pl.ds(i * order, order), :].astype(jnp.int32).astype(jnp.float32)
    return x * scales_of(ref, count * order)[i : i + 1, :]


def store_exps(q_ref, exps, count, order):
    q_ref[pl.ds(count * order, exps.shape[0]), :] = exps[...].astype(jnp.int32).astype(jnp.int16)


def join_kernel(order, vblocks, groups, keep_ref, even_ref, odd_ref, own_ref, rest_ref, right_ref, left_ref, scales, exps):
    span = keep_ref.shape[0] // groups
    half = span // 2
    lines = groups * span // vblocks
    y = lax.axis_index("y")
    got = (even_ref, odd_ref)
    for v, g in enumerate(got):
        scales[pl.ds(v * lines, lines), :] = scales_of(g, lines * order)

    def total(chunk, pair, v):
        n = chunk * (span // vblocks) + pair
        x = got[v][pl.ds(n * order, order), :].astype(jnp.int32).astype(jnp.float32)
        return keep_ref[n * vblocks + v] + x * scales[pl.ds(v * lines + n, 1), :]

    there, far, behind = (lax.rem(y + k, groups) for k in range(1, groups))
    low, high = 0, half // vblocks
    for chunk, start, at in ((y, low, 0), (y, high, half)):
        for i in range(half // vblocks):
            for v in range(vblocks):
                own_ref[at + i * vblocks + v] = total(chunk, start + i, v)
    for chunk, start, at in ((there, low, 0), (behind, high, half)):
        for i in range(half // vblocks):
            for v in range(vblocks):
                rest_ref[at + i * vblocks + v] = total(chunk, start + i, v)
    for q_ref, parts in ((right_ref, ((far, low), (there, high))), (left_ref, ((far, high), (behind, low)))):
        for n, (chunk, start) in enumerate(parts):
            for i in range(half // vblocks):
                for v in range(vblocks):
                    row = n * half + i * vblocks + v
                    coded(total(chunk, start + i, v), q_ref, exps, row * order, row)
        store_exps(q_ref, exps, span, order)


def relay_kernel(order, rest_ref, low_ref, high_ref, right_ref, left_ref, scales, exps):
    span = rest_ref.shape[0]
    half = span // 2
    exps[...] = jnp.zeros_like(exps)
    for side, (got, q_ref) in enumerate(((low_ref, right_ref), (high_ref, left_ref))):
        scales[...] = scales_of(got, span * order)
        for i in range(half):
            part = got[pl.ds(i * order, order), :].astype(jnp.int32).astype(jnp.float32)
            x = rest_ref[side * half + i] + part * scales[pl.ds(i, 1), :]
            coded(x, q_ref, exps, i * order, i)
        store_exps(q_ref, exps, half, order)


def middle_kernel(order, vblocks, own_ref, low_ref, high_ref, low2_ref, high2_ref, out_ref, *refs):
    q_refs, (total, exps) = refs[:-2], refs[-2:]
    span = own_ref.shape[0]
    half = span // 2
    owners = span // vblocks
    mine = lax.div(lax.axis_index("z"), 2)
    exps[...] = jnp.zeros_like(exps)
    for side, (near, last) in enumerate(((high_ref, low2_ref), (low_ref, high2_ref))):
        near_scales, last_scales = scales_of(near, span * order), scales_of(last, half * order)
        for i in range(half):
            x = own_ref[side * half + i]
            for ref, at, scale in ((near, half + i, near_scales[half + i : half + i + 1]), (last, i, last_scales[i : i + 1])):
                x = x + ref[pl.ds(at * order, order), :].astype(jnp.int32).astype(jnp.float32) * scale
            total[side * half + i] = x
    for v in range(vblocks):
        out_ref[pl.ds(v * order, order), :] = total[mine * vblocks + v]
    for k, q_ref in enumerate(q_refs, 1):
        base = lax.rem(mine + k, owners) * vblocks
        for v in range(vblocks):
            coded(total[base + v], q_ref, exps, v * order, v)
        store_exps(q_ref, exps, vblocks, order)


def last_kernel(order, vblocks, own_ref, *refs):
    got, out_ref = refs[:-1], refs[-1]
    for v in range(vblocks):
        x = own_ref[pl.ds(v * order, order), :]
        for g in got:
            x = x + part_of(g, v, order, vblocks)
        out_ref[pl.ds(v * order, order), :] = x


def on_device(features, tile_vals, tile_row, tile_col, tile_work):
    peers = lax.axis_size(GY)
    gx, ny, nz = (lax.axis_size(axis) for axis in GX_GY)
    slots, order, _ = tile_vals.shape
    owned = slots // 2
    width = features.shape[1]
    vblocks = features.shape[0] // order
    blocks = peers * vblocks
    told = pl.pallas_call(
        lambda *refs: tell_kernel(slots, *refs),
        in_specs=[ANY] * 3,
        out_specs=VMEM,
        out_shape=jax.ShapeDtypeStruct((peers, 2, 2 * slots), jnp.int32),
        scratch_shapes=[pltpu.VMEM((3, slots), jnp.int32), pltpu.SemaphoreType.DMA((3,))],
        compiler_params=limit(4),
        name="tell",
    )(*(in_hbm(t) for t in (tile_row, tile_col, tile_work)))

    cores = 2
    mine = [features.reshape(vblocks, order, width)]
    for k in range(1, gx // cores):
        mine.append(lax.ppermute(mine[0], "gx", [(i, (i + cores * k) % gx) for i in range(gx)]))
    meta = lax.all_to_all(told, GY, split_axis=0, concat_axis=0, tiled=True)
    swapped = []
    for f in mine:
        swapped.append(lax.ppermute(f, "gx", [(i, i ^ 1) for i in range(gx)]))
    tiles = pl.pallas_call(
        stage_kernel,
        in_specs=[ANY],
        out_specs=VMEM,
        out_shape=vmem(tile_vals.shape, tile_vals.dtype),
        scratch_shapes=[pltpu.SemaphoreType.DMA((8,))],
        compiler_params=limit(4),
        name="stage",
    )(in_hbm(tile_vals))
    small = jax.ShapeDtypeStruct((owned,), jnp.int32)
    sent = pl.pallas_call(
        lambda *refs: plan_kernel(peers, slots, *refs),
        in_specs=[VMEM, VMEM],
        out_specs=ANY,
        out_shape=pltpu.HBM(tile_vals.shape, tile_vals.dtype),
        scratch_shapes=[pltpu.SemaphoreType.DMA((1,))],
        compiler_params=limit(4),
        name="plan",
    )(in_vmem(meta), in_vmem(tiles))
    moved_row, moved_col, moved_work, kept = pl.pallas_call(
        lambda *refs: list_kernel(peers, slots, *refs),
        in_specs=[SMEM],
        out_specs=[SMEM] * 4,
        out_shape=[small] * 4,
        compiler_params=limit(4),
        name="list",
    )(meta)
    got = lax.all_to_all(sent, GY, split_axis=0, concat_axis=0, tiled=True)

    steps = 8
    span = blocks // ny
    i16 = jnp.int16

    def line(count, more=8):
        return vmem((count * order + more, width), i16)

    lines = blocks // 2 // vblocks
    few = span // 2
    keep, even, odd = pl.pallas_call(
        lambda *refs: product_kernel(gx, peers, ny, steps, *refs),
        in_specs=[SMEM] * 3 + [VMEM] * (1 + gx),
        out_specs=[ANY] * 3,
        out_shape=[pltpu.HBM((blocks // 2, order, width), jnp.float32)]
        + [pltpu.HBM((lines * order + lines, width), i16)] * 2,
        scratch_shapes=[
            pltpu.VMEM((blocks, order, width), jnp.float32),
            pltpu.VMEM((gx * vblocks, order, width), jnp.bfloat16),
            pltpu.VMEM((slots // steps, order, width), jnp.float32),
            pltpu.VMEM((lines, width), jnp.float32),
            pltpu.VMEM((2, lines * order + lines, width), i16),
            pltpu.SemaphoreType.DMA((5,)),
        ],
        compiler_params=limit(16),
        name="products",
    )(tile_row, tile_col, tile_work, *(in_vmem(f) for f in (tiles, *mine, *swapped)))
    near = []
    for v, q in enumerate((even, odd)):
        near.append(lax.ppermute(q, "z", [(i, ((i + v) ^ 1) - v & nz - 1) for i in range(nz)]))
    some = vmem((few, order, width), jnp.float32)
    own, rest, right, left = pl.pallas_call(
        lambda *refs: join_kernel(order, vblocks, ny, *refs),
        in_specs=[VMEM] * 3,
        out_specs=[VMEM] * 4,
        out_shape=[some, some, line(few), line(few)],
        scratch_shapes=[pltpu.VMEM((2 * lines, width), jnp.float32), pltpu.VMEM((8, width), jnp.float32)],
        compiler_params=limit(12),
        name="join",
    )(keep, *near)
    low, high = shifted(right, "y", 1), shifted(left, "y", -1)
    right, left = pl.pallas_call(
        lambda *refs: relay_kernel(order, *refs),
        in_specs=[VMEM] * 3,
        out_specs=[VMEM] * 2,
        out_shape=[line(few // 2)] * 2,
        scratch_shapes=[pltpu.VMEM((8, width), jnp.float32), pltpu.VMEM((8, width), jnp.float32)],
        compiler_params=limit(8),
        name="relay",
    )(rest, low, high)
    low2, high2 = shifted(right, "y", 1), shifted(left, "y", -1)
    own_z, *coded_z = pl.pallas_call(
        lambda *refs: middle_kernel(order, vblocks, *refs),
        in_specs=[VMEM] * 5,
        out_specs=[VMEM] * (nz // 2),
        out_shape=[vmem((vblocks * order, width), jnp.float32)] + [line(vblocks)] * (nz // 2 - 1),
        scratch_shapes=[pltpu.VMEM((few, order, width), jnp.float32), pltpu.VMEM((8, width), jnp.float32)],
        compiler_params=limit(8),
        name="middle",
    )(own, low, high, low2, high2)
    got_z = []
    for k, q in enumerate(coded_z, 1):
        got_z.append(shifted(q, "z", 2 * k))
    product = pl.pallas_call(
        lambda *refs: last_kernel(order, vblocks, *refs),
        in_specs=[VMEM] * (nz // 2),
        out_specs=VMEM,
        out_shape=jax.ShapeDtypeStruct((vblocks * order, width), jnp.float32),
        compiler_params=limit(4),
        name="last",
    )(*(in_vmem(g) for g in (own_z, *got_z)))

    moved_vals = pl.pallas_call(
        lambda *refs: keep_kernel(owned, *refs),
        in_specs=[SMEM, VMEM],
        out_specs=ANY,
        out_shape=jax.ShapeDtypeStruct((owned, *tile_vals.shape[1:]), tile_vals.dtype),
        scratch_shapes=[pltpu.SemaphoreType.DMA((1,))],
        compiler_params=limit(4),
        name="keep",
    )(kept, in_vmem(got))
    return (product, moved_vals, moved_row, moved_col, moved_work)


def solution(mesh):
    finer = Mesh(mesh.devices.reshape(mesh.shape["gx"], 4, 8), GX_GY)
    in_specs = (P(GX_GY, None), P(GX_GY, None, None), P(GX_GY), P(GX_GY), P(GX_GY))

    return jax.shard_map(on_device, mesh=finer, in_specs=in_specs, out_specs=in_specs, check_vma=False)
```

```python
import jax
import jax.numpy as jnp
from jax import lax
from jax.experimental import pallas as pl
from jax.experimental.pallas import tpu as pltpu
from jax.sharding import Mesh
from jax.sharding import PartitionSpec as P

GY = ("y", "z")
GX_GY = ("gx", "y", "z")

ANY = pl.BlockSpec(memory_space=pl.ANY)
SMEM = pl.BlockSpec(memory_space=pltpu.SMEM)
VMEM = pl.BlockSpec(memory_space=pltpu.VMEM)


def in_vmem(array):
    return pltpu.with_memory_space_constraint(array, pltpu.VMEM)


def in_hbm(array):
    return pltpu.with_memory_space_constraint(array, pltpu.HBM)


def vmem(shape, dtype):
    return pltpu.VMEM(shape, dtype)


def limit(mib):
    return pltpu.CompilerParams(vmem_limit_bytes=mib * 2**20)


def shifted(array, axis, by):
    size = lax.axis_size(axis)
    return lax.ppermute(array, axis, [(i, (i + by) % size) for i in range(size)])


def tell_kernel(slots, row_ref, col_ref, work_ref, vals_ref, out_ref, tiles_ref, held, sems, tile_sems):
    copies = [
        pltpu.make_async_copy(ref, held.at[i], sems.at[i]) for i, ref in enumerate((row_ref, col_ref, work_ref))
    ]
    groups = tile_sems.shape[0]
    size = slots // groups
    staged = [
        pltpu.make_async_copy(
            vals_ref.at[pl.ds(g * size, size)], tiles_ref.at[pl.ds(g * size, size)], tile_sems.at[g]
        )
        for g in range(groups)
    ]
    for c in (*copies, *staged):
        c.start()
    for c in copies:
        c.wait()
    row, col, work = (held[i].reshape(1, slots) for i in range(3))
    count = jnp.sum((work > 0).astype(jnp.int32), axis=1, keepdims=True)
    for i, pair in enumerate(((row, col), (work, jnp.broadcast_to(count, (1, slots))))):
        line = jnp.concatenate(pair, axis=1)
        out_ref[:, i, :] = jnp.broadcast_to(line, (out_ref.shape[0], 2 * slots))
    for c in staged:
        c.wait()


def place_of():
    return lax.axis_index("y") * lax.axis_size("z") + lax.axis_index("z")


def plan_kernel(peers, slots, meta_ref, vals_ref, sent_ref, sems):
    me = place_of()
    share = slots // peers

    counts = meta_ref[:, 1, :]
    earlier = (lax.broadcasted_iota(jnp.int32, counts.shape, 0) < me) & (
        lax.broadcasted_iota(jnp.int32, counts.shape, 1) == slots
    )
    first = jnp.sum(jnp.where(earlier, counts, 0).astype(jnp.float32)).astype(jnp.int32)
    turn = lax.rem(first, peers)

    def start(d, carry):
        at = lax.rem(d - turn + peers, peers)
        for w in range(share):
            pltpu.make_async_copy(
                vals_ref.at[at + w * peers], sent_ref.at[d * share + w], sems.at[0]
            ).start()
        return carry

    lax.fori_loop(0, peers, start, 0, unroll=8)
    pltpu.make_async_copy(vals_ref, sent_ref, sems.at[0]).wait()


def list_kernel(peers, slots, meta_ref, row_ref, col_ref, work_ref, slot_ref):
    me = place_of()
    share = slots // peers

    def source(s, begin):
        count = meta_ref[s, 1, slots]
        j = lax.rem(me - lax.rem(begin, peers) + peers, peers)
        for w in range(share):
            at = j + w * peers

            @pl.when(at < count)
            def _():
                k = lax.div(begin + at, peers)
                row_ref[k] = meta_ref[s, 0, at]
                col_ref[k] = meta_ref[s, 0, slots + at]
                work_ref[k] = meta_ref[s, 1, at]
                slot_ref[k] = s * share + w

        return begin + count

    lax.fori_loop(0, peers, source, jnp.int32(0))


def keep_kernel(owned, slot_ref, got_ref, out_ref, sems):
    def start(k, carry):
        pltpu.make_async_copy(got_ref.at[slot_ref[k]], out_ref.at[k], sems.at[0]).start()
        return carry

    lax.fori_loop(0, owned, start, 0)
    pltpu.make_async_copy(got_ref.at[pl.ds(0, owned)], out_ref, sems.at[0]).wait()


MARGIN = 0.999


def coded(x, q_ref, exps_ref, at, row):
    top = jnp.maximum(jnp.max(jnp.abs(x), axis=0, keepdims=True), 1e-30)
    exponent = jnp.ceil(jnp.log2(top))
    scaled = jnp.round(x * (jnp.exp2(15.0 - exponent) * MARGIN))
    q_ref[pl.ds(at, x.shape[0]), :] = scaled.astype(jnp.int32).astype(jnp.int16)
    exps_ref[pl.ds(row, 1), :] = exponent


def product_kernel(gx, gy, groups, steps, row_ref, col_ref, work_ref, tiles, *refs):
    feats, refs = refs[:gx], refs[gx:]
    keep_ref, even_ref, odd_ref, acc, held, made, exps, codes, sems = refs
    slots, order, _ = tiles.shape
    per_step = slots // steps
    vblocks = held.shape[0] // gx
    blocks = acc.shape[0]
    span = blocks // groups
    a = lax.axis_index("gx")
    cores = 2

    acc[...] = jnp.zeros_like(acc)
    for k, f in enumerate(feats):
        held[pl.ds(k * f.shape[0], f.shape[0])] = f[...]

    pattern = lax.broadcasted_iota(jnp.int32, (order, order), 0) * order + lax.broadcasted_iota(
        jnp.int32, (order, order), 1
    )
    for i in range(steps):

        def form(t, carry):
            tile = i * per_step + t
            col = col_ref[tile]
            home = lax.div(col, gy * vblocks)
            away = lax.rem(lax.div(a, cores) - lax.div(home, cores) + gx, gx // cores)
            side = lax.rem(a + home, cores)
            place = (side * (gx // cores) + away) * vblocks + lax.rem(col, vblocks)
            masked = jnp.where(pattern < work_ref[tile], tiles[tile], jnp.zeros((), jnp.bfloat16))
            made[t] = jnp.dot(masked, held[place], preferred_element_type=jnp.float32)
            return carry

        lax.fori_loop(0, per_step, form, 0, unroll=True)

        def add(t, carry):
            row = lax.rem(row_ref[i * per_step + t], blocks)
            acc[row] += made[t]
            return carry

        lax.fori_loop(0, per_step, add, 0, unroll=True)

    owners = span // vblocks
    pairs = owners // 2
    side = lax.rem(lax.axis_index("z"), 2)

    def leave(n, carry):
        at = lax.div(n, pairs) * span + (2 * lax.rem(n, pairs) + side) * vblocks
        pltpu.make_async_copy(
            acc.at[pl.ds(at, vblocks)], keep_ref.at[pl.ds(n * vblocks, vblocks)], sems.at[0]
        ).start()
        return carry

    lax.fori_loop(0, groups * pairs, leave, 0)
    lines = groups * pairs
    parts = 2
    leaving = []
    for v, q_ref in enumerate((even_ref, odd_ref)):
        held_codes = codes.at[v]

        def code(n, carry):
            at = lax.div(n, pairs) * span + (2 * lax.rem(n, pairs) + 1 - side) * vblocks + v
            coded(acc[at], held_codes, exps, n * order, n)
            return carry

        for i in range(parts):
            lax.fori_loop(i * lines // parts, (i + 1) * lines // parts, code, 0, unroll=2)
            if i == parts - 1:
                store_exps(held_codes, exps, lines, order)
            begin = i * lines * order // parts
            size = q_ref.shape[0] - begin if i == parts - 1 else lines * order // parts
            leaving.append(
                pltpu.make_async_copy(
                    held_codes.at[pl.ds(begin, size)], q_ref.at[pl.ds(begin, size)], sems.at[1 + v * parts + i]
                )
            )
            leaving[-1].start()
    for c in leaving:
        c.wait()
    pltpu.make_async_copy(acc.at[pl.ds(0, keep_ref.shape[0])], keep_ref, sems.at[0]).wait()


def scales_of(ref, at):
    exps = ref[pl.ds(at, ref.shape[0] - at), :].astype(jnp.int32).astype(jnp.float32)
    return jnp.exp2(exps - 15.0) * (1.0 / MARGIN)


def part_of(ref, i, order, count):
    x = ref[pl.ds(i * order, order), :].astype(jnp.int32).astype(jnp.float32)
    return x * scales_of(ref, count * order)[i : i + 1, :]


def store_exps(q_ref, exps, count, order):
    q_ref[pl.ds(count * order, exps.shape[0]), :] = exps[...].astype(jnp.int32).astype(jnp.int16)


def join_kernel(order, vblocks, groups, keep_ref, even_ref, odd_ref, own_ref, rest_ref, right_ref, left_ref, scales, exps):
    span = keep_ref.shape[0] // groups
    half = span // 2
    lines = groups * span // vblocks
    y = lax.axis_index("y")
    got = (even_ref, odd_ref)
    for v, g in enumerate(got):
        scales[pl.ds(v * lines, lines), :] = scales_of(g, lines * order)

    def total(chunk, pair, v):
        n = chunk * (span // vblocks) + pair
        x = got[v][pl.ds(n * order, order), :].astype(jnp.int32).astype(jnp.float32)
        return keep_ref[n * vblocks + v] + x * scales[pl.ds(v * lines + n, 1), :]

    there, far, behind = (lax.rem(y + k, groups) for k in range(1, groups))
    low, high = 0, half // vblocks
    for chunk, start, at in ((y, low, 0), (y, high, half)):
        for i in range(half // vblocks):
            for v in range(vblocks):
                own_ref[at + i * vblocks + v] = total(chunk, start + i, v)
    for chunk, start, at in ((there, low, 0), (behind, high, half)):
        for i in range(half // vblocks):
            for v in range(vblocks):
                rest_ref[at + i * vblocks + v] = total(chunk, start + i, v)
    for q_ref, parts in ((right_ref, ((far, low), (there, high))), (left_ref, ((far, high), (behind, low)))):
        for n, (chunk, start) in enumerate(parts):
            for i in range(half // vblocks):
                for v in range(vblocks):
                    row = n * half + i * vblocks + v
                    coded(total(chunk, start + i, v), q_ref, exps, row * order, row)
        store_exps(q_ref, exps, span, order)


def relay_kernel(order, rest_ref, low_ref, high_ref, right_ref, left_ref, scales, exps):
    span = rest_ref.shape[0]
    half = span // 2
    exps[...] = jnp.zeros_like(exps)
    for side, (got, q_ref) in enumerate(((low_ref, right_ref), (high_ref, left_ref))):
        scales[...] = scales_of(got, span * order)
        for i in range(half):
            part = got[pl.ds(i * order, order), :].astype(jnp.int32).astype(jnp.float32)
            x = rest_ref[side * half + i] + part * scales[pl.ds(i, 1), :]
            coded(x, q_ref, exps, i * order, i)
        store_exps(q_ref, exps, half, order)


def middle_kernel(order, vblocks, own_ref, low_ref, high_ref, low2_ref, high2_ref, out_ref, *refs):
    q_refs, (total, exps) = refs[:-2], refs[-2:]
    span = own_ref.shape[0]
    half = span // 2
    owners = span // vblocks
    mine = lax.div(lax.axis_index("z"), 2)
    exps[...] = jnp.zeros_like(exps)
    for side, (near, last) in enumerate(((high_ref, low2_ref), (low_ref, high2_ref))):
        near_scales, last_scales = scales_of(near, span * order), scales_of(last, half * order)
        for i in range(half):
            x = own_ref[side * half + i]
            for ref, at, scale in ((near, half + i, near_scales[half + i : half + i + 1]), (last, i, last_scales[i : i + 1])):
                x = x + ref[pl.ds(at * order, order), :].astype(jnp.int32).astype(jnp.float32) * scale
            total[side * half + i] = x
    for v in range(vblocks):
        out_ref[pl.ds(v * order, order), :] = total[mine * vblocks + v]
    for k, q_ref in enumerate(q_refs, 1):
        base = lax.rem(mine + k, owners) * vblocks
        for v in range(vblocks):
            coded(total[base + v], q_ref, exps, v * order, v)
        store_exps(q_ref, exps, vblocks, order)


def last_kernel(order, vblocks, own_ref, *refs):
    got, out_ref = refs[:-1], refs[-1]
    for v in range(vblocks):
        x = own_ref[pl.ds(v * order, order), :]
        for g in got:
            x = x + part_of(g, v, order, vblocks)
        out_ref[pl.ds(v * order, order), :] = x


def on_device(features, tile_vals, tile_row, tile_col, tile_work):
    peers = lax.axis_size(GY)
    gx, ny, nz = (lax.axis_size(axis) for axis in GX_GY)
    slots, order, _ = tile_vals.shape
    owned = slots // 2
    width = features.shape[1]
    vblocks = features.shape[0] // order
    blocks = peers * vblocks
    told, tiles = pl.pallas_call(
        lambda *refs: tell_kernel(slots, *refs),
        in_specs=[ANY] * 4,
        out_specs=[VMEM, VMEM],
        out_shape=[pltpu.HBM((peers, 2, 2 * slots), jnp.int32), vmem(tile_vals.shape, tile_vals.dtype)],
        scratch_shapes=[
            pltpu.VMEM((3, slots), jnp.int32),
            pltpu.SemaphoreType.DMA((3,)),
            pltpu.SemaphoreType.DMA((8,)),
        ],
        compiler_params=limit(4),
        name="tell",
    )(*(in_hbm(t) for t in (tile_row, tile_col, tile_work, tile_vals)))

    cores = 2
    mine = [features.reshape(vblocks, order, width)]
    for k in range(1, gx // cores):
        mine.append(lax.ppermute(mine[0], "gx", [(i, (i + cores * k) % gx) for i in range(gx)]))
    meta = lax.all_to_all(told, GY, split_axis=0, concat_axis=0, tiled=True)
    swapped = []
    for f in mine:
        swapped.append(lax.ppermute(f, "gx", [(i, i ^ 1) for i in range(gx)]))
    small = jax.ShapeDtypeStruct((owned,), jnp.int32)
    sent = pl.pallas_call(
        lambda *refs: plan_kernel(peers, slots, *refs),
        in_specs=[VMEM, VMEM],
        out_specs=ANY,
        out_shape=pltpu.HBM(tile_vals.shape, tile_vals.dtype),
        scratch_shapes=[pltpu.SemaphoreType.DMA((1,))],
        compiler_params=limit(4),
        name="plan",
    )(in_vmem(meta), in_vmem(tiles))
    moved_row, moved_col, moved_work, kept = pl.pallas_call(
        lambda *refs: list_kernel(peers, slots, *refs),
        in_specs=[SMEM],
        out_specs=[SMEM] * 4,
        out_shape=[small] * 4,
        compiler_params=limit(4),
        name="list",
    )(meta)
    got = lax.all_to_all(sent, GY, split_axis=0, concat_axis=0, tiled=True)

    steps = 8
    span = blocks // ny
    i16 = jnp.int16

    def line(count, more=8):
        return vmem((count * order + more, width), i16)

    lines = blocks // 2 // vblocks
    few = span // 2
    keep, even, odd = pl.pallas_call(
        lambda *refs: product_kernel(gx, peers, ny, steps, *refs),
        in_specs=[SMEM] * 3 + [VMEM] * (1 + gx),
        out_specs=[ANY] * 3,
        out_shape=[pltpu.HBM((blocks // 2, order, width), jnp.float32)]
        + [pltpu.HBM((lines * order + lines, width), i16)] * 2,
        scratch_shapes=[
            pltpu.VMEM((blocks, order, width), jnp.float32),
            pltpu.VMEM((gx * vblocks, order, width), jnp.bfloat16),
            pltpu.VMEM((slots // steps, order, width), jnp.float32),
            pltpu.VMEM((lines, width), jnp.float32),
            pltpu.VMEM((2, lines * order + lines, width), i16),
            pltpu.SemaphoreType.DMA((5,)),
        ],
        compiler_params=limit(16),
        name="products",
    )(tile_row, tile_col, tile_work, *(in_vmem(f) for f in (tiles, *mine, *swapped)))
    near = []
    for v, q in enumerate((even, odd)):
        near.append(lax.ppermute(q, "z", [(i, ((i + v) ^ 1) - v & nz - 1) for i in range(nz)]))
    some = vmem((few, order, width), jnp.float32)
    own, rest, right, left = pl.pallas_call(
        lambda *refs: join_kernel(order, vblocks, ny, *refs),
        in_specs=[VMEM] * 3,
        out_specs=[VMEM] * 4,
        out_shape=[some, some, line(few), line(few)],
        scratch_shapes=[pltpu.VMEM((2 * lines, width), jnp.float32), pltpu.VMEM((8, width), jnp.float32)],
        compiler_params=limit(12),
        name="join",
    )(keep, *near)
    low, high = shifted(right, "y", 1), shifted(left, "y", -1)
    right, left = pl.pallas_call(
        lambda *refs: relay_kernel(order, *refs),
        in_specs=[VMEM] * 3,
        out_specs=[VMEM] * 2,
        out_shape=[line(few // 2)] * 2,
        scratch_shapes=[pltpu.VMEM((8, width), jnp.float32), pltpu.VMEM((8, width), jnp.float32)],
        compiler_params=limit(8),
        name="relay",
    )(rest, low, high)
    low2, high2 = shifted(right, "y", 1), shifted(left, "y", -1)
    own_z, *coded_z = pl.pallas_call(
        lambda *refs: middle_kernel(order, vblocks, *refs),
        in_specs=[VMEM] * 5,
        out_specs=[VMEM] * (nz // 2),
        out_shape=[vmem((vblocks * order, width), jnp.float32)] + [line(vblocks)] * (nz // 2 - 1),
        scratch_shapes=[pltpu.VMEM((few, order, width), jnp.float32), pltpu.VMEM((8, width), jnp.float32)],
        compiler_params=limit(8),
        name="middle",
    )(own, low, high, low2, high2)
    got_z = []
    for k, q in enumerate(coded_z, 1):
        got_z.append(shifted(q, "z", 2 * k))
    product = pl.pallas_call(
        lambda *refs: last_kernel(order, vblocks, *refs),
        in_specs=[VMEM] * (nz // 2),
        out_specs=VMEM,
        out_shape=jax.ShapeDtypeStruct((vblocks * order, width), jnp.float32),
        compiler_params=limit(4),
        name="last",
    )(*(in_vmem(g) for g in (own_z, *got_z)))

    moved_vals = pl.pallas_call(
        lambda *refs: keep_kernel(owned, *refs),
        in_specs=[SMEM, VMEM],
        out_specs=ANY,
        out_shape=jax.ShapeDtypeStruct((owned, *tile_vals.shape[1:]), tile_vals.dtype),
        scratch_shapes=[pltpu.SemaphoreType.DMA((1,))],
        compiler_params=limit(4),
        name="keep",
    )(kept, in_vmem(got))
    return (product, moved_vals, moved_row, moved_col, moved_work)


def solution(mesh):
    finer = Mesh(mesh.devices.reshape(mesh.shape["gx"], 4, 8), GX_GY)
    in_specs = (P(GX_GY, None), P(GX_GY, None, None), P(GX_GY), P(GX_GY), P(GX_GY))

    return jax.shard_map(on_device, mesh=finer, in_specs=in_specs, out_specs=in_specs, check_vma=False)
```

```python
import jax
import jax.numpy as jnp
from jax import lax
from jax.experimental import pallas as pl
from jax.experimental.pallas import tpu as pltpu
from jax.sharding import Mesh
from jax.sharding import PartitionSpec as P

GY = ("y", "z")
GX_GY = ("gx", "y", "z")

ANY = pl.BlockSpec(memory_space=pl.ANY)
SMEM = pl.BlockSpec(memory_space=pltpu.SMEM)
VMEM = pl.BlockSpec(memory_space=pltpu.VMEM)


def in_vmem(array):
    return pltpu.with_memory_space_constraint(array, pltpu.VMEM)


def in_hbm(array):
    return pltpu.with_memory_space_constraint(array, pltpu.HBM)


def vmem(shape, dtype):
    return pltpu.VMEM(shape, dtype)


def limit(mib):
    return pltpu.CompilerParams(vmem_limit_bytes=mib * 2**20)


def shifted(array, axis, by):
    size = lax.axis_size(axis)
    return lax.ppermute(array, axis, [(i, (i + by) % size) for i in range(size)])


def tell_kernel(slots, row_ref, col_ref, work_ref, out_ref, held, sems):
    copies = [
        pltpu.make_async_copy(ref, held.at[i], sems.at[i]) for i, ref in enumerate((row_ref, col_ref, work_ref))
    ]
    for c in copies:
        c.start()
    for c in copies:
        c.wait()
    row, col, work = (held[i].reshape(1, slots) for i in range(3))
    count = jnp.sum((work > 0).astype(jnp.int32), axis=1, keepdims=True)
    for i, pair in enumerate(((row, col), (work, jnp.broadcast_to(count, (1, slots))))):
        line = jnp.concatenate(pair, axis=1)
        out_ref[:, i, :] = jnp.broadcast_to(line, (out_ref.shape[0], 2 * slots))


def stage_kernel(vals_ref, out_ref, sems):
    groups = sems.shape[0]
    size = vals_ref.shape[0] // groups
    copies = [
        pltpu.make_async_copy(
            vals_ref.at[pl.ds(g * size, size)], out_ref.at[pl.ds(g * size, size)], sems.at[g]
        )
        for g in range(groups)
    ]
    for c in copies:
        c.start()
    for c in copies:
        c.wait()


def place_of():
    return lax.axis_index("y") * lax.axis_size("z") + lax.axis_index("z")


def plan_kernel(peers, slots, meta_ref, vals_ref, sent_ref, sems):
    me = place_of()
    share = slots // peers

    counts = meta_ref[:, 1, :]
    earlier = (lax.broadcasted_iota(jnp.int32, counts.shape, 0) < me) & (
        lax.broadcasted_iota(jnp.int32, counts.shape, 1) == slots
    )
    first = jnp.sum(jnp.where(earlier, counts, 0).astype(jnp.float32)).astype(jnp.int32)
    turn = lax.rem(first, peers)

    def start(d, carry):
        at = lax.rem(d - turn + peers, peers)
        for w in range(share):
            pltpu.make_async_copy(
                vals_ref.at[at + w * peers], sent_ref.at[d * share + w], sems.at[0]
            ).start()
        return carry

    lax.fori_loop(0, peers, start, 0, unroll=8)
    pltpu.make_async_copy(vals_ref, sent_ref, sems.at[0]).wait()


def list_kernel(peers, slots, meta_ref, row_ref, col_ref, work_ref, slot_ref):
    me = place_of()
    share = slots // peers

    def source(s, begin):
        count = meta_ref[s, 1, slots]
        j = lax.rem(me - lax.rem(begin, peers) + peers, peers)
        for w in range(share):
            at = j + w * peers

            @pl.when(at < count)
            def _():
                k = lax.div(begin + at, peers)
                row_ref[k] = meta_ref[s, 0, at]
                col_ref[k] = meta_ref[s, 0, slots + at]
                work_ref[k] = meta_ref[s, 1, at]
                slot_ref[k] = s * share + w

        return begin + count

    lax.fori_loop(0, peers, source, jnp.int32(0))


def keep_kernel(owned, slot_ref, got_ref, out_ref, sems):
    def start(k, carry):
        pltpu.make_async_copy(got_ref.at[slot_ref[k]], out_ref.at[k], sems.at[0]).start()
        return carry

    lax.fori_loop(0, owned, start, 0)
    pltpu.make_async_copy(got_ref.at[pl.ds(0, owned)], out_ref, sems.at[0]).wait()


MARGIN = 0.999


def coded(x, q_ref, exps_ref, at, row):
    top = jnp.maximum(jnp.max(jnp.abs(x), axis=0, keepdims=True), 1e-30)
    exponent = jnp.ceil(jnp.log2(top))
    scaled = jnp.round(x * (jnp.exp2(15.0 - exponent) * MARGIN))
    q_ref[pl.ds(at, x.shape[0]), :] = scaled.astype(jnp.int32).astype(jnp.int16)
    exps_ref[pl.ds(row, 1), :] = exponent


def product_kernel(gx, gy, groups, steps, row_ref, col_ref, work_ref, tiles, feats_ref, swap_ref, *refs):
    keep_ref, even_ref, odd_ref, acc, held, made, exps, codes, sems = refs
    slots, order, _ = tiles.shape
    per_step = slots // steps
    vblocks = held.shape[0] // gx
    blocks = acc.shape[0]
    span = blocks // groups
    a = lax.axis_index("gx")
    cores = 2

    acc[...] = jnp.zeros_like(acc)
    for k, f in enumerate((feats_ref, swap_ref)):
        held[pl.ds(k * f.shape[0], f.shape[0])] = f[...]

    pattern = lax.broadcasted_iota(jnp.int32, (order, order), 0) * order + lax.broadcasted_iota(
        jnp.int32, (order, order), 1
    )
    for i in range(steps):

        def form(t, carry):
            tile = i * per_step + t
            col = col_ref[tile]
            home = lax.div(col, gy * vblocks)
            away = lax.rem(lax.div(a, cores) - lax.div(home, cores) + gx, gx // cores)
            side = lax.rem(a + home, cores)
            place = (side * (gx // cores) + away) * vblocks + lax.rem(col, vblocks)
            masked = jnp.where(pattern < work_ref[tile], tiles[tile], jnp.zeros((), jnp.bfloat16))
            made[t] = jnp.dot(masked, held[place], preferred_element_type=jnp.float32)
            return carry

        lax.fori_loop(0, per_step, form, 0, unroll=True)

        def add(t, carry):
            row = lax.rem(row_ref[i * per_step + t], blocks)
            acc[row] += made[t]
            return carry

        lax.fori_loop(0, per_step, add, 0, unroll=True)

    owners = span // vblocks
    pairs = owners // 2
    side = lax.rem(lax.axis_index("z"), 2)

    def leave(n, carry):
        at = lax.div(n, pairs) * span + (2 * lax.rem(n, pairs) + side) * vblocks
        pltpu.make_async_copy(
            acc.at[pl.ds(at, vblocks)], keep_ref.at[pl.ds(n * vblocks, vblocks)], sems.at[0]
        ).start()
        return carry

    lax.fori_loop(0, groups * pairs, leave, 0)
    lines = groups * pairs
    parts = 2
    leaving = []
    for v, q_ref in enumerate((even_ref, odd_ref)):
        held_codes = codes.at[v]

        def code(n, carry):
            at = lax.div(n, pairs) * span + (2 * lax.rem(n, pairs) + 1 - side) * vblocks + v
            coded(acc[at], held_codes, exps, n * order, n)
            return carry

        for i in range(parts):
            lax.fori_loop(i * lines // parts, (i + 1) * lines // parts, code, 0, unroll=4)
            if i == parts - 1:
                store_exps(held_codes, exps, lines, order)
            begin = i * lines * order // parts
            size = q_ref.shape[0] - begin if i == parts - 1 else lines * order // parts
            leaving.append(
                pltpu.make_async_copy(
                    held_codes.at[pl.ds(begin, size)], q_ref.at[pl.ds(begin, size)], sems.at[1 + v * parts + i]
                )
            )
            leaving[-1].start()
    for c in leaving:
        c.wait()
    pltpu.make_async_copy(acc.at[pl.ds(0, keep_ref.shape[0])], keep_ref, sems.at[0]).wait()


def scales_of(ref, at):
    exps = ref[pl.ds(at, ref.shape[0] - at), :].astype(jnp.int32).astype(jnp.float32)
    return jnp.exp2(exps - 15.0) * (1.0 / MARGIN)


def part_of(ref, i, order, count):
    x = ref[pl.ds(i * order, order), :].astype(jnp.int32).astype(jnp.float32)
    return x * scales_of(ref, count * order)[i : i + 1, :]


def store_exps(q_ref, exps, count, order):
    q_ref[pl.ds(count * order, exps.shape[0]), :] = exps[...].astype(jnp.int32).astype(jnp.int16)


def join_kernel(order, vblocks, groups, keep_ref, even_ref, odd_ref, own_ref, rest_ref, right_ref, left_ref, scales, exps):
    span = keep_ref.shape[0] // groups
    half = span // 2
    lines = groups * span // vblocks
    y = lax.axis_index("y")
    got = (even_ref, odd_ref)
    for v, g in enumerate(got):
        scales[pl.ds(v * lines, lines), :] = scales_of(g, lines * order)

    def total(chunk, pair, v):
        n = chunk * (span // vblocks) + pair
        x = got[v][pl.ds(n * order, order), :].astype(jnp.int32).astype(jnp.float32)
        return keep_ref[n * vblocks + v] + x * scales[pl.ds(v * lines + n, 1), :]

    there, far, behind = (lax.rem(y + k, groups) for k in range(1, groups))
    low, high = 0, half // vblocks
    for chunk, start, at in ((y, low, 0), (y, high, half)):
        for i in range(half // vblocks):
            for v in range(vblocks):
                own_ref[at + i * vblocks + v] = total(chunk, start + i, v)
    for chunk, start, at in ((there, low, 0), (behind, high, half)):
        for i in range(half // vblocks):
            for v in range(vblocks):
                rest_ref[at + i * vblocks + v] = total(chunk, start + i, v)
    for q_ref, parts in ((right_ref, ((far, low), (there, high))), (left_ref, ((far, high), (behind, low)))):
        for n, (chunk, start) in enumerate(parts):
            for i in range(half // vblocks):
                for v in range(vblocks):
                    row = n * half + i * vblocks + v
                    coded(total(chunk, start + i, v), q_ref, exps, row * order, row)
        store_exps(q_ref, exps, span, order)


def relay_kernel(order, rest_ref, low_ref, high_ref, right_ref, left_ref, scales, exps):
    span = rest_ref.shape[0]
    half = span // 2
    exps[...] = jnp.zeros_like(exps)
    for side, (got, q_ref) in enumerate(((low_ref, right_ref), (high_ref, left_ref))):
        scales[...] = scales_of(got, span * order)
        for i in range(half):
            part = got[pl.ds(i * order, order), :].astype(jnp.int32).astype(jnp.float32)
            x = rest_ref[side * half + i] + part * scales[pl.ds(i, 1), :]
            coded(x, q_ref, exps, i * order, i)
        store_exps(q_ref, exps, half, order)


def middle_kernel(order, vblocks, own_ref, low_ref, high_ref, low2_ref, high2_ref, out_ref, *refs):
    q_refs, (total, exps) = refs[:-2], refs[-2:]
    span = own_ref.shape[0]
    half = span // 2
    owners = span // vblocks
    mine = lax.div(lax.axis_index("z"), 2)
    exps[...] = jnp.zeros_like(exps)
    for side, (near, last) in enumerate(((high_ref, low2_ref), (low_ref, high2_ref))):
        near_scales, last_scales = scales_of(near, span * order), scales_of(last, half * order)
        for i in range(half):
            x = own_ref[side * half + i]
            for ref, at, scale in ((near, half + i, near_scales[half + i : half + i + 1]), (last, i, last_scales[i : i + 1])):
                x = x + ref[pl.ds(at * order, order), :].astype(jnp.int32).astype(jnp.float32) * scale
            total[side * half + i] = x
    for v in range(vblocks):
        out_ref[pl.ds(v * order, order), :] = total[mine * vblocks + v]
    for k, q_ref in enumerate(q_refs, 1):
        base = lax.rem(mine + k, owners) * vblocks
        for v in range(vblocks):
            coded(total[base + v], q_ref, exps, v * order, v)
        store_exps(q_ref, exps, vblocks, order)


def last_kernel(order, vblocks, own_ref, *refs):
    got, out_ref = refs[:-1], refs[-1]
    for v in range(vblocks):
        x = own_ref[pl.ds(v * order, order), :]
        for g in got:
            x = x + part_of(g, v, order, vblocks)
        out_ref[pl.ds(v * order, order), :] = x


def on_device(features, tile_vals, tile_row, tile_col, tile_work):
    peers = lax.axis_size(GY)
    gx, ny, nz = (lax.axis_size(axis) for axis in GX_GY)
    slots, order, _ = tile_vals.shape
    owned = slots // 2
    width = features.shape[1]
    vblocks = features.shape[0] // order
    blocks = peers * vblocks
    told = pl.pallas_call(
        lambda *refs: tell_kernel(slots, *refs),
        in_specs=[ANY] * 3,
        out_specs=VMEM,
        out_shape=jax.ShapeDtypeStruct((peers, 2, 2 * slots), jnp.int32),
        scratch_shapes=[pltpu.VMEM((3, slots), jnp.int32), pltpu.SemaphoreType.DMA((3,))],
        compiler_params=limit(4),
        name="tell",
    )(*(in_hbm(t) for t in (tile_row, tile_col, tile_work)))

    cores = 2
    mine = [features.reshape(vblocks, order, width)]
    for k in range(1, gx // cores):
        mine.append(lax.ppermute(mine[0], "gx", [(i, (i + cores * k) % gx) for i in range(gx)]))
    meta = lax.all_to_all(told, GY, split_axis=0, concat_axis=0, tiled=True)
    feats = jnp.concatenate(mine)
    swapped = lax.ppermute(feats, "gx", [(i, i ^ 1) for i in range(gx)])
    tiles = pl.pallas_call(
        stage_kernel,
        in_specs=[ANY],
        out_specs=VMEM,
        out_shape=vmem(tile_vals.shape, tile_vals.dtype),
        scratch_shapes=[pltpu.SemaphoreType.DMA((8,))],
        compiler_params=limit(4),
        name="stage",
    )(in_hbm(tile_vals))
    small = jax.ShapeDtypeStruct((owned,), jnp.int32)
    sent = pl.pallas_call(
        lambda *refs: plan_kernel(peers, slots, *refs),
        in_specs=[VMEM, VMEM],
        out_specs=ANY,
        out_shape=pltpu.HBM(tile_vals.shape, tile_vals.dtype),
        scratch_shapes=[pltpu.SemaphoreType.DMA((1,))],
        compiler_params=limit(4),
        name="plan",
    )(in_vmem(meta), in_vmem(tiles))
    moved_row, moved_col, moved_work, kept = pl.pallas_call(
        lambda *refs: list_kernel(peers, slots, *refs),
        in_specs=[SMEM],
        out_specs=[SMEM] * 4,
        out_shape=[small] * 4,
        compiler_params=limit(4),
        name="list",
    )(meta)
    got = lax.all_to_all(sent, GY, split_axis=0, concat_axis=0, tiled=True)

    steps = 4
    span = blocks // ny
    i16 = jnp.int16

    def line(count, more=8):
        return vmem((count * order + more, width), i16)

    lines = blocks // 2 // vblocks
    few = span // 2
    keep, even, odd = pl.pallas_call(
        lambda *refs: product_kernel(gx, peers, ny, steps, *refs),
        in_specs=[SMEM] * 3 + [VMEM] * 3,
        out_specs=[ANY] * 3,
        out_shape=[pltpu.HBM((blocks // 2, order, width), jnp.float32)]
        + [pltpu.HBM((lines * order + lines, width), i16)] * 2,
        scratch_shapes=[
            pltpu.VMEM((blocks, order, width), jnp.float32),
            pltpu.VMEM((gx * vblocks, order, width), jnp.bfloat16),
            pltpu.VMEM((slots // steps, order, width), jnp.float32),
            pltpu.VMEM((lines, width), jnp.float32),
            pltpu.VMEM((2, lines * order + lines, width), i16),
            pltpu.SemaphoreType.DMA((5,)),
        ],
        compiler_params=limit(16),
        name="products",
    )(tile_row, tile_col, tile_work, *(in_vmem(f) for f in (tiles, feats, swapped)))
    near = []
    for v, q in enumerate((even, odd)):
        near.append(lax.ppermute(q, "z", [(i, ((i + v) ^ 1) - v & nz - 1) for i in range(nz)]))
    some = vmem((few, order, width), jnp.float32)
    own, rest, right, left = pl.pallas_call(
        lambda *refs: join_kernel(order, vblocks, ny, *refs),
        in_specs=[VMEM] * 3,
        out_specs=[VMEM] * 4,
        out_shape=[some, some, line(few), line(few)],
        scratch_shapes=[pltpu.VMEM((2 * lines, width), jnp.float32), pltpu.VMEM((8, width), jnp.float32)],
        compiler_params=limit(12),
        name="join",
    )(keep, *near)
    low, high = shifted(right, "y", 1), shifted(left, "y", -1)
    right, left = pl.pallas_call(
        lambda *refs: relay_kernel(order, *refs),
        in_specs=[VMEM] * 3,
        out_specs=[VMEM] * 2,
        out_shape=[line(few // 2)] * 2,
        scratch_shapes=[pltpu.VMEM((8, width), jnp.float32), pltpu.VMEM((8, width), jnp.float32)],
        compiler_params=limit(8),
        name="relay",
    )(rest, low, high)
    low2, high2 = shifted(right, "y", 1), shifted(left, "y", -1)
    own_z, *coded_z = pl.pallas_call(
        lambda *refs: middle_kernel(order, vblocks, *refs),
        in_specs=[VMEM] * 5,
        out_specs=[VMEM] * (nz // 2),
        out_shape=[vmem((vblocks * order, width), jnp.float32)] + [line(vblocks)] * (nz // 2 - 1),
        scratch_shapes=[pltpu.VMEM((few, order, width), jnp.float32), pltpu.VMEM((8, width), jnp.float32)],
        compiler_params=limit(8),
        name="middle",
    )(own, low, high, low2, high2)
    got_z = []
    for k, q in enumerate(coded_z, 1):
        got_z.append(shifted(q, "z", 2 * k))
    product = pl.pallas_call(
        lambda *refs: last_kernel(order, vblocks, *refs),
        in_specs=[VMEM] * (nz // 2),
        out_specs=VMEM,
        out_shape=jax.ShapeDtypeStruct((vblocks * order, width), jnp.float32),
        compiler_params=limit(4),
        name="last",
    )(*(in_vmem(g) for g in (own_z, *got_z)))

    moved_vals = pl.pallas_call(
        lambda *refs: keep_kernel(owned, *refs),
        in_specs=[SMEM, VMEM],
        out_specs=ANY,
        out_shape=jax.ShapeDtypeStruct((owned, *tile_vals.shape[1:]), tile_vals.dtype),
        scratch_shapes=[pltpu.SemaphoreType.DMA((1,))],
        compiler_params=limit(4),
        name="keep",
    )(kept, in_vmem(got))
    return (product, moved_vals, moved_row, moved_col, moved_work)


def solution(mesh):
    finer = Mesh(mesh.devices.reshape(mesh.shape["gx"], 4, 8), GX_GY)
    in_specs = (P(GX_GY, None), P(GX_GY, None, None), P(GX_GY), P(GX_GY), P(GX_GY))

    return jax.shard_map(on_device, mesh=finer, in_specs=in_specs, out_specs=in_specs, check_vma=False)
```

```python
import jax
import jax.numpy as jnp
from jax import lax
from jax.experimental import pallas as pl
from jax.experimental.pallas import tpu as pltpu
from jax.sharding import Mesh
from jax.sharding import PartitionSpec as P

GY = ("y", "z")
GX_GY = ("gx", "y", "z")

ANY = pl.BlockSpec(memory_space=pl.ANY)
SMEM = pl.BlockSpec(memory_space=pltpu.SMEM)
VMEM = pl.BlockSpec(memory_space=pltpu.VMEM)


def in_vmem(array):
    return pltpu.with_memory_space_constraint(array, pltpu.VMEM)


def in_hbm(array):
    return pltpu.with_memory_space_constraint(array, pltpu.HBM)


def vmem(shape, dtype):
    return pltpu.VMEM(shape, dtype)


def limit(mib):
    return pltpu.CompilerParams(vmem_limit_bytes=mib * 2**20)


def shifted(array, axis, by):
    size = lax.axis_size(axis)
    return lax.ppermute(array, axis, [(i, (i + by) % size) for i in range(size)])


def tell_kernel(slots, row_ref, col_ref, work_ref, out_ref, held, sems):
    copies = [
        pltpu.make_async_copy(ref, held.at[i], sems.at[i]) for i, ref in enumerate((row_ref, col_ref, work_ref))
    ]
    for c in copies:
        c.start()
    for c in copies:
        c.wait()
    row, col, work = (held[i].reshape(1, slots) for i in range(3))
    count = jnp.sum((work > 0).astype(jnp.int32), axis=1, keepdims=True)
    for i, pair in enumerate(((row, col), (work, jnp.broadcast_to(count, (1, slots))))):
        line = jnp.concatenate(pair, axis=1)
        out_ref[:, i, :] = jnp.broadcast_to(line, (out_ref.shape[0], 2 * slots))


def stage_kernel(vals_ref, out_ref, sems):
    groups = sems.shape[0]
    size = vals_ref.shape[0] // groups
    copies = [
        pltpu.make_async_copy(
            vals_ref.at[pl.ds(g * size, size)], out_ref.at[pl.ds(g * size, size)], sems.at[g]
        )
        for g in range(groups)
    ]
    for c in copies:
        c.start()
    for c in copies:
        c.wait()


def place_of():
    return lax.axis_index("y") * lax.axis_size("z") + lax.axis_index("z")


def plan_kernel(peers, slots, meta_ref, vals_ref, sent_ref, sems):
    me = place_of()
    share = slots // peers

    counts = meta_ref[:, 1, :]
    earlier = (lax.broadcasted_iota(jnp.int32, counts.shape, 0) < me) & (
        lax.broadcasted_iota(jnp.int32, counts.shape, 1) == slots
    )
    first = jnp.sum(jnp.where(earlier, counts, 0).astype(jnp.float32)).astype(jnp.int32)
    turn = lax.rem(first, peers)

    def start(d, carry):
        at = lax.rem(d - turn + peers, peers)
        for w in range(share):
            pltpu.make_async_copy(
                vals_ref.at[at + w * peers], sent_ref.at[d * share + w], sems.at[0]
            ).start()
        return carry

    lax.fori_loop(0, peers, start, 0, unroll=True)
    pltpu.make_async_copy(vals_ref, sent_ref, sems.at[0]).wait()


def list_kernel(peers, slots, meta_ref, row_ref, col_ref, work_ref, slot_ref):
    me = place_of()
    share = slots // peers

    def source(s, begin):
        count = meta_ref[s, 1, slots]
        j = lax.rem(me - lax.rem(begin, peers) + peers, peers)
        for w in range(share):
            at = j + w * peers

            @pl.when(at < count)
            def _():
                k = lax.div(begin + at, peers)
                row_ref[k] = meta_ref[s, 0, at]
                col_ref[k] = meta_ref[s, 0, slots + at]
                work_ref[k] = meta_ref[s, 1, at]
                slot_ref[k] = s * share + w

        return begin + count

    lax.fori_loop(0, peers, source, jnp.int32(0))


def keep_kernel(owned, slot_ref, got_ref, out_ref, sems):
    def start(k, carry):
        pltpu.make_async_copy(got_ref.at[slot_ref[k]], out_ref.at[k], sems.at[0]).start()
        return carry

    lax.fori_loop(0, owned, start, 0, unroll=True)
    pltpu.make_async_copy(got_ref.at[pl.ds(0, owned)], out_ref, sems.at[0]).wait()


MARGIN = 0.999


def coded(x, q_ref, exps_ref, at, row):
    top = jnp.maximum(jnp.max(jnp.abs(x), axis=0, keepdims=True), 1e-30)
    exponent = jnp.ceil(jnp.log2(top))
    scaled = jnp.round(x * (jnp.exp2(15.0 - exponent) * MARGIN))
    q_ref[pl.ds(at, x.shape[0]), :] = scaled.astype(jnp.int32).astype(jnp.int16)
    exps_ref[pl.ds(row, 1), :] = exponent


def product_kernel(gx, gy, groups, steps, row_ref, col_ref, work_ref, tiles, feats_ref, swap_ref, *refs):
    keep_ref, even_ref, odd_ref, acc, held, made, exps, codes, sems = refs
    slots, order, _ = tiles.shape
    per_step = slots // steps
    vblocks = held.shape[0] // gx
    blocks = acc.shape[0]
    span = blocks // groups
    a = lax.axis_index("gx")
    cores = 2

    acc[...] = jnp.zeros_like(acc)
    for k, f in enumerate((feats_ref, swap_ref)):
        held[pl.ds(k * f.shape[0], f.shape[0])] = f[...]

    pattern = lax.broadcasted_iota(jnp.int32, (order, order), 0) * order + lax.broadcasted_iota(
        jnp.int32, (order, order), 1
    )
    for i in range(steps):

        def form(t, carry):
            tile = i * per_step + t
            col = col_ref[tile]
            home = lax.div(col, gy * vblocks)
            away = lax.rem(lax.div(a, cores) - lax.div(home, cores) + gx, gx // cores)
            side = lax.rem(a + home, cores)
            place = (side * (gx // cores) + away) * vblocks + lax.rem(col, vblocks)
            masked = jnp.where(pattern < work_ref[tile], tiles[tile], jnp.zeros((), jnp.bfloat16))
            made[t] = jnp.dot(masked, held[place], preferred_element_type=jnp.float32)
            return carry

        lax.fori_loop(0, per_step, form, 0, unroll=True)

        def add(t, carry):
            row = lax.rem(row_ref[i * per_step + t], blocks)
            acc[row] += made[t]
            return carry

        lax.fori_loop(0, per_step, add, 0, unroll=True)

    owners = span // vblocks
    pairs = owners // 2
    side = lax.rem(lax.axis_index("z"), 2)

    def leave(n, carry):
        at = lax.div(n, pairs) * span + (2 * lax.rem(n, pairs) + side) * vblocks
        pltpu.make_async_copy(
            acc.at[pl.ds(at, vblocks)], keep_ref.at[pl.ds(n * vblocks, vblocks)], sems.at[0]
        ).start()
        return carry

    lax.fori_loop(0, groups * pairs, leave, 0)
    lines = groups * pairs
    parts = 2
    leaving = []
    for v, q_ref in enumerate((even_ref, odd_ref)):
        held_codes = codes.at[v]

        def code(n, carry):
            at = lax.div(n, pairs) * span + (2 * lax.rem(n, pairs) + 1 - side) * vblocks + v
            coded(acc[at], held_codes, exps, n * order, n)
            return carry

        for i in range(parts):
            lax.fori_loop(i * lines // parts, (i + 1) * lines // parts, code, 0, unroll=2)
            if i == parts - 1:
                store_exps(held_codes, exps, lines, order)
            begin = i * lines * order // parts
            size = q_ref.shape[0] - begin if i == parts - 1 else lines * order // parts
            leaving.append(
                pltpu.make_async_copy(
                    held_codes.at[pl.ds(begin, size)], q_ref.at[pl.ds(begin, size)], sems.at[1 + v * parts + i]
                )
            )
            leaving[-1].start()
    for c in leaving:
        c.wait()
    pltpu.make_async_copy(acc.at[pl.ds(0, keep_ref.shape[0])], keep_ref, sems.at[0]).wait()


def scales_of(ref, at):
    exps = ref[pl.ds(at, ref.shape[0] - at), :].astype(jnp.int32).astype(jnp.float32)
    return jnp.exp2(exps - 15.0) * (1.0 / MARGIN)


def part_of(ref, i, order, count):
    x = ref[pl.ds(i * order, order), :].astype(jnp.int32).astype(jnp.float32)
    return x * scales_of(ref, count * order)[i : i + 1, :]


def store_exps(q_ref, exps, count, order):
    q_ref[pl.ds(count * order, exps.shape[0]), :] = exps[...].astype(jnp.int32).astype(jnp.int16)


def join_kernel(order, vblocks, groups, keep_ref, even_ref, odd_ref, own_ref, rest_ref, right_ref, left_ref, scales, exps):
    span = keep_ref.shape[0] // groups
    half = span // 2
    lines = groups * span // vblocks
    y = lax.axis_index("y")
    got = (even_ref, odd_ref)
    for v, g in enumerate(got):
        scales[pl.ds(v * lines, lines), :] = scales_of(g, lines * order)

    def total(chunk, pair, v):
        n = chunk * (span // vblocks) + pair
        x = got[v][pl.ds(n * order, order), :].astype(jnp.int32).astype(jnp.float32)
        return keep_ref[n * vblocks + v] + x * scales[pl.ds(v * lines + n, 1), :]

    there, far, behind = (lax.rem(y + k, groups) for k in range(1, groups))
    low, high = 0, half // vblocks
    for chunk, start, at in ((y, low, 0), (y, high, half)):
        for i in range(half // vblocks):
            for v in range(vblocks):
                own_ref[at + i * vblocks + v] = total(chunk, start + i, v)
    for chunk, start, at in ((there, low, 0), (behind, high, half)):
        for i in range(half // vblocks):
            for v in range(vblocks):
                rest_ref[at + i * vblocks + v] = total(chunk, start + i, v)
    for q_ref, parts in ((right_ref, ((far, low), (there, high))), (left_ref, ((far, high), (behind, low)))):
        for n, (chunk, start) in enumerate(parts):
            for i in range(half // vblocks):
                for v in range(vblocks):
                    row = n * half + i * vblocks + v
                    coded(total(chunk, start + i, v), q_ref, exps, row * order, row)
        store_exps(q_ref, exps, span, order)


def relay_kernel(order, rest_ref, low_ref, high_ref, right_ref, left_ref, scales, exps):
    span = rest_ref.shape[0]
    half = span // 2
    exps[...] = jnp.zeros_like(exps)
    for side, (got, q_ref) in enumerate(((low_ref, right_ref), (high_ref, left_ref))):
        scales[...] = scales_of(got, span * order)
        for i in range(half):
            part = got[pl.ds(i * order, order), :].astype(jnp.int32).astype(jnp.float32)
            x = rest_ref[side * half + i] + part * scales[pl.ds(i, 1), :]
            coded(x, q_ref, exps, i * order, i)
        store_exps(q_ref, exps, half, order)


def middle_kernel(order, vblocks, own_ref, low_ref, high_ref, low2_ref, high2_ref, out_ref, *refs):
    q_refs, (total, exps) = refs[:-2], refs[-2:]
    span = own_ref.shape[0]
    half = span // 2
    owners = span // vblocks
    mine = lax.div(lax.axis_index("z"), 2)
    exps[...] = jnp.zeros_like(exps)
    for side, (near, last) in enumerate(((high_ref, low2_ref), (low_ref, high2_ref))):
        near_scales, last_scales = scales_of(near, span * order), scales_of(last, half * order)
        for i in range(half):
            x = own_ref[side * half + i]
            for ref, at, scale in ((near, half + i, near_scales[half + i : half + i + 1]), (last, i, last_scales[i : i + 1])):
                x = x + ref[pl.ds(at * order, order), :].astype(jnp.int32).astype(jnp.float32) * scale
            total[side * half + i] = x
    for v in range(vblocks):
        out_ref[pl.ds(v * order, order), :] = total[mine * vblocks + v]
    for k, q_ref in enumerate(q_refs, 1):
        base = lax.rem(mine + k, owners) * vblocks
        for v in range(vblocks):
            coded(total[base + v], q_ref, exps, v * order, v)
        store_exps(q_ref, exps, vblocks, order)


def last_kernel(order, vblocks, own_ref, *refs):
    got, out_ref = refs[:-1], refs[-1]
    for v in range(vblocks):
        x = own_ref[pl.ds(v * order, order), :]
        for g in got:
            x = x + part_of(g, v, order, vblocks)
        out_ref[pl.ds(v * order, order), :] = x


def on_device(features, tile_vals, tile_row, tile_col, tile_work):
    peers = lax.axis_size(GY)
    gx, ny, nz = (lax.axis_size(axis) for axis in GX_GY)
    slots, order, _ = tile_vals.shape
    owned = slots // 2
    width = features.shape[1]
    vblocks = features.shape[0] // order
    blocks = peers * vblocks
    told = pl.pallas_call(
        lambda *refs: tell_kernel(slots, *refs),
        in_specs=[ANY] * 3,
        out_specs=VMEM,
        out_shape=jax.ShapeDtypeStruct((peers, 2, 2 * slots), jnp.int32),
        scratch_shapes=[pltpu.VMEM((3, slots), jnp.int32), pltpu.SemaphoreType.DMA((3,))],
        compiler_params=limit(4),
        name="tell",
    )(*(in_hbm(t) for t in (tile_row, tile_col, tile_work)))

    cores = 2
    mine = [features.reshape(vblocks, order, width)]
    for k in range(1, gx // cores):
        mine.append(lax.ppermute(mine[0], "gx", [(i, (i + cores * k) % gx) for i in range(gx)]))
    meta = lax.all_to_all(told, GY, split_axis=0, concat_axis=0, tiled=True)
    feats = jnp.concatenate(mine)
    swapped = lax.ppermute(feats, "gx", [(i, i ^ 1) for i in range(gx)])
    tiles = pl.pallas_call(
        stage_kernel,
        in_specs=[ANY],
        out_specs=VMEM,
        out_shape=vmem(tile_vals.shape, tile_vals.dtype),
        scratch_shapes=[pltpu.SemaphoreType.DMA((8,))],
        compiler_params=limit(4),
        name="stage",
    )(in_hbm(tile_vals))
    small = jax.ShapeDtypeStruct((owned,), jnp.int32)
    sent = pl.pallas_call(
        lambda *refs: plan_kernel(peers, slots, *refs),
        in_specs=[VMEM, VMEM],
        out_specs=ANY,
        out_shape=pltpu.HBM(tile_vals.shape, tile_vals.dtype),
        scratch_shapes=[pltpu.SemaphoreType.DMA((1,))],
        compiler_params=limit(4),
        name="plan",
    )(in_vmem(meta), in_vmem(tiles))
    moved_row, moved_col, moved_work, kept = pl.pallas_call(
        lambda *refs: list_kernel(peers, slots, *refs),
        in_specs=[SMEM],
        out_specs=[SMEM] * 4,
        out_shape=[small] * 4,
        compiler_params=limit(4),
        name="list",
    )(meta)
    got = lax.all_to_all(sent, GY, split_axis=0, concat_axis=0, tiled=True)

    steps = 8
    span = blocks // ny
    i16 = jnp.int16

    def line(count, more=8):
        return vmem((count * order + more, width), i16)

    lines = blocks // 2 // vblocks
    few = span // 2
    keep, even, odd = pl.pallas_call(
        lambda *refs: product_kernel(gx, peers, ny, steps, *refs),
        in_specs=[SMEM] * 3 + [VMEM] * 3,
        out_specs=[ANY] * 3,
        out_shape=[pltpu.HBM((blocks // 2, order, width), jnp.float32)]
        + [pltpu.HBM((lines * order + lines, width), i16)] * 2,
        scratch_shapes=[
            pltpu.VMEM((blocks, order, width), jnp.float32),
            pltpu.VMEM((gx * vblocks, order, width), jnp.bfloat16),
            pltpu.VMEM((slots // steps, order, width), jnp.float32),
            pltpu.VMEM((lines, width), jnp.float32),
            pltpu.VMEM((2, lines * order + lines, width), i16),
            pltpu.SemaphoreType.DMA((5,)),
        ],
        compiler_params=limit(16),
        name="products",
    )(tile_row, tile_col, tile_work, *(in_vmem(f) for f in (tiles, feats, swapped)))
    near = []
    for v, q in enumerate((even, odd)):
        near.append(lax.ppermute(q, "z", [(i, ((i + v) ^ 1) - v & nz - 1) for i in range(nz)]))
    some = vmem((few, order, width), jnp.float32)
    own, rest, right, left = pl.pallas_call(
        lambda *refs: join_kernel(order, vblocks, ny, *refs),
        in_specs=[VMEM] * 3,
        out_specs=[VMEM] * 4,
        out_shape=[some, some, line(few), line(few)],
        scratch_shapes=[pltpu.VMEM((2 * lines, width), jnp.float32), pltpu.VMEM((8, width), jnp.float32)],
        compiler_params=limit(12),
        name="join",
    )(keep, *near)
    low, high = shifted(right, "y", 1), shifted(left, "y", -1)
    right, left = pl.pallas_call(
        lambda *refs: relay_kernel(order, *refs),
        in_specs=[VMEM] * 3,
        out_specs=[VMEM] * 2,
        out_shape=[line(few // 2)] * 2,
        scratch_shapes=[pltpu.VMEM((8, width), jnp.float32), pltpu.VMEM((8, width), jnp.float32)],
        compiler_params=limit(8),
        name="relay",
    )(rest, low, high)
    low2, high2 = shifted(right, "y", 1), shifted(left, "y", -1)
    own_z, *coded_z = pl.pallas_call(
        lambda *refs: middle_kernel(order, vblocks, *refs),
        in_specs=[VMEM] * 5,
        out_specs=[VMEM] * (nz // 2),
        out_shape=[vmem((vblocks * order, width), jnp.float32)] + [line(vblocks)] * (nz // 2 - 1),
        scratch_shapes=[pltpu.VMEM((few, order, width), jnp.float32), pltpu.VMEM((8, width), jnp.float32)],
        compiler_params=limit(8),
        name="middle",
    )(own, low, high, low2, high2)
    got_z = []
    for k, q in enumerate(coded_z, 1):
        got_z.append(shifted(q, "z", 2 * k))
    product = pl.pallas_call(
        lambda *refs: last_kernel(order, vblocks, *refs),
        in_specs=[VMEM] * (nz // 2),
        out_specs=VMEM,
        out_shape=jax.ShapeDtypeStruct((vblocks * order, width), jnp.float32),
        compiler_params=limit(4),
        name="last",
    )(*(in_vmem(g) for g in (own_z, *got_z)))

    moved_vals = pl.pallas_call(
        lambda *refs: keep_kernel(owned, *refs),
        in_specs=[SMEM, VMEM],
        out_specs=ANY,
        out_shape=jax.ShapeDtypeStruct((owned, *tile_vals.shape[1:]), tile_vals.dtype),
        scratch_shapes=[pltpu.SemaphoreType.DMA((1,))],
        compiler_params=limit(4),
        name="keep",
    )(kept, in_vmem(got))
    return (product, moved_vals, moved_row, moved_col, moved_work)


def solution(mesh):
    finer = Mesh(mesh.devices.reshape(mesh.shape["gx"], 4, 8), GX_GY)
    in_specs = (P(GX_GY, None), P(GX_GY, None, None), P(GX_GY), P(GX_GY), P(GX_GY))

    return jax.shard_map(on_device, mesh=finer, in_specs=in_specs, out_specs=in_specs, check_vma=False)
```
